32 devices in a mesh: row: 8 (over z, core), col: 4 (over y, x).
Axes of the slice: x: 2, y: 2, z: 4, core: 2. Of those that a mesh axis runs over, the one named last changes fastest.
Arguments:
- pair_exchange: bfloat16 [64, 16, 1024], P(('row', 'col')), may hold values from -6 to 6
- conduction: bfloat16 [64, 4, 1024], P(('row', 'col')), may hold values from -6 to 6
- valence: bfloat16 [64, 4, 1024], P(('row', 'col')), may hold values from -6 to 6
- coulomb: float32 [1024], replicated, may hold values from 0.5 to 5
- screening: float32 [34, 1024], replicated, may hold values from 0.1 to 1
- energies: float32 [64, 16], P(('row', 'col')), may hold values from 1 to 9
- vectors: bfloat16 [64, 512], P(('row', 'col')), may hold values from -6 to 6
- k_coords: int32 [64, 2], P(('row', 'col')), may hold values from 0 to 31, as said below
Outputs:
- residual_block: float32 [64, 512], P(('row', 'col'))
- alpha: float32 [32, 32], replicated
The draws below stay inside these ranges and needn't reach their ends.
Inputs may be any that keep to these rules, and one draw needn't show every extreme that they name: `k_coords`: each row holds a k-point's coordinates on the periodic 32 x 2 mesh, first then second; every mesh point occurs exactly once.
All inputs are finite; a program needn't handle non-finite values.
Results may differ from the reference program's by a relative error of at most 0.0028.
Values may be sent and summed in bfloat16 or wider, within the bound.
A program may use at most 64 MiB of HBM per device.

```python
import math
import jax
import jax.numpy as jnp
from jax import lax

NV = 4
NC = 4
NB = 16
NG = 1024
NVEC = 32
MX = 32
NK = 64
MY = 2
NT = 1024
NQF = 34


def draw_energies(key, part):
    ramp = 1.0 + 2.0 * jnp.arange(NK, dtype=jnp.float32)[:, None] / NK
    base = jnp.exp(jax.random.uniform(key, (NK, NB), jnp.float32, 0.0, math.log(3.0)))
    return (base * ramp).astype(jnp.float32)


def draw_k_coords(key, part):
    order = jax.random.permutation(key, NK)
    return jnp.stack([order // MY, order % MY], axis=1).astype(jnp.int32)


def block_levels(key, dims, shards, least, largest):
    level = 1.0
    for axis_at, blocks in shards:
        draws = jax.random.uniform(jax.random.fold_in(jax.random.fold_in(key, 6), axis_at), (blocks,), jnp.float32, least / len(shards), largest / len(shards))
        level = level * jnp.repeat(jnp.exp(draws), dims[axis_at] // blocks).reshape((-1,) + (1,) * (len(dims) - 1 - axis_at))
    return level


def bell_draw(own_key, extent, spread, limit, cuts=(), kind=jnp.bfloat16):
    factor_of = block_levels(own_key, extent, cuts, -0.22, 0.18) if cuts else 1.0
    values = jax.random.normal(own_key, extent, jnp.float32) * spread * factor_of
    return jnp.minimum(jnp.maximum(values, -limit), limit).astype(kind)


def setup_inputs(seed: int = 0) -> dict:
    key_of = jax.random.split(jax.random.key(seed), 9)
    pair_exchange = bell_draw(key_of[0], (NK, NB, NG), 1.0, 6.0, ((0, 32),))
    conduction = bell_draw(key_of[1], (NK, NC, NG), 1.0, 6.0, ((0, 32),))
    valence = bell_draw(key_of[2], (NK, NV, NG), 1.0, 6.0, ((0, 32),))
    coulomb = jnp.clip(jnp.exp(jax.random.uniform(key_of[3], (NG,), jnp.float32, math.log(0.5), math.log(5.0))), 0.5, 5.0)
    screening = jnp.clip(jnp.exp(jax.random.uniform(key_of[4], (NQF, NG), jnp.float32, math.log(0.1), math.log(1.0))), 0.1, 1.0)
    energies = draw_energies(jax.random.fold_in(key_of[8], 71), 0)
    vectors = bell_draw(key_of[6], (NK, NB * NVEC), 1.0, 6.0, ((0, 32),))
    k_coords = draw_k_coords(jax.random.fold_in(key_of[8], 71), 0)
    return dict(pair_exchange=pair_exchange, conduction=conduction, valence=valence, coulomb=coulomb, screening=screening, energies=energies, vectors=vectors, k_coords=k_coords)


highest = lax.Precision.HIGHEST


def reference(pair_exchange, conduction, valence, coulomb, screening, energies, vectors, k_coords):
    moving = vectors.astype(jnp.float32).reshape(NK, NB, NVEC)
    joined = (valence.astype(jnp.float32)[:, :, None, :] * conduction.astype(jnp.float32)[:, None, :, :]).reshape(NK, NB, NG)
    pair_rows = lax.optimization_barrier(joined.astype(jnp.bfloat16)).astype(jnp.float32)
    along_first = jnp.arange(MX)
    along_second = jnp.arange(MY)
    fold_first = jnp.minimum(along_first, MX - along_first)
    fold_second = jnp.minimum(along_second, MY - along_second)
    mesh_index = (fold_first[:, None] * (MY // 2 + 1) + fold_second[None, :]).astype(jnp.int32)
    spectrum = jnp.fft.fft2(screening[mesh_index], axes=(0, 1)).real
    density = jnp.einsum("ktg,ktn->gn", pair_exchange.astype(jnp.float32), moving, precision=highest)
    place_first = k_coords[:, 0]
    place_second = k_coords[:, 1]
    block_size = 64 if NG % 64 == 0 else NG

    def one_block(running, anchor):
        piece_rows = lax.dynamic_slice_in_dim(pair_rows, anchor, block_size, 2)
        projected = jnp.einsum("ktg,ktn->kgn", piece_rows, moving, precision=highest)
        mesh_grid = jnp.zeros((MX, MY, block_size, NVEC), jnp.float32).at[place_first, place_second].set(projected)
        spectrum_part = lax.dynamic_slice_in_dim(spectrum, anchor, block_size, 2)
        potential = jnp.fft.ifft2(jnp.fft.fft2(mesh_grid, axes=(0, 1)) * spectrum_part[:, :, :, None], axes=(0, 1)).real
        sampled = potential[place_first, place_second]
        return running + jnp.einsum("ktg,kgn->ktn", piece_rows, sampled, precision=highest), None

    anchors = (jnp.arange(NG // block_size) * block_size).astype(jnp.int32)
    direct, _ = lax.scan(one_block, jnp.zeros((NK, NB, NVEC), jnp.float32), anchors)
    exchange_term = jnp.einsum("ktg,gn->ktn", pair_exchange.astype(jnp.float32) * coulomb, density, precision=highest)
    applied = energies[:, :, None] * moving + (2.0 / NT) * exchange_term - direct / NK
    alpha = jnp.einsum("ktm,ktn->mn", moving, applied, precision=highest) / NT
    residual = applied - jnp.einsum("ktm,mn->ktn", moving, alpha, precision=highest)
    return residual.reshape(NK, NB * NVEC), alpha
```

```python
import functools

import jax
import jax.numpy as jnp
from jax import lax
from jax.experimental import pallas as pl
from jax.experimental.pallas import tpu as pltpu
from jax.sharding import PartitionSpec as P

MX = 32
LANES = 128
MESH = pl.DeviceIdType.MESH
F32 = jnp.float32
BF16 = jnp.bfloat16


def split_pair(value):
    high = value.astype(BF16)
    return high, (value - high.astype(F32)).astype(BF16)


def dot(a, b, contract):
    return lax.dot_general(a, b, ((contract[0:1], contract[1:2]), ((), ())), preferred_element_type=F32)


def iota(shape, axis):
    return lax.broadcasted_iota(jnp.int32, shape, axis)


def one_hot(condition):
    return jnp.where(condition, 1.0, 0.0).astype(BF16)


def kernel(
    dims, px_hbm, cond_hbm, val_hbm, coulomb_hbm, screening_hbm, vec_hbm, energy_hbm, place_hbm,
    out_ref, alpha_ref,
    px_ref, cond_ref, val_ref, coulomb_ref, screening_ref, vec_ref, energy_ref, place_ref, msg_ref, wide_ref, load_sem,
    slots, px_slots, sel_v, sel_c, tile_m, block_m, perm, sel_k, screen, tiled, pairs, proj, coords, coupling,
    dens_slots, partial, out_send, out_slots, gram_slots,
    in_recv, relay_recv, sends, arrivals,
):
    rows, cols, nk, nv, nc, nvec, total, mesh_cols = dims
    row, col = lax.axis_index("row"), lax.axis_index("col")
    me = row * cols + col
    count = rows * cols
    kb = rows * nk
    nb = nv * nc
    unit = nk * nv
    per = kb * nv
    batch = per * nc

    def other(step):
        peer = lax.rem(me + step, count)
        return peer // cols, lax.rem(peer, cols)

    barrier = pltpu.get_barrier_semaphore()

    for step in range(1, rows):
        pl.semaphore_signal(barrier, inc=1, device_id=(lax.rem(row + step, rows), col), device_id_type=MESH)
    for step in range(1, cols):
        pl.semaphore_signal(barrier, inc=1, device_id=(row, lax.rem(col + step, cols)), device_id_type=MESH)

    mine = pl.ds(pl.multiple_of(row * LANES, LANES), LANES)
    loads = [
        pltpu.make_async_copy(src, dst, load_sem.at[at])
        for at, (src, dst) in enumerate((
            (val_hbm, val_ref), (cond_hbm, cond_ref), (vec_hbm, vec_ref), (place_hbm, place_ref), (energy_hbm, energy_ref), (px_hbm, px_ref),
            (screening_hbm.at[:, mine], screening_ref), (coulomb_hbm.at[:, mine], coulomb_ref)))
    ]
    for load in loads:
        load.start()
    for load in loads[:5]:
        load.wait()
    row8 = iota((8, LANES), 0)
    lane8 = iota((8, LANES), 1)
    spots = jnp.zeros((8, LANES), F32)
    for axis in range(2):
        for k in range(nk):
            spots = jnp.where(row8 == axis * nk + k, place_ref[k, axis].astype(F32), spots)
    energy = jnp.zeros((8, LANES), F32)
    for k in range(nk):
        for t in range(nb):
            energy = jnp.where((row8 == k * nv + t // nc) & (lane8 // nvec == t % nc), energy_ref[k, t], energy)
    vec = vec_ref[...].astype(F32)
    packed_own = jnp.concatenate(
        [vec[k:k + 1, j * LANES:(j + 1) * LANES] for k in range(nk) for j in range(nv)], axis=0)
    wide_ref[0] = packed_own
    wide_ref[1] = energy * packed_own
    message = jnp.concatenate(
        [ref[k].astype(F32) for k in range(nk) for ref in (val_ref, cond_ref)], axis=0).astype(BF16)
    extra = jnp.concatenate([packed_own, spots], axis=0).astype(BF16)
    for r in range(rows):
        msg_ref[r, 0:16] = message[:, r * LANES:(r + 1) * LANES]
        msg_ref[r, 16:32] = extra

    loads[5].wait()
    slots[col, row] = msg_ref[row]

    pl.semaphore_wait(barrier, rows + cols - 2)

    def in_copy(step):
        pr = lax.rem(row + step, rows)
        return pltpu.make_async_remote_copy(
            src_ref=msg_ref.at[pr, 0:28], dst_ref=slots.at[col, row, 0:28],
            send_sem=sends.at[0], recv_sem=in_recv.at[row],
            device_id=(pr, col), device_id_type=MESH)

    def across(step):
        far = lax.rem(col // 2 + step // 2, cols // 2)
        return far * 2 + lax.rem(lax.rem(col, 2) + lax.rem(step, 2), 2)

    def relay_copy(r, step):
        pc = across(step)
        return pltpu.make_async_remote_copy(
            src_ref=slots.at[col, r, 0:28], dst_ref=slots.at[col, r, 0:28],
            send_sem=sends.at[1], recv_sem=relay_recv.at[col],
            device_id=(row, pc), device_id_type=MESH)

    def px_copy(step):
        pr = lax.rem(row + step, rows)
        return pltpu.make_async_remote_copy(
            src_ref=px_ref.at[:, :, pl.ds(pl.multiple_of(pr * LANES, LANES), LANES)], dst_ref=px_slots.at[row],
            send_sem=sends.at[2], recv_sem=arrivals.at[0],
            device_id=(pr, col), device_id_type=MESH)

    def dens_copy(step):
        pc = lax.rem(col + step, cols)
        return pltpu.make_async_remote_copy(
            src_ref=dens_slots.at[col], dst_ref=dens_slots.at[col],
            send_sem=sends.at[3], recv_sem=arrivals.at[1],
            device_id=(row, pc), device_id_type=MESH)

    def gram_copy(step):
        pr, pc = other(step)
        return pltpu.make_async_remote_copy(
            src_ref=gram_slots.at[me], dst_ref=gram_slots.at[me],
            send_sem=sends.at[4], recv_sem=arrivals.at[2],
            device_id=(pr, pc), device_id_type=MESH)

    def o_copy(step):
        pr = lax.rem(row + step, rows)
        return pltpu.make_async_remote_copy(
            src_ref=out_send.at[pr], dst_ref=out_slots.at[row],
            send_sem=sends.at[5], recv_sem=arrivals.at[3],
            device_id=(pr, col), device_id_type=MESH)

    def start_all(copy, end):
        def body(step, carry):
            copy(step).start()
            return carry
        lax.fori_loop(1, end, body, 0)

    def landed(ref, sem):
        pltpu.make_async_copy(ref, ref, sem).wait()

    start_all(in_copy, rows)
    start_all(px_copy, rows)
    px_slots[row] = px_ref[:, :, mine]

    for step in range(1, cols):
        relay_copy(row, step).start()
    at = iota((batch, rows * 16), 0)
    to = iota((batch, rows * 16), 1)
    base = (at // unit) % rows * 16 + (at // nv) % nk * 8
    sel_v[...] = one_hot(to == base + at % nv)
    sel_c[...] = one_hot(to == base + nv + at // per)
    at = iota((LANES, nc * LANES), 0)
    to = iota((LANES, nc * LANES), 1)
    tile_m[...] = one_hot((at // nvec == to // LANES) & (at % nvec == to % nvec))
    at = iota((batch, kb * nvec), 0)
    to = iota((batch, kb * nvec), 1)
    block_m[...] = one_hot((at // nv) % kb == to // nvec)
    at = iota((batch, rows * nk * nb), 0)
    to = iota((batch, rows * nk * nb), 1)
    perm[...] = one_hot(to == (at // nv) % kb * nb + at % nv * nc + at // per)
    at = iota((2 * cols * kb, count * 8), 0)
    to = iota((2 * cols * kb, count * 8), 1)
    point = at % (cols * kb)
    sel_k[...] = one_hot(to == point // nk * 8 + at // (cols * kb) * nk + point % nk)
    for load in loads[6:]:
        load.wait()
    high, low = split_pair(jnp.concatenate(
        [screening_ref[...], jnp.zeros((LANES - screening_ref.shape[0], LANES), F32)], axis=0))
    screen[0:LANES] = high
    screen[LANES:2 * LANES] = low

    def relay(d, carry):
        r = lax.rem(row + d, rows)
        landed(slots.at[col, r, 0:28], in_recv.at[r])
        for step in range(1, cols):
            relay_copy(r, step).start()
        return carry

    lax.fori_loop(1, rows, relay, 0)

    def take_batch(which):
        got = slots[which]
        factors = got[:, 0:16, :].reshape(rows * 16, LANES)
        rest = got[:, 16:32, :].astype(F32)
        packed = rest[:, 0:8, :].reshape(per, LANES).astype(BF16)
        spots_in = rest[:, 8:16, :].reshape(rows * 8, LANES)
        coords[which] = jnp.where(iota(spots_in.shape, 0) % 8 < 4, spots_in, 0.0).astype(BF16)
        wide = dot(packed, tile_m[...], (1, 0)).astype(BF16)
        stacked = jnp.concatenate([wide[:, s * LANES:(s + 1) * LANES] for s in range(nc)], axis=0)
        tiled[which] = stacked
        joined = (dot(sel_v[...], factors, (1, 0)) * dot(sel_c[...], factors, (1, 0))).astype(BF16)
        pairs[which] = joined.astype(F32)
        spread = jnp.concatenate([stacked] * (kb * nvec // LANES), axis=1) * block_m[...]
        projected = dot(spread, joined, (0, 0))
        proj[pl.ds(which * kb, kb)] = projected.reshape(kb, nvec, LANES)

    take_batch(col)

    landed(px_slots.at[0:rows - 1], arrivals.at[0])
    px = dot(perm[...], px_slots[...].reshape(rows * nk * nb, LANES), (1, 0)).astype(BF16)
    own_x = tiled[col][:, 0:nvec]
    dens_slots[col] = dot(own_x, px, (0, 0))
    start_all(dens_copy, cols)

    def rest_batches(step, carry):
        c = across(step)
        landed(slots.at[c, :, 0:28], relay_recv.at[c])
        take_batch(c)
        return carry

    lax.fori_loop(1, cols, rest_batches, 0)

    place = dot(sel_k[...], coords[...].reshape(count * 8, LANES), (1, 0))
    points = cols * kb
    first, second = place[0:points], place[points:2 * points]
    lane = iota((points, LANES), 1).astype(F32)
    coupling[0, 0:points] = first
    coupling[1, 0:points] = second
    start = pl.multiple_of(col * kb, kb)
    own_first = coupling[0, pl.ds(start, kb), :]
    own_second = coupling[1, pl.ds(start, kb), :]
    hots = []
    for i in range(kb):
        da = jnp.abs(own_first[i:i + 1] - first)
        db = jnp.abs(own_second[i:i + 1] - second)
        q = jnp.minimum(da, MX - da) * (mesh_cols // 2 + 1) + jnp.minimum(db, mesh_cols - db)
        hots.append(one_hot(q == lane))
    for i in range(kb):
        coupling[i] = dot(jnp.concatenate([hots[i], hots[i]], axis=1), screen[...], (1, 0))

    landed(dens_slots.at[0:cols - 1], arrivals.at[1])
    density = dens_slots[0]
    for c in range(1, cols):
        density = density + dens_slots[c]
    high, low = split_pair(density * coulomb_ref[...] * (2.0 / (total * nb)))
    partial[...] = (dot(px, high, (1, 1)) + dot(px, low, (1, 1))).reshape(nc, rows, unit, nvec)

    wide_own = wide_ref[1]
    for s in range(nc):
        partial[s, row] = partial[s, row] + wide_own[:, s * nvec:(s + 1) * nvec]

    group = 4
    row_k = (iota((nc * unit, LANES), 0) // nv) % nk
    potentials = []
    for block in range(kb // group):
        def gather(j, sums):
            term = proj[j]
            return tuple(
                sums[u] + coupling[block * group + u, pl.ds(j, 1), :] * term for u in range(group))
        potentials += list(lax.fori_loop(
            0, points, gather, tuple(jnp.zeros((nvec, LANES), F32) for _ in range(group)), unroll=8))
    for r in range(rows):
        mine_pairs = pairs[col].reshape(nc, rows, unit, LANES)[:, r].reshape(nc * unit, LANES)
        left = jnp.concatenate(
            [jnp.where(row_k == k, mine_pairs, 0.0) for k in range(nk)], axis=1).astype(BF16)
        high, low = split_pair(jnp.concatenate([potentials[r * nk + k] for k in range(nk)], axis=1))
        direct = dot(left, high, (1, 1)) + dot(left, low, (1, 1))
        for s in range(nc):
            partial[s, r] = partial[s, r] - direct[s * unit:(s + 1) * unit] * (1.0 / total)

    whole = partial[...]
    packed = jnp.concatenate([whole[s].reshape(per, nvec) for s in range(nc)], axis=1)
    out_send[...] = packed.reshape(rows, unit, LANES)
    start_all(o_copy, rows)
    high, low = split_pair(whole.reshape(batch, nvec))
    gram = dot(own_x, high, (0, 0)) + dot(own_x, low, (0, 0))
    step = nvec // nc
    gram_slots[me] = jnp.concatenate([gram[s * step:(s + 1) * step] for s in range(nc)], axis=1)
    start_all(gram_copy, count)

    out_slots[row] = out_send[row]
    landed(out_slots.at[0:rows - 1], arrivals.at[3])
    applied = jnp.sum(out_slots[...], axis=0)
    landed(gram_slots.at[0:count - 1], arrivals.at[2])
    sums = jnp.sum(gram_slots[...], axis=0) * (1.0 / (total * nb))
    alpha = jnp.concatenate([sums[:, s * nvec:(s + 1) * nvec] for s in range(nc)], axis=0)
    alpha_ref[...] = alpha
    own = wide_ref[0]
    own_rows = jnp.concatenate([own[:, s * nvec:(s + 1) * nvec] for s in range(nc)], axis=0).astype(BF16)
    high, low = split_pair(alpha)
    taken = dot(own_rows, high, (1, 0)) + dot(own_rows, low, (1, 0))
    residual = applied - jnp.concatenate([taken[s * unit:(s + 1) * unit] for s in range(nc)], axis=1)
    for j in range(nv):
        out_ref[:, j * LANES:(j + 1) * LANES] = jnp.concatenate(
            [residual[k * nv + j:k * nv + j + 1] for k in range(nk)], axis=0)

    landed(slots.at[0, 0:rows - 1, 0:28], sends.at[0])
    landed(slots.at[0:cols - 1, :, 0:28], sends.at[1])
    landed(px_slots.at[0:rows - 1], sends.at[2])
    landed(dens_slots.at[0:cols - 1], sends.at[3])
    landed(gram_slots.at[0:count - 1], sends.at[4])
    landed(out_slots.at[0:rows - 1], sends.at[5])


def fast_on_device(pair_exchange, conduction, valence, coulomb, screening, energies, vectors, k_coords):
    nk, nb, planes = pair_exchange.shape
    nv, nc = valence.shape[1], conduction.shape[1]
    nvec = vectors.shape[1] // nb
    rows, cols = lax.axis_size("row"), lax.axis_size("col")
    count = rows * cols
    total = nk * count
    unit = nk * nv
    kb = rows * nk
    batch = kb * nb
    vmem = pl.BlockSpec(memory_space=pltpu.VMEM)
    dma = pltpu.SemaphoreType.DMA
    points = cols * kb
    return pl.pallas_call(
        functools.partial(kernel, (rows, cols, nk, nv, nc, nvec, total, total // MX)),
        out_shape=(
            pltpu.VMEM((nk, nb * nvec), F32),
            pltpu.VMEM((nvec, nvec), F32),
        ),
        in_specs=[pl.BlockSpec(memory_space=pl.ANY)] * 8,
        out_specs=(vmem, vmem),
        scratch_shapes=[
            pltpu.VMEM(pair_exchange.shape, BF16),
            pltpu.VMEM(conduction.shape, BF16),
            pltpu.VMEM(valence.shape, BF16),
            pltpu.VMEM((1, LANES), F32),
            pltpu.VMEM((screening.shape[0], LANES), F32),
            pltpu.VMEM(vectors.shape, BF16),
            pltpu.SMEM(energies.shape, F32),
            pltpu.SMEM(k_coords.shape, jnp.int32),
            pltpu.VMEM((rows, 32, LANES), BF16),
            pltpu.VMEM((2, unit, LANES), F32),
            dma((8,)),
            pltpu.VMEM((cols, rows, 32, LANES), BF16),
            pltpu.VMEM((rows, nk, nb, LANES), BF16),
            pltpu.VMEM((batch, rows * 16), BF16),
            pltpu.VMEM((batch, rows * 16), BF16),
            pltpu.VMEM((LANES, nc * LANES), BF16),
            pltpu.VMEM((batch, kb * nvec), BF16),
            pltpu.VMEM((batch, batch), BF16),
            pltpu.VMEM((2 * points, count * 8), BF16),
            pltpu.VMEM((2 * LANES, LANES), BF16),
            pltpu.VMEM((cols, batch, LANES), BF16),
            pltpu.VMEM((cols, batch, LANES), F32),
            pltpu.VMEM((points, nvec, LANES), F32),
            pltpu.VMEM((cols, rows * 8, LANES), BF16),
            pltpu.VMEM((kb, points, LANES), F32),
            pltpu.VMEM((cols, nvec, LANES), F32),
            pltpu.VMEM((nc, rows, unit, nvec), F32),
            pltpu.VMEM((rows, unit, LANES), F32),
            pltpu.VMEM((rows, unit, LANES), F32),
            pltpu.VMEM((count, nvec // nc, LANES), F32),
            dma((rows,)), dma((cols,)), dma((6,)), dma((4,)),
        ],
        compiler_params=pltpu.CompilerParams(collective_id=0, has_side_effects=True),
    )(pair_exchange, conduction, valence, coulomb.reshape(1, planes), screening, vectors, energies, k_coords)


highest = lax.Precision.HIGHEST


def pair_factors(conduction, valence):
    count, valence_count, plane_count = valence.shape
    joined = (
        valence.astype(jnp.float32)[:, :, None, :] * conduction.astype(jnp.float32)[:, None, :, :]
    )
    return joined.reshape(count, valence_count * conduction.shape[1], plane_count).astype(
        jnp.bfloat16
    )


def transfer_index(rows_at, cols_at, mesh_cols):
    delta_first = jnp.mod(rows_at[:, None, 0] - cols_at[None, :, 0], MX)
    delta_second = jnp.mod(rows_at[:, None, 1] - cols_at[None, :, 1], mesh_cols)
    fold_first = jnp.minimum(delta_first, MX - delta_first)
    fold_second = jnp.minimum(delta_second, mesh_cols - delta_second)
    return (fold_first * (mesh_cols // 2 + 1) + fold_second).astype(jnp.int32)


def on_device(pair_exchange, conduction, valence, coulomb, screening, energies, vectors, k_coords):
    local_count, band_count, plane_count = pair_exchange.shape
    vector_count = vectors.shape[1] // band_count
    row_count = lax.axis_size("row")
    col_count = lax.axis_size("col")
    total_count = local_count * row_count * col_count
    mesh_cols = total_count // MX
    moving = vectors.reshape(local_count, band_count, vector_count)
    partial_density = jnp.einsum(
        "ktg,ktn->gn", pair_exchange, moving, preferred_element_type=jnp.float32
    )
    density = lax.psum(partial_density, ("row", "col"))
    block_size = 128
    sweeps = plane_count // block_size
    col_cond, col_val, col_vec, col_at = (
        lax.all_gather(conduction, "row", axis=0, tiled=True),
        lax.all_gather(valence, "row", axis=0, tiled=True),
        lax.all_gather(vectors, "row", axis=0, tiled=True),
        lax.all_gather(k_coords, "row", axis=0, tiled=True),
    )
    row_cond, row_val, row_at = (
        lax.all_gather(conduction, "col", axis=0, tiled=True),
        lax.all_gather(valence, "col", axis=0, tiled=True),
        lax.all_gather(k_coords, "col", axis=0, tiled=True),
    )
    row_pairs = pair_factors(row_cond, row_val)
    col_pairs = pair_factors(col_cond, col_val)
    indices = transfer_index(row_at, col_at, mesh_cols)
    col_moving = col_vec.reshape(-1, band_count, vector_count)

    def square_sweep(sweep_index, running):
        anchor = sweep_index * block_size
        coupling = jnp.take(
            lax.dynamic_slice_in_dim(screening, anchor, block_size, 1), indices, axis=0
        )
        row_block = lax.dynamic_slice_in_dim(row_pairs, anchor, block_size, 2)
        col_block = lax.dynamic_slice_in_dim(col_pairs, anchor, block_size, 2)
        col_proj = jnp.einsum(
            "ktg,ktn->kng", col_block, col_moving, preferred_element_type=jnp.float32
        )
        potential = jnp.einsum("ijg,jng->ing", coupling, col_proj, precision=highest)
        return running + jnp.einsum(
            "ktg,kng->ktn", row_block.astype(jnp.float32), potential, precision=highest
        )

    forward = lax.fori_loop(
        0,
        sweeps,
        square_sweep,
        jnp.zeros((row_pairs.shape[0], band_count, vector_count), jnp.float32),
    )
    owned = lax.psum_scatter(
        forward.reshape(col_count, local_count, band_count, vector_count),
        "col",
        scatter_dimension=0,
        tiled=True,
    )[0]
    moving_wide = moving.astype(jnp.float32)
    exchange_term = jnp.einsum(
        "ktg,gn->ktn", pair_exchange.astype(jnp.float32) * coulomb, density, precision=highest
    )
    applied = (
        energies[:, :, None] * moving_wide
        + 2.0 / (total_count * band_count) * exchange_term
        - owned / total_count
    )
    gram = jnp.einsum("ktm,ktn->mn", moving_wide, applied, precision=highest)
    alpha = lax.psum(gram, ("row", "col")) / (total_count * band_count)
    residual = applied - jnp.einsum("ktm,mn->ktn", moving_wide, alpha, precision=highest)
    return (residual.reshape(local_count, band_count * vector_count), alpha)


def fits(args, mesh):
    pair_exchange, conduction, valence, _, screening, _, vectors, _ = args
    rows, cols = mesh.shape["row"], mesh.shape["col"]
    points, nb, planes = pair_exchange.shape
    nk = points // (rows * cols)
    nv, nc = valence.shape[1], conduction.shape[1]
    nvec = vectors.shape[1] // nb
    return (
        planes == rows * LANES and nc * nvec == LANES and nk * nv == 8 and nk * (nv + nc) == 16
        and nk == 2 and nvec // nc == 8 and rows % 2 == 0 and cols % 2 == 0 and screening.shape[0] <= LANES
        and points <= LANES
    )


def solution(mesh):
    in_specs = (
        P(("row", "col"), None, None),
        P(("row", "col"), None, None),
        P(("row", "col"), None, None),
        P(),
        P(),
        P(("row", "col"), None),
        P(("row", "col"), None),
        P(("row", "col"), None),
    )
    out_specs = (P(("row", "col"), None), P())

    def run(*args):
        body = fast_on_device if fits(args, mesh) else on_device
        return jax.shard_map(
            body, mesh=mesh, in_specs=in_specs, out_specs=out_specs, check_vma=False
        )(*args)

    return run
```

```python
import functools
import math

import jax
import jax.numpy as jnp
from jax import lax
from jax.experimental import pallas as pl
from jax.experimental.pallas import tpu as pltpu
from jax.sharding import PartitionSpec as P

MX = 32
LANES = 128
MESH = pl.DeviceIdType.MESH
F32 = jnp.float32
BF16 = jnp.bfloat16


def split_pair(value):
    high = value.astype(BF16)
    return high, (value - high.astype(F32)).astype(BF16)


def dot(a, b, contract):
    return lax.dot_general(a, b, ((contract[0:1], contract[1:2]), ((), ())), preferred_element_type=F32)


def iota(shape, axis):
    return lax.broadcasted_iota(jnp.int32, shape, axis)


def one_hot(condition):
    return jnp.where(condition, 1.0, 0.0).astype(BF16)


def wide_dot(a, b, contract):
    high, low = a
    main, rest = b
    return dot(high, main, contract) + dot(low, main, contract) + dot(high, rest, contract)


def swap_blocks(tile, lanes, rows):
    row_bit = (iota(tile.shape, 0) // rows) % 2
    lane_bit = (iota(tile.shape, 1) // lanes) % 2
    up = pltpu.roll(pltpu.roll(tile, lanes, 1), tile.shape[0] - rows, 0)
    down = pltpu.roll(pltpu.roll(tile, LANES - lanes, 1), rows, 0)
    return jnp.where(row_bit == lane_bit, tile, jnp.where(lane_bit == 1, up, down))


def fold_blocks(square, width):
    kept = jnp.where(iota(square.shape, 0) // width == iota(square.shape, 1) // width, square, 0.0)
    rows = kept[0:width]
    for at in range(width, square.shape[0], width):
        rows = rows + kept[at:at + width]
    half = rows + pltpu.roll(rows, LANES // 2, 1)
    return half + pltpu.roll(half, LANES // 4, 1)


def basis(phase, sign):
    angle = (phase % MX).astype(F32) * (2.0 * math.pi / MX)
    return (jnp.cos(angle) + jnp.sin(angle)) * (1 - 2 * (sign % 2)).astype(F32)


def kernel(
    dims, px_hbm, cond_hbm, val_hbm, coulomb_hbm, screening_hbm, vec_hbm, energy_hbm, place_hbm,
    out_ref, alpha_ref,
    px_ref, cond_ref, val_ref, coulomb_ref, screening_ref, vec_ref, energy_ref, place_ref,
    load_sem, msg_ref, slots, px_msg, px_slots, select, select_q, lam, pairs, moved, proj, part, out_send, out_slots, gram_slots,
    sends, arrivals,
):
    rows, cols, nk, nv, nc, nvec, total = dims
    row, col = lax.axis_index("row"), lax.axis_index("col")
    me = row * cols + col
    count = rows * cols
    nb = nv * nc
    width = LANES // cols
    deep = width // 2
    unit = nk * nv
    half = LANES // 2

    depth, core = row // 2, lax.rem(row, 2)
    back, odd = depth // 2, lax.rem(depth, 2)
    layers = [3 * (1 - back), 2 - back, depth + 1 - 2 * odd, depth]
    far_rows = [2 * layer + side for layer in layers for side in (1 - core, core)]
    left = lax.rem(col, 2)
    far_cols = [cols - 1 - col, lax.rem(col + 2, cols), col + 1 - 2 * left, col]
    peers = [(pr, pc) for i, pr in enumerate(far_rows) for j, pc in enumerate(far_cols) if i + j + 2 < rows + cols]
    mixed_peers = [(pr, pc) for j, pc in enumerate(far_cols) for i, pr in enumerate(far_rows) if i + j + 2 < rows + cols]
    ring_rows = [row] + [lax.rem(row + step, rows) for step in range(1, rows)]
    ring_cols = [col] + [lax.rem(col + step, cols) for step in range(1, cols)]
    ring_peers = [(pr, pc) for i, pr in enumerate(ring_rows) for j, pc in enumerate(ring_cols) if i + j]
    ring2_peers = [(pr, pc) for j, pc in enumerate(ring_cols) for i, pr in enumerate(ring_rows) if i + j]
    near_peers = peers[::-1]
    barrier = pltpu.get_barrier_semaphore()
    for peer in peers:
        pl.semaphore_signal(barrier, inc=1, device_id=peer, device_id_type=MESH)

    mine = pl.ds(pl.multiple_of(row * LANES, LANES), LANES)
    loads = [
        pltpu.make_async_copy(src, dst, load_sem.at[at])
        for at, (src, dst) in enumerate((
            (val_hbm, val_ref), (cond_hbm, cond_ref), (vec_hbm, vec_ref), (place_hbm, place_ref), (px_hbm, px_ref),
            (energy_hbm, energy_ref), (screening_hbm.at[:, mine], screening_ref), (coulomb_hbm.at[:, mine], coulomb_ref)))
    ]
    for load in loads:
        load.start()
    row8 = iota((8, LANES), 0)
    lane8 = iota((8, LANES), 1)
    slots[:, 14:16] = jnp.zeros((count, 2, LANES), BF16)
    px_slots[:, 8:16] = jnp.zeros((count, 8, LANES), BF16)
    for load in loads[:4]:
        load.wait()

    vec = vec_ref[...].astype(F32)
    own = jnp.concatenate(
        [vec[k:k + 1, j * LANES:(j + 1) * LANES] for k in range(nk) for j in range(nv)], axis=0)
    tail = jnp.zeros((8, LANES), F32)
    wave = lane8 % half
    for k in range(nk):
        value = basis((wave // 2) * place_ref[k, 0], (wave % 2) * place_ref[k, 1])
        high = value.astype(BF16).astype(F32)
        tail = jnp.where(row8 == 2 * nk + k, jnp.where(lane8 < half, high, value - high), tail)
    for r in range(rows):
        span = slice(r * LANES, (r + 1) * LANES)
        turned = []
        for k in range(nk):
            tile = jnp.concatenate([val_ref[k, :, span].astype(F32), cond_ref[k, :, span].astype(F32)], axis=0)
            for size in (4, 2, 1):
                tile = swap_blocks(tile, deep * size, size)
            turned.append(tile)
        for q in range(cols):
            low = tail
            for k in range(nk):
                shift = (2 * k - 2 * q) % 8
                piece = turned[k] if shift == 0 else pltpu.roll(turned[k], shift, 0)
                low = jnp.where(row8 // 2 == k, piece, low)
            msg_ref[r * cols + q] = jnp.concatenate([own, low], axis=0).astype(BF16)

    pl.semaphore_wait(barrier, count - 1)

    def main_copy(device):
        peer = device[0] * cols + device[1]
        return pltpu.make_async_remote_copy(
            src_ref=msg_ref.at[peer, 0:14], dst_ref=slots.at[me, 0:14],
            send_sem=sends.at[0], recv_sem=arrivals.at[0], device_id=device, device_id_type=MESH)

    def px_copy(device):
        peer = device[0] * cols + device[1]
        return pltpu.make_async_remote_copy(
            src_ref=px_msg.at[peer], dst_ref=px_slots.at[me, 0:8],
            send_sem=sends.at[1], recv_sem=arrivals.at[1], device_id=device, device_id_type=MESH)

    def out_copy(device):
        peer = device[0] * cols + device[1]
        return pltpu.make_async_remote_copy(
            src_ref=out_send.at[peer], dst_ref=out_slots.at[me],
            send_sem=sends.at[2], recv_sem=arrivals.at[2], device_id=device, device_id_type=MESH)

    def gram_copy(device):
        return pltpu.make_async_remote_copy(
            src_ref=gram_slots.at[me], dst_ref=gram_slots.at[me],
            send_sem=sends.at[3], recv_sem=arrivals.at[3], device_id=device, device_id_type=MESH)

    def start_all(copy, targets):
        for peer in targets:
            copy(peer).start()

    def pack(block):
        piece = block[0:8]
        for b in range(1, nc):
            piece = jnp.where(lane8 // nvec == b, block[b * 8:b * 8 + 8], piece)
        return piece

    def landed(ref, sem):
        pltpu.make_async_copy(ref, ref, sem).wait()

    start_all(main_copy, mixed_peers)
    slots[me] = msg_ref[me]

    loads[4].wait()
    at = iota((nk * nb, nk * nb), 0)
    to = iota((nk * nb, nk * nb), 1)
    order = one_hot(to == (at % unit) // nv * nb + at % nv * nc + at // unit)
    arranged = dot(order, px_ref[...].reshape(nk * nb, px_ref.shape[2]), (1, 0))
    for r in range(rows):
        span = slice(r * LANES, (r + 1) * LANES)
        for q in range(cols):
            tile = arranged[q * 8:q * 8 + 8, span]
            for b in range(cols):
                if b != q:
                    moving = pltpu.roll(arranged[b * 8:b * 8 + 8, span], (width * (b - q)) % LANES, 1)
                    tile = jnp.where(lane8 // width == b, moving, tile)
            px_msg[r * cols + q] = tile.astype(BF16)
    start_all(px_copy, mixed_peers)
    px_slots[me, 0:8] = px_msg[me]

    at = iota((count * 16, LANES), 0)
    to = iota((count * 16, LANES), 1)
    same = at // 16 == (to % half) // nk
    place = at % 16
    select[:, 0:LANES] = one_hot(same & (place == 8 + to % nk * 2 + to // half))
    for j in range(nv):
        select[:, (j + 1) * LANES:(j + 2) * LANES] = one_hot(same & (place == to % nk * nv + j))
    at = iota((LANES, count * 16), 0)
    to = iota((LANES, count * 16), 1)
    select_q[...] = one_hot((to // 16 == (at % half) // nk) & (to % 16 == 12 + at % nk))
    for load in loads[5:]:
        load.wait()
    at = iota((LANES, LANES), 0)
    to = iota((LANES, LANES), 1)
    fold = at // 2
    angle = ((fold * ((to % half) // 2)) % MX).astype(F32) * (2.0 * math.pi / MX)
    weight = jnp.where((fold == 0) | (fold == MX // 2), 1.0, 2.0) * (1 - 2 * ((at % 2) * (to % 2))).astype(F32)
    table = jnp.where(fold <= MX // 2, jnp.cos(angle) * weight, 0.0)
    screened = jnp.concatenate(
        [screening_ref[...], jnp.zeros((LANES - screening_ref.shape[0], LANES), F32)], axis=0)
    lam[...] = wide_dot(split_pair(screened), split_pair(table), (0, 0)) * (-1.0 / (total * total))
    band = lam[pl.ds(pl.multiple_of(col * width, 8), width), :]
    spectrum = jnp.where(iota((deep, LANES), 1) < half, band[0:deep], band[deep:width])
    charge = jnp.broadcast_to(coulomb_ref[...], (width, LANES))
    lane_w = iota((width, LANES), 1)
    tiles = jnp.zeros((width, LANES), F32)
    for b in range(cols):
        for q in range(cols):
            moving = charge if b == q else pltpu.roll(charge, (width * (b - q)) % LANES, 1)
            tiles = jnp.where((lane_w // width == b) & (col == q), moving, tiles)
    charge = tiles * (2.0 / (total * nb))
    energy = jnp.zeros((8, LANES), F32)
    for k in range(nk):
        for t in range(nb):
            energy = jnp.where((row8 == k * nv + t // nc) & (lane8 // nvec == t % nc), energy_ref[k, t], energy)

    lifted = energy * own
    high, low = split_pair(lifted)
    own_low = own.astype(BF16)
    base = pack(fold_blocks(dot(own_low, high, (0, 0)) + dot(own_low, low, (0, 0)), nvec))

    landed(slots.at[0:count - 1, 0:14], arrivals.at[0])
    everything = slots[...].reshape(count * 16, LANES)
    spread = dot(everything, select[...], (0, 0))
    for v in range(nv):
        for c in range(nc):
            joined = spread[v * deep:(v + 1) * deep, 0:LANES] * spread[half + c * deep:half + (c + 1) * deep, 0:LANES]
            pairs[v * nc + c] = joined.astype(BF16).astype(F32)
    for t in range(nb):
        moved[t] = spread[t % nc * nvec:(t % nc + 1) * nvec, (t // nc + 1) * LANES:(t // nc + 2) * LANES]
    waves = dot(select_q[...], everything, (1, 0))
    crossed = pltpu.roll(waves, half, 1)
    first = (at < half) & (to < half)
    second = (at >= half) & (to >= half)
    waves = (
        jnp.where(first, waves, jnp.where(second, crossed, 0.0)).astype(BF16),
        jnp.where(first, crossed, jnp.where(second, waves, 0.0)).astype(BF16))

    group = 2
    for first_l in range(0, deep, group):
        sums_l = [None] * group
        for t in range(nb):
            for u in range(group):
                term = pairs[t, first_l + u:first_l + u + 1, :] * moved[t]
                sums_l[u] = term if t == 0 else sums_l[u] + term
        for u in range(group):
            proj[first_l + u] = sums_l[u]
    spectral = wide_dot(split_pair(proj[...].reshape(deep * nvec, LANES)), waves, (1, 0)).reshape(deep, nvec, LANES)
    scaled = spectral * spectrum[:, None, :]
    sides = [
        split_pair(jnp.concatenate([side[l] for l in range(deep)], axis=1)) for side in (spectral, scaled)]
    gram = wide_dot(*sides, (1, 1))

    landed(px_slots.at[0:count - 1, 0:8], arrivals.at[1])
    exchange = px_slots[...].reshape(count * 16, LANES)
    density = fold_blocks(dot(everything, exchange, (0, 0)), nvec)
    charged = density * charge
    gram = gram + wide_dot(split_pair(density), split_pair(charged * (1.0 / cols)), (1, 1))
    gram = jnp.concatenate([gram] * nc, axis=1)
    gram_slots[me] = (base + pack(gram)).astype(BF16)
    start_all(gram_copy, ring_peers)

    proj[...] = wide_dot(
        split_pair(scaled.reshape(deep * nvec, LANES)), waves, (1, 1)).reshape(deep, nvec, LANES)
    lifted_x = jnp.where(
        at // nvec == to // width, jnp.concatenate([charged] * (LANES // nvec), axis=0), 0.0)
    high, low = split_pair(lifted_x)
    whole = dot(exchange, high, (1, 1)) + dot(exchange, low, (1, 1))
    for first_t in range(0, nb, group):
        sums_t = [None] * group
        for l in range(deep):
            for u in range(group):
                term = pairs[first_t + u, l:l + 1, :] * proj[l]
                sums_t[u] = term if l == 0 else sums_t[u] + term
        for u in range(group):
            moved[first_t + u] = sums_t[u]
    placed = jnp.concatenate(
        [jnp.concatenate([moved[j * nc + c] for c in range(nc)], axis=0) for j in range(nv)], axis=1)
    high, low = split_pair(placed)
    chosen = select[:, LANES:]
    whole = whole + dot(chosen, high, (1, 1)) + dot(chosen, low, (1, 1))
    part[...] = whole.reshape(count, 16, LANES)
    out_send[...] = part[:, 0:8].astype(BF16)
    start_all(out_copy, ring_peers)
    out_slots[me] = jnp.zeros((8, LANES), BF16)
    kept = part[me, 0:8] + lifted

    landed(gram_slots.at[0:count - 1], arrivals.at[3])
    sums = jnp.sum(gram_slots[...].astype(F32), axis=0) * (1.0 / (total * nb))
    turns = [sums] + [pltpu.roll(sums, b * nvec, 1) for b in range(1, nc)]
    for b in range(nc):
        alpha_ref[b * 8:b * 8 + 8] = turns[(-b) % nc][:, 0:nvec]
    mixed = jnp.concatenate(
        [jnp.where(lane8 // nvec == q, turns[(q - b) % nc], 0.0) for q in range(nc) for b in range(nc)], axis=0)
    high, low = split_pair(mixed)
    taken = dot(own_low, high, (1, 0)) + dot(own_low, low, (1, 0))

    landed(out_slots.at[0:count - 1], arrivals.at[2])
    residual = kept - taken + jnp.sum(out_slots[...].astype(F32), axis=0)
    for j in range(nv):
        out_ref[:, j * LANES:(j + 1) * LANES] = jnp.concatenate(
            [residual[k * nv + j:k * nv + j + 1] for k in range(nk)], axis=0)

    landed(slots.at[0:count - 1, 0:14], sends.at[0])
    landed(px_slots.at[0:count - 1, 0:8], sends.at[1])
    landed(out_slots.at[0:count - 1], sends.at[2])
    landed(gram_slots.at[0:count - 1], sends.at[3])


def finish(out_ref, alpha_ref, out_hbm, alpha_hbm, sems):
    copies = [
        pltpu.make_async_copy(src, dst, sems.at[at])
        for at, (src, dst) in enumerate(((out_ref, out_hbm), (alpha_ref, alpha_hbm)))]
    for copy in copies:
        copy.start()
    for copy in copies:
        copy.wait()


def fast_on_device(pair_exchange, conduction, valence, coulomb, screening, energies, vectors, k_coords):
    nk, nb, planes = pair_exchange.shape
    nv, nc = valence.shape[1], conduction.shape[1]
    nvec = vectors.shape[1] // nb
    rows, cols = lax.axis_size("row"), lax.axis_size("col")
    count = rows * cols
    total = nk * count
    deep = LANES // cols // 2
    vmem = pl.BlockSpec(memory_space=pltpu.VMEM)
    dma = pltpu.SemaphoreType.DMA
    results = pl.pallas_call(
        functools.partial(kernel, (rows, cols, nk, nv, nc, nvec, total)),
        out_shape=(
            pltpu.VMEM((nk, nb * nvec), F32),
            pltpu.VMEM((nvec, nvec), F32),
        ),
        in_specs=[pl.BlockSpec(memory_space=pl.ANY)] * 8,
        out_specs=(vmem, vmem),
        scratch_shapes=[
            pltpu.VMEM(pair_exchange.shape, BF16),
            pltpu.VMEM(conduction.shape, BF16),
            pltpu.VMEM(valence.shape, BF16),
            pltpu.VMEM((1, LANES), F32),
            pltpu.VMEM((screening.shape[0], LANES), F32),
            pltpu.VMEM(vectors.shape, BF16),
            pltpu.SMEM(energies.shape, F32),
            pltpu.SMEM(k_coords.shape, jnp.int32),
            dma((8,)),
            pltpu.VMEM((count, 16, LANES), BF16),
            pltpu.VMEM((count, 16, LANES), BF16),
            pltpu.VMEM((count, 8, LANES), BF16),
            pltpu.VMEM((count, 16, LANES), BF16),
            pltpu.VMEM((count * 16, (1 + nv) * LANES), BF16),
            pltpu.VMEM((LANES, count * 16), BF16),
            pltpu.VMEM((LANES, LANES), F32),
            pltpu.VMEM((nb, deep, LANES), F32),
            pltpu.VMEM((nb, nvec, LANES), F32),
            pltpu.VMEM((deep, nvec, LANES), F32),
            pltpu.VMEM((count, 16, LANES), F32),
            pltpu.VMEM((count, 8, LANES), BF16),
            pltpu.VMEM((count, 8, LANES), BF16),
            pltpu.VMEM((count, 8, LANES), BF16),
            dma((4,)), dma((4,)),
        ],
        compiler_params=pltpu.CompilerParams(collective_id=0, has_side_effects=True),
    )(pair_exchange, conduction, valence, coulomb.reshape(1, planes), screening, vectors, energies, k_coords)
    return pl.pallas_call(
        finish,
        out_shape=(jax.ShapeDtypeStruct((nk, nb * nvec), F32), jax.ShapeDtypeStruct((nvec, nvec), F32)),
        in_specs=[vmem, vmem],
        out_specs=(pl.BlockSpec(memory_space=pl.ANY), pl.BlockSpec(memory_space=pl.ANY)),
        scratch_shapes=[dma((2,))],
    )(*[pltpu.with_memory_space_constraint(result, pltpu.VMEM) for result in results])


highest = lax.Precision.HIGHEST


def pair_factors(conduction, valence):
    count, valence_count, plane_count = valence.shape
    joined = (
        valence.astype(jnp.float32)[:, :, None, :] * conduction.astype(jnp.float32)[:, None, :, :]
    )
    return joined.reshape(count, valence_count * conduction.shape[1], plane_count).astype(
        jnp.bfloat16
    )


def transfer_index(rows_at, cols_at, mesh_cols):
    delta_first = jnp.mod(rows_at[:, None, 0] - cols_at[None, :, 0], MX)
    delta_second = jnp.mod(rows_at[:, None, 1] - cols_at[None, :, 1], mesh_cols)
    fold_first = jnp.minimum(delta_first, MX - delta_first)
    fold_second = jnp.minimum(delta_second, mesh_cols - delta_second)
    return (fold_first * (mesh_cols // 2 + 1) + fold_second).astype(jnp.int32)


def on_device(pair_exchange, conduction, valence, coulomb, screening, energies, vectors, k_coords):
    local_count, band_count, plane_count = pair_exchange.shape
    vector_count = vectors.shape[1] // band_count
    row_count = lax.axis_size("row")
    col_count = lax.axis_size("col")
    total_count = local_count * row_count * col_count
    mesh_cols = total_count // MX
    moving = vectors.reshape(local_count, band_count, vector_count)
    partial_density = jnp.einsum(
        "ktg,ktn->gn", pair_exchange, moving, preferred_element_type=jnp.float32
    )
    density = lax.psum(partial_density, ("row", "col"))
    block_size = 128
    sweeps = plane_count // block_size
    col_cond, col_val, col_vec, col_at = (
        lax.all_gather(conduction, "row", axis=0, tiled=True),
        lax.all_gather(valence, "row", axis=0, tiled=True),
        lax.all_gather(vectors, "row", axis=0, tiled=True),
        lax.all_gather(k_coords, "row", axis=0, tiled=True),
    )
    row_cond, row_val, row_at = (
        lax.all_gather(conduction, "col", axis=0, tiled=True),
        lax.all_gather(valence, "col", axis=0, tiled=True),
        lax.all_gather(k_coords, "col", axis=0, tiled=True),
    )
    row_pairs = pair_factors(row_cond, row_val)
    col_pairs = pair_factors(col_cond, col_val)
    indices = transfer_index(row_at, col_at, mesh_cols)
    col_moving = col_vec.reshape(-1, band_count, vector_count)

    def square_sweep(sweep_index, running):
        anchor = sweep_index * block_size
        coupling = jnp.take(
            lax.dynamic_slice_in_dim(screening, anchor, block_size, 1), indices, axis=0
        )
        row_block = lax.dynamic_slice_in_dim(row_pairs, anchor, block_size, 2)
        col_block = lax.dynamic_slice_in_dim(col_pairs, anchor, block_size, 2)
        col_proj = jnp.einsum(
            "ktg,ktn->kng", col_block, col_moving, preferred_element_type=jnp.float32
        )
        potential = jnp.einsum("ijg,jng->ing", coupling, col_proj, precision=highest)
        return running + jnp.einsum(
            "ktg,kng->ktn", row_block.astype(jnp.float32), potential, precision=highest
        )

    forward = lax.fori_loop(
        0,
        sweeps,
        square_sweep,
        jnp.zeros((row_pairs.shape[0], band_count, vector_count), jnp.float32),
    )
    owned = lax.psum_scatter(
        forward.reshape(col_count, local_count, band_count, vector_count),
        "col",
        scatter_dimension=0,
        tiled=True,
    )[0]
    moving_wide = moving.astype(jnp.float32)
    exchange_term = jnp.einsum(
        "ktg,gn->ktn", pair_exchange.astype(jnp.float32) * coulomb, density, precision=highest
    )
    applied = (
        energies[:, :, None] * moving_wide
        + 2.0 / (total_count * band_count) * exchange_term
        - owned / total_count
    )
    gram = jnp.einsum("ktm,ktn->mn", moving_wide, applied, precision=highest)
    alpha = lax.psum(gram, ("row", "col")) / (total_count * band_count)
    residual = applied - jnp.einsum("ktm,mn->ktn", moving_wide, alpha, precision=highest)
    return (residual.reshape(local_count, band_count * vector_count), alpha)


def fits(args, mesh):
    pair_exchange, conduction, valence, _, screening, _, vectors, _ = args
    rows, cols = mesh.shape["row"], mesh.shape["col"]
    points, nb, planes = pair_exchange.shape
    nk = points // (rows * cols)
    nv, nc = valence.shape[1], conduction.shape[1]
    nvec = vectors.shape[1] // nb
    return (
        planes == rows * LANES and rows == 8 and cols == 4 and rows * cols * nk * 2 == LANES and nk == 2 and nv == 4 and nc == 4
        and nc * nvec == LANES and points == 2 * MX and screening.shape[0] == MX + 2
    )


def solution(mesh):
    in_specs = (
        P(("row", "col"), None, None),
        P(("row", "col"), None, None),
        P(("row", "col"), None, None),
        P(),
        P(),
        P(("row", "col"), None),
        P(("row", "col"), None),
        P(("row", "col"), None),
    )
    out_specs = (P(("row", "col"), None), P())

    def run(*args):
        body = fast_on_device if fits(args, mesh) else on_device
        return jax.shard_map(
            body, mesh=mesh, in_specs=in_specs, out_specs=out_specs, check_vma=False
        )(*args)

    return run
```

```python
import functools
import math

import jax
import jax.numpy as jnp
from jax import lax
from jax.experimental import pallas as pl
from jax.experimental.pallas import tpu as pltpu
from jax.sharding import PartitionSpec as P

MX = 32
LANES = 128
MESH = pl.DeviceIdType.MESH
F32 = jnp.float32
BF16 = jnp.bfloat16


def split_pair(value):
    high = value.astype(BF16)
    return high, (value - high.astype(F32)).astype(BF16)


def dot(a, b, contract):
    return lax.dot_general(a, b, ((contract[0:1], contract[1:2]), ((), ())), preferred_element_type=F32)


def iota(shape, axis):
    return lax.broadcasted_iota(jnp.int32, shape, axis)


def one_hot(condition):
    return jnp.where(condition, 1.0, 0.0).astype(BF16)


def wide_dot(a, b, contract):
    high, low = a
    main, rest = b
    return dot(high, main, contract) + dot(low, main, contract) + dot(high, rest, contract)


def beside(*parts):
    return jnp.concatenate(parts, axis=1)


def above(*parts):
    return jnp.concatenate(parts, axis=0)


def swap_blocks(tile, lanes, rows):
    row_bit = (iota(tile.shape, 0) // rows) % 2
    lane_bit = (iota(tile.shape, 1) // lanes) % 2
    up = pltpu.roll(pltpu.roll(tile, lanes, 1), tile.shape[0] - rows, 0)
    down = pltpu.roll(pltpu.roll(tile, LANES - lanes, 1), rows, 0)
    return jnp.where(row_bit == lane_bit, tile, jnp.where(lane_bit == 1, up, down))


def fold_blocks(square, width):
    kept = jnp.where(iota(square.shape, 0) // width == iota(square.shape, 1) // width, square, 0.0)
    rows = kept[0:width]
    for at in range(width, square.shape[0], width):
        rows = rows + kept[at:at + width]
    half = rows + pltpu.roll(rows, LANES // 2, 1)
    return half + pltpu.roll(half, LANES // 4, 1)


def basis(phase, sign):
    angle = (phase % MX).astype(F32) * (2.0 * math.pi / MX)
    return (jnp.cos(angle) + jnp.sin(angle)) * (1 - 2 * (sign % 2)).astype(F32)


def kernel(
    dims, px_hbm, cond_hbm, val_hbm, coulomb_hbm, screening_hbm, vec_hbm, energy_hbm, place_hbm,
    out_ref, alpha_ref,
    px_ref, cond_ref, val_ref, coulomb_ref, screening_ref, vec_ref, energy_ref, place_ref,
    load_sem, msg_ref, slots, px_msg, px_slots, select, select_q, lam, pairs, moved, proj, out_send, out_slots, gram_slots,
    base_send, base_slot, sends, arrivals,
):
    rows, cols, nk, nv, nc, nvec, total = dims
    row, col = lax.axis_index("row"), lax.axis_index("col")
    me = row * cols + col
    count = rows * cols
    nb = nv * nc
    low_row, high_row = rows // 4, rows - rows // 4
    hosts = (high_row - low_row) * cols
    host = (row >= low_row) & (row < high_row)
    guest = jnp.logical_not(host)
    near_row = jnp.where(row < low_row, row + low_row, jnp.where(row >= high_row, row - low_row, row))
    seat = (near_row - low_row) * cols + col
    width = LANES // cols
    deep = width // 2
    unit = nk * nv
    half = LANES // 2
    sheets = count * 8
    spans = rows * LANES // hosts // width
    levels = spans * deep

    ring_rows = [row] + [lax.rem(row + step, rows) for step in range(1, rows)]
    ring_cols = [col] + [lax.rem(col + step, cols) for step in range(1, cols)]
    everyone = [(pr, pc) for i, pr in enumerate(ring_rows) for j, pc in enumerate(ring_cols) if i + j]
    host_rows = [low_row + lax.rem(near_row - low_row + step, high_row - low_row) for step in range(high_row - low_row)]
    left = lax.rem(col, 2)
    host_cols = [cols - 1 - col, lax.rem(col + 2, cols), col + 1 - 2 * left, col]
    host_peers = [(pr, pc) for pc in host_cols for pr in host_rows[::-1]]

    barrier = pltpu.get_barrier_semaphore()
    mine = pl.ds(pl.multiple_of(seat // 2 * LANES, LANES), LANES)
    loads = [
        pltpu.make_async_copy(src, dst, load_sem.at[at])
        for at, (src, dst) in enumerate((
            (val_hbm, val_ref), (cond_hbm, cond_ref), (vec_hbm, vec_ref), (place_hbm, place_ref), (px_hbm, px_ref),
            (energy_hbm, energy_ref), (screening_hbm.at[:, mine], screening_ref), (coulomb_hbm.at[:, mine], coulomb_ref)))
    ]
    for load in loads[:4]:
        load.start()

    @pl.when(host)
    def _():
        for peer in everyone:
            pl.semaphore_signal(barrier, inc=1, device_id=peer, device_id_type=MESH)

    for load in loads[4:]:
        load.start()
    row8 = iota((8, LANES), 0)
    lane8 = iota((8, LANES), 1)
    for load in loads[:4]:
        load.wait()

    vec = vec_ref[...].astype(F32)
    own = jnp.concatenate(
        [vec[k:k + 1, j * LANES:(j + 1) * LANES] for k in range(nk) for j in range(nv)], axis=0)
    tail = jnp.zeros((8, LANES), F32)
    wave = lane8 % half
    for k in range(nk):
        value = basis((wave // 2) * place_ref[k, 0], (wave % 2) * place_ref[k, 1])
        high = value.astype(BF16).astype(F32)
        tail = jnp.where(row8 == k, jnp.where(lane8 < half, high, value - high), tail)
    tail = above(tail, jnp.zeros((8, LANES), F32)).astype(BF16)
    for r in range(rows):
        span = slice(r * LANES, (r + 1) * LANES)
        turned = []
        for k in range(nk):
            tile = above(val_ref[k, :, span].astype(F32), cond_ref[k, :, span].astype(F32))
            for size in (4, 2, 1):
                tile = swap_blocks(tile, deep * size, size)
            turned.append(tile)
        flipped = [pltpu.roll(tile, 4, 0) for tile in turned]
        first_half = jnp.where(row8 < 4, turned[0], flipped[1])
        other_half = jnp.where(row8 < 4, flipped[0], turned[1])
        for q, low in enumerate((first_half, other_half)):
            msg_ref[r * 2 + q, 0:16] = above(own, low).astype(BF16)
            msg_ref[r * 2 + q, 16:32] = tail

    @pl.when(host)
    def _():
        pl.semaphore_wait(barrier, hosts - 1)

    @pl.when(guest)
    def _():
        pl.semaphore_wait(barrier, hosts)

    def main_copy(device):
        peer = (device[0] - low_row) * cols + device[1]
        return pltpu.make_async_remote_copy(
            src_ref=msg_ref.at[peer, 0:18], dst_ref=slots.at[me, 0:18],
            send_sem=sends.at[0], recv_sem=arrivals.at[0], device_id=device, device_id_type=MESH)

    def px_copy(device):
        peer = (device[0] - low_row) * cols + device[1]
        return pltpu.make_async_remote_copy(
            src_ref=px_msg.at[peer], dst_ref=px_slots.at[me],
            send_sem=sends.at[1], recv_sem=arrivals.at[1], device_id=device, device_id_type=MESH)

    def out_copy(device):
        peer = device[0] * cols + device[1]
        return pltpu.make_async_remote_copy(
            src_ref=out_send.at[peer], dst_ref=out_slots.at[seat],
            send_sem=sends.at[2], recv_sem=arrivals.at[2], device_id=device, device_id_type=MESH)

    def gram_copy(device):
        return pltpu.make_async_remote_copy(
            src_ref=gram_slots.at[seat], dst_ref=gram_slots.at[seat],
            send_sem=sends.at[3], recv_sem=arrivals.at[3], device_id=device, device_id_type=MESH)

    def base_copy():
        return pltpu.make_async_remote_copy(
            src_ref=base_send, dst_ref=base_slot,
            send_sem=sends.at[4], recv_sem=arrivals.at[4], device_id=(near_row, col), device_id_type=MESH)

    def start_all(copy, targets):
        for peer in targets:
            copy(peer).start()

    def pack(block):
        piece = block[0:8]
        for b in range(1, nc):
            piece = jnp.where(lane8 // nvec == b, block[b * 8:b * 8 + 8], piece)
        return piece

    def landed(ref, sem):
        pltpu.make_async_copy(ref, ref, sem).wait()

    def to_hosts(copy, here, there):
        start_all(copy, host_peers[:-1])

        @pl.when(guest)
        def _():
            copy(host_peers[-1]).start()

        @pl.when(host)
        def _():
            there[me] = here[seat]

    to_hosts(main_copy, msg_ref, slots)

    loads[4].wait()
    at = iota((nk * nb, nk * nb), 0)
    to = iota((nk * nb, nk * nb), 1)
    order = one_hot(to == (at % unit) // nv * nb + at % nv * nc + at // unit)
    arranged = dot(order, px_ref[...].reshape(nk * nb, px_ref.shape[2]), (1, 0))
    for r in range(rows):
        span = slice(r * LANES, (r + 1) * LANES)
        tiles = []
        for q in range(cols):
            tile = arranged[q * 8:q * 8 + 8, span]
            for b in range(cols):
                if b != q:
                    moving = pltpu.roll(arranged[b * 8:b * 8 + 8, span], (width * (b - q)) % LANES, 1)
                    tile = jnp.where(lane8 // width == b, moving, tile)
            tiles.append(tile)
        for q in range(2):
            px_msg[r * 2 + q] = above(tiles[2 * q], tiles[2 * q + 1]).astype(BF16)
    to_hosts(px_copy, px_msg, px_slots)

    loads[5].wait()
    energy = jnp.zeros((8, LANES), F32)
    for k in range(nk):
        for t in range(nb):
            energy = jnp.where((row8 == k * nv + t // nc) & (lane8 // nvec == t % nc), energy_ref[k, t], energy)
    lifted = energy * own
    high, low = split_pair(lifted)
    own_low = own.astype(BF16)
    base_send[...] = pack(fold_blocks(dot(own_low, high, (0, 0)) + dot(own_low, low, (0, 0)), nvec))

    @pl.when(guest)
    def _():
        base_copy().start()

    for load in loads[6:]:
        load.wait()

    @pl.when(host)
    def _():
        at = iota((sheets, LANES), 0)
        to = iota((sheets, LANES), 1)
        same = at // 8 == (to % half) // nk
        place = at % 8
        for j in range(nv):
            select[:, j * LANES:(j + 1) * LANES] = one_hot(same & (place == to % nk * nv + j))
        for a in range(spans):
            select[:, (nv + a) * LANES:(nv + a + 1) * LANES] = one_hot(
                same & (place == to % nk * 2 * spans + 2 * a + to // half))
        at = iota((LANES, sheets), 0)
        to = iota((LANES, sheets), 1)
        select_q[...] = one_hot((to // 8 == (at % half) // nk) & (to % 8 == at % nk))
        at = iota((LANES, LANES), 0)
        to = iota((LANES, LANES), 1)
        fold = at // 2
        angle = ((fold * ((to % half) // 2)) % MX).astype(F32) * (2.0 * math.pi / MX)
        weight = jnp.where((fold == 0) | (fold == MX // 2), 1.0, 2.0) * (1 - 2 * ((at % 2) * (to % 2))).astype(F32)
        table = jnp.where(fold <= MX // 2, jnp.cos(angle) * weight, 0.0)
        screened = above(screening_ref[...], jnp.zeros((LANES - screening_ref.shape[0], LANES), F32))
        lam[...] = wide_dot(split_pair(screened), split_pair(table), (0, 0)) * (-1.0 / (total * total))
        second_half = lax.rem(seat, 2)
        band = lam[pl.ds(pl.multiple_of(second_half * half, 8), half), :]
        lane_d = iota((deep, LANES), 1)
        spectrum = above(*[
            jnp.where(lane_d < half, band[2 * a * deep:(2 * a + 1) * deep], band[(2 * a + 1) * deep:(2 * a + 2) * deep])
            for a in range(spans)])
        raw = jnp.broadcast_to(coulomb_ref[...], (width, LANES)) * (2.0 / (total * nb))
        lane_w = iota((width, LANES), 1)
        charges = []
        for a in range(spans):
            tiles = jnp.zeros((width, LANES), F32)
            for b in range(cols):
                for q in range(2):
                    shift = (width * (b - 2 * q - a)) % LANES
                    moving = raw if shift == 0 else pltpu.roll(raw, shift, 1)
                    tiles = jnp.where((lane_w // width == b) & (second_half == q), moving, tiles)
            charges.append(tiles)

        landed(slots.at[0:count - 1, 0:18], arrivals.at[0])
        got = slots[...].astype(F32)
        own_all, rest_all, wave_all = [
            got[:, 8 * part:8 * part + 8].reshape(sheets, LANES) for part in range(3)]
        own_all, rest_all = own_all.astype(BF16), rest_all.astype(BF16)
        wave_all = jnp.where(iota((sheets, LANES), 0) % 8 < nk, wave_all, 0.0).astype(BF16)
        factors = dot(rest_all, select[:, nv * LANES:], (0, 0))
        spread = dot(own_all, select[:, 0:nv * LANES], (0, 0))
        for v in range(nv):
            for c in range(nc):
                for a in range(spans):
                    lanes = slice(a * LANES, (a + 1) * LANES)
                    joined = (
                        factors[v * deep:(v + 1) * deep, lanes] * factors[half + c * deep:half + (c + 1) * deep, lanes])
                    pairs[v * nc + c, a * deep:(a + 1) * deep] = joined.astype(BF16).astype(F32)
        for t in range(nb):
            moved[t] = spread[t % nc * nvec:(t % nc + 1) * nvec, t // nc * LANES:(t // nc + 1) * LANES]
        waves = dot(select_q[...], wave_all, (1, 0))
        crossed = pltpu.roll(waves, half, 1)
        first = (at < half) & (to < half)
        second = (at >= half) & (to >= half)
        main = jnp.where(first, waves, jnp.where(second, crossed, 0.0)).astype(BF16)
        fine = jnp.where(first, crossed, jnp.where(second, waves, 0.0)).astype(BF16)
        none = jnp.zeros((LANES, LANES), BF16)
        ahead = above(beside(main, fine), beside(main, none))
        astern = above(beside(main, main), beside(fine, none))

        def through(values, weights, contract):
            both = dot(beside(*split_pair(values)), weights, contract)
            return both[:, 0:LANES] + both[:, LANES:]

        group = 2
        for first_l in range(0, levels, group):
            sums_l = [None] * group
            for t in range(nb):
                for u in range(group):
                    term = pairs[t, first_l + u:first_l + u + 1, :] * moved[t]
                    sums_l[u] = term if t == 0 else sums_l[u] + term
            for u in range(group):
                proj[first_l + u] = sums_l[u]
        spectral = through(proj[...].reshape(levels * nvec, LANES), ahead, (1, 0)).reshape(levels, nvec, LANES)
        scaled = spectral * spectrum[:, None, :]
        sides = [
            split_pair(jnp.concatenate([side[l] for l in range(levels)], axis=1)) for side in (spectral, scaled)]
        gram = wide_dot(*sides, (1, 1))

        landed(px_slots.at[0:count - 1], arrivals.at[1])
        taken_px = px_slots[...].astype(F32)
        exchange = beside(*[
            taken_px[:, 8 * a:8 * a + 8].reshape(sheets, LANES).astype(BF16) for a in range(spans)])
        crowd = dot(own_all, exchange, (0, 0))
        densities = [fold_blocks(crowd[:, a * LANES:(a + 1) * LANES], nvec) for a in range(spans)]
        charged = [density * charge for density, charge in zip(densities, charges)]
        gram = gram + wide_dot(
            split_pair(beside(*densities)), split_pair(beside(*charged) * (1.0 / cols)), (1, 1))
        landed(base_slot, arrivals.at[4])
        gram_slots[seat] = (
            base_send[...] + base_slot[...] + pack(jnp.concatenate([gram] * nc, axis=1))).astype(BF16)
        start_all(gram_copy, everyone)

        proj[...] = through(scaled.reshape(levels * nvec, LANES), astern, (1, 1)).reshape(levels, nvec, LANES)
        blocks = beside(*[
            jnp.where(at // nvec == to // width, jnp.concatenate([charge] * (LANES // nvec), axis=0), 0.0)
            for charge in charged])
        whole = dot(exchange, above(*split_pair(blocks)), (1, 1))
        for first_t in range(0, nb, group):
            sums_t = [None] * group
            for l in range(levels):
                for u in range(group):
                    term = pairs[first_t + u, l:l + 1, :] * proj[l]
                    sums_t[u] = term if l == 0 else sums_t[u] + term
            for u in range(group):
                moved[first_t + u] = sums_t[u]
        placed = jnp.concatenate(
            [jnp.concatenate([moved[j * nc + c] for c in range(nc)], axis=0) for j in range(nv)], axis=1)
        whole = whole + dot(select[:, 0:nv * LANES], above(*split_pair(placed)), (1, 1))
        whole = whole[:, 0:LANES] + whole[:, LANES:]
        out_send[...] = whole.astype(BF16).reshape(count, 8, LANES)
        start_all(out_copy, everyone)
        out_slots[seat] = out_send[me]

    def each(run):
        @pl.when(host)
        def _():
            run(hosts - 1)

        @pl.when(guest)
        def _():
            run(hosts)

    each(lambda n: landed(gram_slots.at[0:n], arrivals.at[3]))
    sums = jnp.sum(gram_slots[...].astype(F32), axis=0) * (1.0 / (total * nb))
    turns = [sums] + [pltpu.roll(sums, b * nvec, 1) for b in range(1, nc)]
    for b in range(nc):
        alpha_ref[b * 8:b * 8 + 8] = turns[(-b) % nc][:, 0:nvec]
    mixed = jnp.concatenate(
        [jnp.where(lane8 // nvec == q, turns[(q - b) % nc], 0.0) for q in range(nc) for b in range(nc)], axis=0)
    high, low = split_pair(mixed)
    rest = lifted - dot(own_low, high, (1, 0)) - dot(own_low, low, (1, 0))

    each(lambda n: landed(out_slots.at[0:n], arrivals.at[2]))
    residual = rest + jnp.sum(out_slots[...].astype(F32), axis=0)
    for j in range(nv):
        out_ref[:, j * LANES:(j + 1) * LANES] = jnp.concatenate(
            [residual[k * nv + j:k * nv + j + 1] for k in range(nk)], axis=0)

    def drain(n):
        landed(slots.at[0:n, 0:18], sends.at[0])
        landed(px_slots.at[0:n], sends.at[1])

    each(drain)

    @pl.when(guest)
    def _():
        landed(base_slot, sends.at[4])

    @pl.when(host)
    def _():
        landed(out_send.at[0:count - 1], sends.at[2])
        landed(out_send.at[0:count - 1], sends.at[3])


def finish(out_ref, alpha_ref, out_hbm, alpha_hbm, sems):
    copies = [
        pltpu.make_async_copy(src, dst, sems.at[at])
        for at, (src, dst) in enumerate(((out_ref, out_hbm), (alpha_ref, alpha_hbm)))]
    for copy in copies:
        copy.start()
    for copy in copies:
        copy.wait()


def fast_on_device(pair_exchange, conduction, valence, coulomb, screening, energies, vectors, k_coords):
    nk, nb, planes = pair_exchange.shape
    nv, nc = valence.shape[1], conduction.shape[1]
    nvec = vectors.shape[1] // nb
    rows, cols = lax.axis_size("row"), lax.axis_size("col")
    count = rows * cols
    total = nk * count
    hosts = count // 2
    width = LANES // cols
    spans = planes // hosts // width
    levels = spans * width // 2
    vmem = pl.BlockSpec(memory_space=pltpu.VMEM)
    dma = pltpu.SemaphoreType.DMA
    results = pl.pallas_call(
        functools.partial(kernel, (rows, cols, nk, nv, nc, nvec, total)),
        out_shape=(
            pltpu.VMEM((nk, nb * nvec), F32),
            pltpu.VMEM((nvec, nvec), F32),
        ),
        in_specs=[pl.BlockSpec(memory_space=pl.ANY)] * 8,
        out_specs=(vmem, vmem),
        scratch_shapes=[
            pltpu.VMEM(pair_exchange.shape, BF16),
            pltpu.VMEM(conduction.shape, BF16),
            pltpu.VMEM(valence.shape, BF16),
            pltpu.VMEM((1, LANES), F32),
            pltpu.VMEM((screening.shape[0], LANES), F32),
            pltpu.VMEM(vectors.shape, BF16),
            pltpu.SMEM(energies.shape, F32),
            pltpu.SMEM(k_coords.shape, jnp.int32),
            dma((8,)),
            pltpu.VMEM((hosts, 32, LANES), BF16),
            pltpu.VMEM((count, 32, LANES), BF16),
            pltpu.VMEM((hosts, 16, LANES), BF16),
            pltpu.VMEM((count, 16, LANES), BF16),
            pltpu.VMEM((count * 8, (nv + spans) * LANES), BF16),
            pltpu.VMEM((LANES, count * 8), BF16),
            pltpu.VMEM((LANES, LANES), F32),
            pltpu.VMEM((nb, levels, LANES), F32),
            pltpu.VMEM((nb, nvec, LANES), F32),
            pltpu.VMEM((levels, nvec, LANES), F32),
            pltpu.VMEM((count, 8, LANES), BF16),
            pltpu.VMEM((hosts, 8, LANES), BF16),
            pltpu.VMEM((hosts, 8, LANES), BF16),
            pltpu.VMEM((8, LANES), F32),
            pltpu.VMEM((8, LANES), F32),
            dma((5,)), dma((5,)),
        ],
        compiler_params=pltpu.CompilerParams(collective_id=0, has_side_effects=True),
    )(pair_exchange, conduction, valence, coulomb.reshape(1, planes), screening, vectors, energies, k_coords)
    return pl.pallas_call(
        finish,
        out_shape=(jax.ShapeDtypeStruct((nk, nb * nvec), F32), jax.ShapeDtypeStruct((nvec, nvec), F32)),
        in_specs=[vmem, vmem],
        out_specs=(pl.BlockSpec(memory_space=pl.ANY), pl.BlockSpec(memory_space=pl.ANY)),
        scratch_shapes=[dma((2,))],
    )(*[pltpu.with_memory_space_constraint(result, pltpu.VMEM) for result in results])


highest = lax.Precision.HIGHEST


def pair_factors(conduction, valence):
    count, valence_count, plane_count = valence.shape
    joined = (
        valence.astype(jnp.float32)[:, :, None, :] * conduction.astype(jnp.float32)[:, None, :, :]
    )
    return joined.reshape(count, valence_count * conduction.shape[1], plane_count).astype(
        jnp.bfloat16
    )


def transfer_index(rows_at, cols_at, mesh_cols):
    delta_first = jnp.mod(rows_at[:, None, 0] - cols_at[None, :, 0], MX)
    delta_second = jnp.mod(rows_at[:, None, 1] - cols_at[None, :, 1], mesh_cols)
    fold_first = jnp.minimum(delta_first, MX - delta_first)
    fold_second = jnp.minimum(delta_second, mesh_cols - delta_second)
    return (fold_first * (mesh_cols // 2 + 1) + fold_second).astype(jnp.int32)


def on_device(pair_exchange, conduction, valence, coulomb, screening, energies, vectors, k_coords):
    local_count, band_count, plane_count = pair_exchange.shape
    vector_count = vectors.shape[1] // band_count
    row_count = lax.axis_size("row")
    col_count = lax.axis_size("col")
    total_count = local_count * row_count * col_count
    mesh_cols = total_count // MX
    moving = vectors.reshape(local_count, band_count, vector_count)
    partial_density = jnp.einsum(
        "ktg,ktn->gn", pair_exchange, moving, preferred_element_type=jnp.float32
    )
    density = lax.psum(partial_density, ("row", "col"))
    block_size = 128
    sweeps = plane_count // block_size
    col_cond, col_val, col_vec, col_at = (
        lax.all_gather(conduction, "row", axis=0, tiled=True),
        lax.all_gather(valence, "row", axis=0, tiled=True),
        lax.all_gather(vectors, "row", axis=0, tiled=True),
        lax.all_gather(k_coords, "row", axis=0, tiled=True),
    )
    row_cond, row_val, row_at = (
        lax.all_gather(conduction, "col", axis=0, tiled=True),
        lax.all_gather(valence, "col", axis=0, tiled=True),
        lax.all_gather(k_coords, "col", axis=0, tiled=True),
    )
    row_pairs = pair_factors(row_cond, row_val)
    col_pairs = pair_factors(col_cond, col_val)
    indices = transfer_index(row_at, col_at, mesh_cols)
    col_moving = col_vec.reshape(-1, band_count, vector_count)

    def square_sweep(sweep_index, running):
        anchor = sweep_index * block_size
        coupling = jnp.take(
            lax.dynamic_slice_in_dim(screening, anchor, block_size, 1), indices, axis=0
        )
        row_block = lax.dynamic_slice_in_dim(row_pairs, anchor, block_size, 2)
        col_block = lax.dynamic_slice_in_dim(col_pairs, anchor, block_size, 2)
        col_proj = jnp.einsum(
            "ktg,ktn->kng", col_block, col_moving, preferred_element_type=jnp.float32
        )
        potential = jnp.einsum("ijg,jng->ing", coupling, col_proj, precision=highest)
        return running + jnp.einsum(
            "ktg,kng->ktn", row_block.astype(jnp.float32), potential, precision=highest
        )

    forward = lax.fori_loop(
        0,
        sweeps,
        square_sweep,
        jnp.zeros((row_pairs.shape[0], band_count, vector_count), jnp.float32),
    )
    owned = lax.psum_scatter(
        forward.reshape(col_count, local_count, band_count, vector_count),
        "col",
        scatter_dimension=0,
        tiled=True,
    )[0]
    moving_wide = moving.astype(jnp.float32)
    exchange_term = jnp.einsum(
        "ktg,gn->ktn", pair_exchange.astype(jnp.float32) * coulomb, density, precision=highest
    )
    applied = (
        energies[:, :, None] * moving_wide
        + 2.0 / (total_count * band_count) * exchange_term
        - owned / total_count
    )
    gram = jnp.einsum("ktm,ktn->mn", moving_wide, applied, precision=highest)
    alpha = lax.psum(gram, ("row", "col")) / (total_count * band_count)
    residual = applied - jnp.einsum("ktm,mn->ktn", moving_wide, alpha, precision=highest)
    return (residual.reshape(local_count, band_count * vector_count), alpha)


def fits(args, mesh):
    pair_exchange, conduction, valence, _, screening, _, vectors, _ = args
    rows, cols = mesh.shape["row"], mesh.shape["col"]
    points, nb, planes = pair_exchange.shape
    nk = points // (rows * cols)
    nv, nc = valence.shape[1], conduction.shape[1]
    nvec = vectors.shape[1] // nb
    return (
        planes == rows * LANES and rows == 8 and cols == 4 and rows * cols * nk * 2 == LANES and nk == 2 and nv == 4 and nc == 4
        and nc * nvec == LANES and points == 2 * MX and screening.shape[0] == MX + 2
    )


def solution(mesh):
    in_specs = (
        P(("row", "col"), None, None),
        P(("row", "col"), None, None),
        P(("row", "col"), None, None),
        P(),
        P(),
        P(("row", "col"), None),
        P(("row", "col"), None),
        P(("row", "col"), None),
    )
    out_specs = (P(("row", "col"), None), P())

    def run(*args):
        body = fast_on_device if fits(args, mesh) else on_device
        return jax.shard_map(
            body, mesh=mesh, in_specs=in_specs, out_specs=out_specs, check_vma=False
        )(*args)

    return run
```

```python
import functools
import math

import jax
import jax.numpy as jnp
from jax import lax
from jax.experimental import pallas as pl
from jax.experimental.pallas import tpu as pltpu
from jax.sharding import PartitionSpec as P

MX = 32
LANES = 128
MESH = pl.DeviceIdType.MESH
F32 = jnp.float32
BF16 = jnp.bfloat16


def split_pair(value):
    high = value.astype(BF16)
    return high, (value - high.astype(F32)).astype(BF16)


def dot(a, b, contract):
    return lax.dot_general(a, b, ((contract[0:1], contract[1:2]), ((), ())), preferred_element_type=F32)


def iota(shape, axis):
    return lax.broadcasted_iota(jnp.int32, shape, axis)


def one_hot(condition):
    return jnp.where(condition, 1.0, 0.0).astype(BF16)


def wide_dot(a, b, contract):
    high, low = a
    main, rest = b
    return dot(high, main, contract) + dot(low, main, contract) + dot(high, rest, contract)


def beside(*parts):
    return jnp.concatenate(parts, axis=1)


def above(*parts):
    return jnp.concatenate(parts, axis=0)


def swap_blocks(tile, lanes, rows):
    row_bit = (iota(tile.shape, 0) // rows) % 2
    lane_bit = (iota(tile.shape, 1) // lanes) % 2
    up = pltpu.roll(pltpu.roll(tile, lanes, 1), tile.shape[0] - rows, 0)
    down = pltpu.roll(pltpu.roll(tile, LANES - lanes, 1), rows, 0)
    return jnp.where(row_bit == lane_bit, tile, jnp.where(lane_bit == 1, up, down))


def fold_blocks(square, width):
    kept = jnp.where(iota(square.shape, 0) // width == iota(square.shape, 1) // width, square, 0.0)
    rows = kept[0:width]
    for at in range(width, square.shape[0], width):
        rows = rows + kept[at:at + width]
    half = rows + pltpu.roll(rows, LANES // 2, 1)
    return half + pltpu.roll(half, LANES // 4, 1)


def basis(phase, sign):
    angle = (phase % MX).astype(F32) * (2.0 * math.pi / MX)
    return (jnp.cos(angle) + jnp.sin(angle)) * (1 - 2 * (sign % 2)).astype(F32)


def kernel(
    dims, px_hbm, cond_hbm, val_hbm, coulomb_hbm, screening_hbm, vec_hbm, energy_hbm, place_hbm,
    out_ref, alpha_ref,
    px_ref, cond_ref, val_ref, coulomb_ref, screening_ref, vec_ref, energy_ref, place_ref,
    load_sem, msg_ref, slots, px_msg, px_slots, select, select_q, lam, pairs, moved, proj, out_send, out_slots, gram_slots,
    base_send, base_slot, sends, arrivals,
):
    rows, cols, nk, nv, nc, nvec, total = dims
    row, col = lax.axis_index("row"), lax.axis_index("col")
    me = row * cols + col
    count = rows * cols
    nb = nv * nc
    low_row, high_row = rows // 4, rows - rows // 4
    hosts = (high_row - low_row) * cols
    host = (row >= low_row) & (row < high_row)
    guest = jnp.logical_not(host)
    near_row = jnp.where(row < low_row, row + low_row, jnp.where(row >= high_row, row - low_row, row))
    seat = (near_row - low_row) * cols + col
    width = LANES // cols
    deep = width // 2
    unit = nk * nv
    half = LANES // 2
    sheets = count * 8
    spans = rows * LANES // hosts // width
    levels = spans * deep

    ring_rows = [row] + [lax.rem(row + step, rows) for step in range(1, rows)]
    ring_cols = [col] + [lax.rem(col + step, cols) for step in range(1, cols)]
    everyone = [(pr, pc) for i, pr in enumerate(ring_rows) for j, pc in enumerate(ring_cols) if i + j]
    late = jnp.logical_and(col == 0, row < 2)
    rank = jnp.where(late, 0, me - 1 - (me > cols).astype(jnp.int32))

    def turned_to(step):
        at = rank + step
        at = jnp.where(at >= count - 2, at - (count - 2), at)
        spot = at + 1 + (at >= cols - 1).astype(jnp.int32)
        return spot // cols, lax.rem(spot, cols)

    leading = [(0, 0), (1, 0)] + [turned_to(step) for step in range(1, count - 2)]
    host_rows = [low_row + lax.rem(near_row - low_row + step, high_row - low_row) for step in range(high_row - low_row)]
    left = lax.rem(col, 2)
    host_cols = [cols - 1 - col, lax.rem(col + 2, cols), col + 1 - 2 * left, col]
    host_peers = [(pr, pc) for pc in host_cols for pr in host_rows[::-1]]

    barrier = pltpu.get_barrier_semaphore()
    mine = pl.ds(pl.multiple_of(seat // 2 * LANES, LANES), LANES)
    loads = [
        pltpu.make_async_copy(src, dst, load_sem.at[at])
        for at, (src, dst) in enumerate((
            (val_hbm, val_ref), (cond_hbm, cond_ref), (vec_hbm, vec_ref), (place_hbm, place_ref), (px_hbm, px_ref),
            (energy_hbm, energy_ref), (screening_hbm.at[:, mine], screening_ref), (coulomb_hbm.at[:, mine], coulomb_ref)))
    ]
    for load in loads[:4]:
        load.start()

    @pl.when(host)
    def _():
        for peer in leading:
            pl.semaphore_signal(barrier, inc=1, device_id=peer, device_id_type=MESH)

    for load in loads[4:]:
        load.start()
    row8 = iota((8, LANES), 0)
    lane8 = iota((8, LANES), 1)
    for load in loads[:4]:
        load.wait()

    vec = vec_ref[...].astype(F32)
    own = jnp.concatenate(
        [vec[k:k + 1, j * LANES:(j + 1) * LANES] for k in range(nk) for j in range(nv)], axis=0)
    tail = jnp.zeros((8, LANES), F32)
    wave = lane8 % half
    for k in range(nk):
        value = basis((wave // 2) * place_ref[k, 0], (wave % 2) * place_ref[k, 1])
        high = value.astype(BF16).astype(F32)
        tail = jnp.where(row8 == k, jnp.where(lane8 < half, high, value - high), tail)
    tail = above(tail, jnp.zeros((8, LANES), F32)).astype(BF16)
    for r in range(rows):
        span = slice(r * LANES, (r + 1) * LANES)
        turned = []
        for k in range(nk):
            tile = above(val_ref[k, :, span].astype(F32), cond_ref[k, :, span].astype(F32))
            for size in (4, 2, 1):
                tile = swap_blocks(tile, deep * size, size)
            turned.append(tile)
        flipped = [pltpu.roll(tile, 4, 0) for tile in turned]
        first_half = jnp.where(row8 < 4, turned[0], flipped[1])
        other_half = jnp.where(row8 < 4, flipped[0], turned[1])
        for q, low in enumerate((first_half, other_half)):
            msg_ref[r * 2 + q, 0:16] = above(own, low).astype(BF16)
            msg_ref[r * 2 + q, 16:32] = tail

    loads[4].wait()
    at = iota((nk * nb, nk * nb), 0)
    to = iota((nk * nb, nk * nb), 1)
    order = one_hot(to == (at % unit) // nv * nb + at % nv * nc + at // unit)
    arranged = dot(order, px_ref[...].reshape(nk * nb, px_ref.shape[2]), (1, 0))
    for r in range(rows):
        span = slice(r * LANES, (r + 1) * LANES)
        tiles = []
        for q in range(cols):
            tile = arranged[q * 8:q * 8 + 8, span]
            for b in range(cols):
                if b != q:
                    moving = pltpu.roll(arranged[b * 8:b * 8 + 8, span], (width * (b - q)) % LANES, 1)
                    tile = jnp.where(lane8 // width == b, moving, tile)
            tiles.append(tile)
        for q in range(2):
            px_msg[r * 2 + q] = above(tiles[2 * q], tiles[2 * q + 1]).astype(BF16)
    @pl.when(host)
    def _():
        pl.semaphore_wait(barrier, hosts - 1)

    @pl.when(guest)
    def _():
        pl.semaphore_wait(barrier, hosts)

    def main_copy(device):
        peer = (device[0] - low_row) * cols + device[1]
        return pltpu.make_async_remote_copy(
            src_ref=msg_ref.at[peer, 0:18], dst_ref=slots.at[me, 0:18],
            send_sem=sends.at[0], recv_sem=arrivals.at[0], device_id=device, device_id_type=MESH)

    def px_copy(device):
        peer = (device[0] - low_row) * cols + device[1]
        return pltpu.make_async_remote_copy(
            src_ref=px_msg.at[peer], dst_ref=px_slots.at[me],
            send_sem=sends.at[1], recv_sem=arrivals.at[1], device_id=device, device_id_type=MESH)

    def out_copy(device):
        peer = device[0] * cols + device[1]
        return pltpu.make_async_remote_copy(
            src_ref=out_send.at[peer], dst_ref=out_slots.at[seat],
            send_sem=sends.at[2], recv_sem=arrivals.at[2], device_id=device, device_id_type=MESH)

    def gram_copy(device):
        return pltpu.make_async_remote_copy(
            src_ref=gram_slots.at[seat], dst_ref=gram_slots.at[seat],
            send_sem=sends.at[3], recv_sem=arrivals.at[3], device_id=device, device_id_type=MESH)

    def base_copy():
        return pltpu.make_async_remote_copy(
            src_ref=base_send, dst_ref=base_slot,
            send_sem=sends.at[4], recv_sem=arrivals.at[4], device_id=(near_row, col), device_id_type=MESH)

    def start_all(copy, targets):
        for peer in targets:
            copy(peer).start()

    def pack(block):
        piece = block[0:8]
        for b in range(1, nc):
            piece = jnp.where(lane8 // nvec == b, block[b * 8:b * 8 + 8], piece)
        return piece

    def landed(ref, sem):
        pltpu.make_async_copy(ref, ref, sem).wait()

    def to_hosts(copy, here, there):
        start_all(copy, host_peers[:-1])

        @pl.when(guest)
        def _():
            copy(host_peers[-1]).start()

        @pl.when(host)
        def _():
            there[me] = here[seat]

    to_hosts(main_copy, msg_ref, slots)

    to_hosts(px_copy, px_msg, px_slots)

    loads[5].wait()
    energy = jnp.zeros((8, LANES), F32)
    for k in range(nk):
        for t in range(nb):
            energy = jnp.where((row8 == k * nv + t // nc) & (lane8 // nvec == t % nc), energy_ref[k, t], energy)
    lifted = energy * own
    high, low = split_pair(lifted)
    own_low = own.astype(BF16)
    base_send[...] = pack(fold_blocks(dot(own_low, high, (0, 0)) + dot(own_low, low, (0, 0)), nvec))

    @pl.when(guest)
    def _():
        base_copy().start()

    for load in loads[6:]:
        load.wait()

    @pl.when(host)
    def _():
        at = iota((sheets, LANES), 0)
        to = iota((sheets, LANES), 1)
        same = at // 8 == (to % half) // nk
        place = at % 8
        for j in range(nv):
            select[:, j * LANES:(j + 1) * LANES] = one_hot(same & (place == to % nk * nv + j))
        for a in range(spans):
            select[:, (nv + a) * LANES:(nv + a + 1) * LANES] = one_hot(
                same & (place == to % nk * 2 * spans + 2 * a + to // half))
        at = iota((LANES, sheets), 0)
        to = iota((LANES, sheets), 1)
        select_q[...] = one_hot((to // 8 == (at % half) // nk) & (to % 8 == at % nk))
        at = iota((LANES, LANES), 0)
        to = iota((LANES, LANES), 1)
        fold = at // 2
        angle = ((fold * ((to % half) // 2)) % MX).astype(F32) * (2.0 * math.pi / MX)
        weight = jnp.where((fold == 0) | (fold == MX // 2), 1.0, 2.0) * (1 - 2 * ((at % 2) * (to % 2))).astype(F32)
        table = jnp.where(fold <= MX // 2, jnp.cos(angle) * weight, 0.0)
        screened = above(screening_ref[...], jnp.zeros((LANES - screening_ref.shape[0], LANES), F32))
        lam[...] = wide_dot(split_pair(screened), split_pair(table), (0, 0)) * (-1.0 / (total * total))
        second_half = lax.rem(seat, 2)
        band = lam[pl.ds(pl.multiple_of(second_half * half, 8), half), :]
        lane_d = iota((deep, LANES), 1)
        spectrum = above(*[
            jnp.where(lane_d < half, band[2 * a * deep:(2 * a + 1) * deep], band[(2 * a + 1) * deep:(2 * a + 2) * deep])
            for a in range(spans)])
        raw = jnp.broadcast_to(coulomb_ref[...], (width, LANES)) * (2.0 / (total * nb))
        lane_w = iota((width, LANES), 1)
        charges = []
        for a in range(spans):
            tiles = jnp.zeros((width, LANES), F32)
            for b in range(cols):
                for q in range(2):
                    shift = (width * (b - 2 * q - a)) % LANES
                    moving = raw if shift == 0 else pltpu.roll(raw, shift, 1)
                    tiles = jnp.where((lane_w // width == b) & (second_half == q), moving, tiles)
            charges.append(tiles)

        landed(slots.at[0:count - 1, 0:18], arrivals.at[0])
        got = slots[...].astype(F32)
        own_all, rest_all, wave_all = [
            got[:, 8 * part:8 * part + 8].reshape(sheets, LANES) for part in range(3)]
        own_all, rest_all = own_all.astype(BF16), rest_all.astype(BF16)
        wave_all = jnp.where(iota((sheets, LANES), 0) % 8 < nk, wave_all, 0.0).astype(BF16)
        factors = dot(rest_all, select[:, nv * LANES:], (0, 0))
        spread = dot(own_all, select[:, 0:nv * LANES], (0, 0))
        for v in range(nv):
            for c in range(nc):
                for a in range(spans):
                    lanes = slice(a * LANES, (a + 1) * LANES)
                    joined = (
                        factors[v * deep:(v + 1) * deep, lanes] * factors[half + c * deep:half + (c + 1) * deep, lanes])
                    pairs[v * nc + c, a * deep:(a + 1) * deep] = joined.astype(BF16).astype(F32)
        for t in range(nb):
            moved[t] = spread[t % nc * nvec:(t % nc + 1) * nvec, t // nc * LANES:(t // nc + 1) * LANES]
        waves = dot(select_q[...], wave_all, (1, 0))
        crossed = pltpu.roll(waves, half, 1)
        first = (at < half) & (to < half)
        second = (at >= half) & (to >= half)
        main = jnp.where(first, waves, jnp.where(second, crossed, 0.0)).astype(BF16)
        fine = jnp.where(first, crossed, jnp.where(second, waves, 0.0)).astype(BF16)
        none = jnp.zeros((LANES, LANES), BF16)
        ahead = above(beside(main, fine), beside(main, none))
        astern = above(beside(main, main), beside(fine, none))

        def through(values, weights, contract):
            both = dot(beside(*split_pair(values)), weights, contract)
            return both[:, 0:LANES] + both[:, LANES:]

        group = 2
        for first_l in range(0, levels, group):
            sums_l = [None] * group
            for t in range(nb):
                for u in range(group):
                    term = pairs[t, first_l + u:first_l + u + 1, :] * moved[t]
                    sums_l[u] = term if t == 0 else sums_l[u] + term
            for u in range(group):
                proj[first_l + u] = sums_l[u]
        spectral = through(proj[...].reshape(levels * nvec, LANES), ahead, (1, 0)).reshape(levels, nvec, LANES)
        scaled = spectral * spectrum[:, None, :]
        sides = [
            split_pair(jnp.concatenate([side[l] for l in range(levels)], axis=1)) for side in (spectral, scaled)]
        gram = wide_dot(*sides, (1, 1))

        landed(px_slots.at[0:count - 1], arrivals.at[1])
        taken_px = px_slots[...].astype(F32)
        exchange = beside(*[
            taken_px[:, 8 * a:8 * a + 8].reshape(sheets, LANES).astype(BF16) for a in range(spans)])
        crowd = dot(own_all, exchange, (0, 0))
        densities = [fold_blocks(crowd[:, a * LANES:(a + 1) * LANES], nvec) for a in range(spans)]
        charged = [density * charge for density, charge in zip(densities, charges)]
        gram = gram + wide_dot(
            split_pair(beside(*densities)), split_pair(beside(*charged) * (1.0 / cols)), (1, 1))
        proj[...] = through(scaled.reshape(levels * nvec, LANES), astern, (1, 1)).reshape(levels, nvec, LANES)
        for first_t in range(0, nb // 2, group):
            sums_t = [None] * group
            for l in range(levels):
                for u in range(group):
                    term = pairs[first_t + u, l:l + 1, :] * proj[l]
                    sums_t[u] = term if l == 0 else sums_t[u] + term
            for u in range(group):
                moved[first_t + u] = sums_t[u]
        landed(base_slot, arrivals.at[4])
        gram_slots[seat] = (
            base_send[...] + base_slot[...] + pack(jnp.concatenate([gram] * nc, axis=1))).astype(BF16)
        start_all(gram_copy, leading[:2])

        blocks = beside(*[
            jnp.where(at // nvec == to // width, jnp.concatenate([charge] * (LANES // nvec), axis=0), 0.0)
            for charge in charged])
        whole = dot(exchange, above(*split_pair(blocks)), (1, 1))
        for first_t in range(nb // 2, nb, group):
            sums_t = [None] * group
            for l in range(levels):
                for u in range(group):
                    term = pairs[first_t + u, l:l + 1, :] * proj[l]
                    sums_t[u] = term if l == 0 else sums_t[u] + term
            for u in range(group):
                moved[first_t + u] = sums_t[u]
        placed = jnp.concatenate(
            [jnp.concatenate([moved[j * nc + c] for c in range(nc)], axis=0) for j in range(nv)], axis=1)
        whole = whole + dot(select[:, 0:nv * LANES], above(*split_pair(placed)), (1, 1))
        whole = whole[:, 0:LANES] + whole[:, LANES:]
        out_send[...] = whole.reshape(count, 8, LANES)
        start_all(out_copy, leading)
        start_all(gram_copy, leading[2:])
        out_slots[seat] = out_send[me]

    def each(run):
        @pl.when(host)
        def _():
            run(hosts - 1)

        @pl.when(guest)
        def _():
            run(hosts)

    each(lambda n: landed(gram_slots.at[0:n], arrivals.at[3]))
    sums = jnp.sum(gram_slots[...].astype(F32), axis=0) * (1.0 / (total * nb))
    turns = [sums] + [pltpu.roll(sums, b * nvec, 1) for b in range(1, nc)]
    for b in range(nc):
        alpha_ref[b * 8:b * 8 + 8] = turns[(-b) % nc][:, 0:nvec]
    mixed = jnp.concatenate(
        [jnp.where(lane8 // nvec == q, turns[(q - b) % nc], 0.0) for q in range(nc) for b in range(nc)], axis=0)
    high, low = split_pair(mixed)
    rest = lifted - dot(own_low, high, (1, 0)) - dot(own_low, low, (1, 0))

    each(lambda n: landed(out_slots.at[0:n], arrivals.at[2]))
    residual = rest + jnp.sum(out_slots[...], axis=0)
    for j in range(nv):
        out_ref[:, j * LANES:(j + 1) * LANES] = jnp.concatenate(
            [residual[k * nv + j:k * nv + j + 1] for k in range(nk)], axis=0)

    def drain(n):
        landed(slots.at[0:n, 0:18], sends.at[0])
        landed(px_slots.at[0:n], sends.at[1])

    each(drain)

    @pl.when(guest)
    def _():
        landed(base_slot, sends.at[4])

    @pl.when(host)
    def _():
        landed(out_send.at[0:count - 1], sends.at[2])
        landed(slots.at[0:count - 1, 0:8], sends.at[3])


def finish(out_ref, alpha_ref, out_hbm, alpha_hbm, sems):
    copies = [
        pltpu.make_async_copy(src, dst, sems.at[at])
        for at, (src, dst) in enumerate(((out_ref, out_hbm), (alpha_ref, alpha_hbm)))]
    for copy in copies:
        copy.start()
    for copy in copies:
        copy.wait()


def fast_on_device(pair_exchange, conduction, valence, coulomb, screening, energies, vectors, k_coords):
    nk, nb, planes = pair_exchange.shape
    nv, nc = valence.shape[1], conduction.shape[1]
    nvec = vectors.shape[1] // nb
    rows, cols = lax.axis_size("row"), lax.axis_size("col")
    count = rows * cols
    total = nk * count
    hosts = count // 2
    width = LANES // cols
    spans = planes // hosts // width
    levels = spans * width // 2
    vmem = pl.BlockSpec(memory_space=pltpu.VMEM)
    dma = pltpu.SemaphoreType.DMA
    results = pl.pallas_call(
        functools.partial(kernel, (rows, cols, nk, nv, nc, nvec, total)),
        out_shape=(
            pltpu.VMEM((nk, nb * nvec), F32),
            pltpu.VMEM((nvec, nvec), F32),
        ),
        in_specs=[pl.BlockSpec(memory_space=pl.ANY)] * 8,
        out_specs=(vmem, vmem),
        scratch_shapes=[
            pltpu.VMEM(pair_exchange.shape, BF16),
            pltpu.VMEM(conduction.shape, BF16),
            pltpu.VMEM(valence.shape, BF16),
            pltpu.VMEM((1, LANES), F32),
            pltpu.VMEM((screening.shape[0], LANES), F32),
            pltpu.VMEM(vectors.shape, BF16),
            pltpu.SMEM(energies.shape, F32),
            pltpu.SMEM(k_coords.shape, jnp.int32),
            dma((8,)),
            pltpu.VMEM((hosts, 32, LANES), BF16),
            pltpu.VMEM((count, 32, LANES), BF16),
            pltpu.VMEM((hosts, 16, LANES), BF16),
            pltpu.VMEM((count, 16, LANES), BF16),
            pltpu.VMEM((count * 8, (nv + spans) * LANES), BF16),
            pltpu.VMEM((LANES, count * 8), BF16),
            pltpu.VMEM((LANES, LANES), F32),
            pltpu.VMEM((nb, levels, LANES), F32),
            pltpu.VMEM((nb, nvec, LANES), F32),
            pltpu.VMEM((levels, nvec, LANES), F32),
            pltpu.VMEM((count, 8, LANES), F32),
            pltpu.VMEM((hosts, 8, LANES), F32),
            pltpu.VMEM((hosts, 8, LANES), BF16),
            pltpu.VMEM((8, LANES), F32),
            pltpu.VMEM((8, LANES), F32),
            dma((5,)), dma((5,)),
        ],
        compiler_params=pltpu.CompilerParams(collective_id=0, has_side_effects=True),
    )(pair_exchange, conduction, valence, coulomb.reshape(1, planes), screening, vectors, energies, k_coords)
    return pl.pallas_call(
        finish,
        out_shape=(jax.ShapeDtypeStruct((nk, nb * nvec), F32), jax.ShapeDtypeStruct((nvec, nvec), F32)),
        in_specs=[vmem, vmem],
        out_specs=(pl.BlockSpec(memory_space=pl.ANY), pl.BlockSpec(memory_space=pl.ANY)),
        scratch_shapes=[dma((2,))],
    )(*[pltpu.with_memory_space_constraint(result, pltpu.VMEM) for result in results])


highest = lax.Precision.HIGHEST


def pair_factors(conduction, valence):
    count, valence_count, plane_count = valence.shape
    joined = (
        valence.astype(jnp.float32)[:, :, None, :] * conduction.astype(jnp.float32)[:, None, :, :]
    )
    return joined.reshape(count, valence_count * conduction.shape[1], plane_count).astype(
        jnp.bfloat16
    )


def transfer_index(rows_at, cols_at, mesh_cols):
    delta_first = jnp.mod(rows_at[:, None, 0] - cols_at[None, :, 0], MX)
    delta_second = jnp.mod(rows_at[:, None, 1] - cols_at[None, :, 1], mesh_cols)
    fold_first = jnp.minimum(delta_first, MX - delta_first)
    fold_second = jnp.minimum(delta_second, mesh_cols - delta_second)
    return (fold_first * (mesh_cols // 2 + 1) + fold_second).astype(jnp.int32)


def on_device(pair_exchange, conduction, valence, coulomb, screening, energies, vectors, k_coords):
    local_count, band_count, plane_count = pair_exchange.shape
    vector_count = vectors.shape[1] // band_count
    row_count = lax.axis_size("row")
    col_count = lax.axis_size("col")
    total_count = local_count * row_count * col_count
    mesh_cols = total_count // MX
    moving = vectors.reshape(local_count, band_count, vector_count)
    partial_density = jnp.einsum(
        "ktg,ktn->gn", pair_exchange, moving, preferred_element_type=jnp.float32
    )
    density = lax.psum(partial_density, ("row", "col"))
    block_size = 128
    sweeps = plane_count // block_size
    col_cond, col_val, col_vec, col_at = (
        lax.all_gather(conduction, "row", axis=0, tiled=True),
        lax.all_gather(valence, "row", axis=0, tiled=True),
        lax.all_gather(vectors, "row", axis=0, tiled=True),
        lax.all_gather(k_coords, "row", axis=0, tiled=True),
    )
    row_cond, row_val, row_at = (
        lax.all_gather(conduction, "col", axis=0, tiled=True),
        lax.all_gather(valence, "col", axis=0, tiled=True),
        lax.all_gather(k_coords, "col", axis=0, tiled=True),
    )
    row_pairs = pair_factors(row_cond, row_val)
    col_pairs = pair_factors(col_cond, col_val)
    indices = transfer_index(row_at, col_at, mesh_cols)
    col_moving = col_vec.reshape(-1, band_count, vector_count)

    def square_sweep(sweep_index, running):
        anchor = sweep_index * block_size
        coupling = jnp.take(
            lax.dynamic_slice_in_dim(screening, anchor, block_size, 1), indices, axis=0
        )
        row_block = lax.dynamic_slice_in_dim(row_pairs, anchor, block_size, 2)
        col_block = lax.dynamic_slice_in_dim(col_pairs, anchor, block_size, 2)
        col_proj = jnp.einsum(
            "ktg,ktn->kng", col_block, col_moving, preferred_element_type=jnp.float32
        )
        potential = jnp.einsum("ijg,jng->ing", coupling, col_proj, precision=highest)
        return running + jnp.einsum(
            "ktg,kng->ktn", row_block.astype(jnp.float32), potential, precision=highest
        )

    forward = lax.fori_loop(
        0,
        sweeps,
        square_sweep,
        jnp.zeros((row_pairs.shape[0], band_count, vector_count), jnp.float32),
    )
    owned = lax.psum_scatter(
        forward.reshape(col_count, local_count, band_count, vector_count),
        "col",
        scatter_dimension=0,
        tiled=True,
    )[0]
    moving_wide = moving.astype(jnp.float32)
    exchange_term = jnp.einsum(
        "ktg,gn->ktn", pair_exchange.astype(jnp.float32) * coulomb, density, precision=highest
    )
    applied = (
        energies[:, :, None] * moving_wide
        + 2.0 / (total_count * band_count) * exchange_term
        - owned / total_count
    )
    gram = jnp.einsum("ktm,ktn->mn", moving_wide, applied, precision=highest)
    alpha = lax.psum(gram, ("row", "col")) / (total_count * band_count)
    residual = applied - jnp.einsum("ktm,mn->ktn", moving_wide, alpha, precision=highest)
    return (residual.reshape(local_count, band_count * vector_count), alpha)


def fits(args, mesh):
    pair_exchange, conduction, valence, _, screening, _, vectors, _ = args
    rows, cols = mesh.shape["row"], mesh.shape["col"]
    points, nb, planes = pair_exchange.shape
    nk = points // (rows * cols)
    nv, nc = valence.shape[1], conduction.shape[1]
    nvec = vectors.shape[1] // nb
    return (
        planes == rows * LANES and rows == 8 and cols == 4 and rows * cols * nk * 2 == LANES and nk == 2 and nv == 4 and nc == 4
        and nc * nvec == LANES and points == 2 * MX and screening.shape[0] == MX + 2
    )


def solution(mesh):
    in_specs = (
        P(("row", "col"), None, None),
        P(("row", "col"), None, None),
        P(("row", "col"), None, None),
        P(),
        P(),
        P(("row", "col"), None),
        P(("row", "col"), None),
        P(("row", "col"), None),
    )
    out_specs = (P(("row", "col"), None), P())

    def run(*args):
        body = fast_on_device if fits(args, mesh) else on_device
        return jax.shard_map(
            body, mesh=mesh, in_specs=in_specs, out_specs=out_specs, check_vma=False
        )(*args)

    return run
```

```python
import functools
import math

import jax
import jax.numpy as jnp
from jax import lax
from jax.experimental import pallas as pl
from jax.experimental.pallas import tpu as pltpu
from jax.sharding import PartitionSpec as P

MX = 32
LANES = 128
MESH = pl.DeviceIdType.MESH
F32 = jnp.float32
BF16 = jnp.bfloat16


def split_pair(value):
    high = value.astype(BF16)
    return high, (value - high.astype(F32)).astype(BF16)


def dot(a, b, contract):
    return lax.dot_general(a, b, ((contract[0:1], contract[1:2]), ((), ())), preferred_element_type=F32)


def iota(shape, axis):
    return lax.broadcasted_iota(jnp.int32, shape, axis)


def one_hot(condition):
    return jnp.where(condition, 1.0, 0.0).astype(BF16)


def wide_dot(a, b, contract):
    high, low = a
    main, rest = b
    return dot(high, main, contract) + dot(low, main, contract) + dot(high, rest, contract)


def beside(*parts):
    return jnp.concatenate(parts, axis=1)


def above(*parts):
    return jnp.concatenate(parts, axis=0)


def swap_blocks(tile, lanes, rows):
    row_bit = (iota(tile.shape, 0) // rows) % 2
    lane_bit = (iota(tile.shape, 1) // lanes) % 2
    up = pltpu.roll(pltpu.roll(tile, lanes, 1), tile.shape[0] - rows, 0)
    down = pltpu.roll(pltpu.roll(tile, LANES - lanes, 1), rows, 0)
    return jnp.where(row_bit == lane_bit, tile, jnp.where(lane_bit == 1, up, down))


def fold_blocks(square, width):
    kept = jnp.where(iota(square.shape, 0) // width == iota(square.shape, 1) // width, square, 0.0)
    rows = kept[0:width]
    for at in range(width, square.shape[0], width):
        rows = rows + kept[at:at + width]
    half = rows + pltpu.roll(rows, LANES // 2, 1)
    return half + pltpu.roll(half, LANES // 4, 1)


def basis(phase, sign):
    angle = (phase % MX).astype(F32) * (2.0 * math.pi / MX)
    return (jnp.cos(angle) + jnp.sin(angle)) * (1 - 2 * (sign % 2)).astype(F32)


def kernel(
    dims, px_hbm, cond_hbm, val_hbm, coulomb_hbm, screening_hbm, vec_hbm, energy_hbm, place_hbm,
    out_ref, alpha_ref,
    px_ref, cond_ref, val_ref, coulomb_ref, screening_ref, vec_ref, energy_ref, place_ref,
    load_sem, msg_ref, slots, px_msg, px_slots, select, select_q, lam, pairs, moved, proj, out_send, out_slots, gram_slots,
    base_send, base_slot, sends, arrivals,
):
    rows, cols, nk, nv, nc, nvec, total = dims
    row, col = lax.axis_index("row"), lax.axis_index("col")
    me = row * cols + col
    count = rows * cols
    nb = nv * nc
    low_row, high_row = rows // 4, rows - rows // 4
    hosts = (high_row - low_row) * cols
    host = (row >= low_row) & (row < high_row)
    guest = jnp.logical_not(host)
    near_row = jnp.where(row < low_row, row + low_row, jnp.where(row >= high_row, row - low_row, row))
    seat = (near_row - low_row) * cols + col
    width = LANES // cols
    deep = width // 2
    unit = nk * nv
    half = LANES // 2
    sheets = count * 8
    spans = rows * LANES // hosts // width
    levels = spans * deep

    ring_rows = [row] + [lax.rem(row + step, rows) for step in range(1, rows)]
    ring_cols = [col] + [lax.rem(col + step, cols) for step in range(1, cols)]
    everyone = [(pr, pc) for i, pr in enumerate(ring_rows) for j, pc in enumerate(ring_cols) if i + j]
    signalled = [
        (jnp.where(me == at, rows - 1, at // cols), jnp.where(me == at, cols - 1, at % cols)) for at in range(count - 1)]
    host_rows = [low_row + lax.rem(near_row - low_row + step, high_row - low_row) for step in range(high_row - low_row)]
    left = lax.rem(col, 2)
    host_cols = [cols - 1 - col, lax.rem(col + 2, cols), col + 1 - 2 * left, col]
    host_peers = [(pr, pc) for pc in host_cols for pr in host_rows[::-1]]

    barrier = pltpu.get_barrier_semaphore()
    mine = pl.ds(pl.multiple_of(seat // 2 * LANES, LANES), LANES)
    loads = [
        pltpu.make_async_copy(src, dst, load_sem.at[at])
        for at, (src, dst) in enumerate((
            (val_hbm, val_ref), (cond_hbm, cond_ref), (vec_hbm, vec_ref), (place_hbm, place_ref), (px_hbm, px_ref),
            (energy_hbm, energy_ref), (screening_hbm.at[:, mine], screening_ref), (coulomb_hbm.at[:, mine], coulomb_ref)))
    ]
    for load in loads[:4]:
        load.start()

    @pl.when(host)
    def _():
        for peer in signalled:
            pl.semaphore_signal(barrier, inc=1, device_id=peer, device_id_type=MESH)

    for load in loads[4:]:
        load.start()
    row8 = iota((8, LANES), 0)
    lane8 = iota((8, LANES), 1)
    for load in loads[:4]:
        load.wait()

    vec = vec_ref[...].astype(F32)
    own = jnp.concatenate(
        [vec[k:k + 1, j * LANES:(j + 1) * LANES] for k in range(nk) for j in range(nv)], axis=0)
    tail = jnp.zeros((8, LANES), F32)
    wave = lane8 % half
    for k in range(nk):
        value = basis((wave // 2) * place_ref[k, 0], (wave % 2) * place_ref[k, 1])
        high = value.astype(BF16).astype(F32)
        tail = jnp.where(row8 == k, jnp.where(lane8 < half, high, value - high), tail)
    tail = above(tail, jnp.zeros((8, LANES), F32)).astype(BF16)
    for r in range(rows):
        span = slice(r * LANES, (r + 1) * LANES)
        turned = []
        for k in range(nk):
            tile = above(val_ref[k, :, span].astype(F32), cond_ref[k, :, span].astype(F32))
            for size in (4, 2, 1):
                tile = swap_blocks(tile, deep * size, size)
            turned.append(tile)
        flipped = [pltpu.roll(tile, 4, 0) for tile in turned]
        first_half = jnp.where(row8 < 4, turned[0], flipped[1])
        other_half = jnp.where(row8 < 4, flipped[0], turned[1])
        for q, low in enumerate((first_half, other_half)):
            msg_ref[r * 2 + q, 0:16] = above(own, low).astype(BF16)
            msg_ref[r * 2 + q, 16:32] = tail

    loads[4].wait()
    at = iota((nk * nb, nk * nb), 0)
    to = iota((nk * nb, nk * nb), 1)
    order = one_hot(to == (at % unit) // nv * nb + at % nv * nc + at // unit)
    arranged = dot(order, px_ref[...].reshape(nk * nb, px_ref.shape[2]), (1, 0))
    for r in range(rows):
        span = slice(r * LANES, (r + 1) * LANES)
        tiles = []
        for q in range(cols):
            tile = arranged[q * 8:q * 8 + 8, span]
            for b in range(cols):
                if b != q:
                    moving = pltpu.roll(arranged[b * 8:b * 8 + 8, span], (width * (b - q)) % LANES, 1)
                    tile = jnp.where(lane8 // width == b, moving, tile)
            tiles.append(tile)
        for q in range(2):
            px_msg[r * 2 + q] = above(tiles[2 * q], tiles[2 * q + 1]).astype(BF16)
    @pl.when(host)
    def _():
        pl.semaphore_wait(barrier, hosts - 1)

    @pl.when(guest)
    def _():
        pl.semaphore_wait(barrier, hosts)

    def main_copy(device):
        peer = (device[0] - low_row) * cols + device[1]
        return pltpu.make_async_remote_copy(
            src_ref=msg_ref.at[peer, 0:18], dst_ref=slots.at[me, 0:18],
            send_sem=sends.at[0], recv_sem=arrivals.at[0], device_id=device, device_id_type=MESH)

    def px_copy(device):
        peer = (device[0] - low_row) * cols + device[1]
        return pltpu.make_async_remote_copy(
            src_ref=px_msg.at[peer], dst_ref=px_slots.at[me],
            send_sem=sends.at[1], recv_sem=arrivals.at[1], device_id=device, device_id_type=MESH)

    def out_copy(device):
        peer = device[0] * cols + device[1]
        return pltpu.make_async_remote_copy(
            src_ref=out_send.at[peer], dst_ref=out_slots.at[seat],
            send_sem=sends.at[2], recv_sem=arrivals.at[2], device_id=device, device_id_type=MESH)

    def gram_copy(device):
        return pltpu.make_async_remote_copy(
            src_ref=gram_slots.at[seat], dst_ref=gram_slots.at[seat],
            send_sem=sends.at[3], recv_sem=arrivals.at[3], device_id=device, device_id_type=MESH)

    def base_copy():
        return pltpu.make_async_remote_copy(
            src_ref=base_send, dst_ref=base_slot,
            send_sem=sends.at[4], recv_sem=arrivals.at[4], device_id=(near_row, col), device_id_type=MESH)

    def start_all(copy, targets):
        for peer in targets:
            copy(peer).start()

    def pack(block):
        piece = block[0:8]
        for b in range(1, nc):
            piece = jnp.where(lane8 // nvec == b, block[b * 8:b * 8 + 8], piece)
        return piece

    def landed(ref, sem):
        pltpu.make_async_copy(ref, ref, sem).wait()

    def to_hosts(copy, here, there):
        start_all(copy, host_peers[:-1])

        @pl.when(guest)
        def _():
            copy(host_peers[-1]).start()

        @pl.when(host)
        def _():
            there[me] = here[seat]

    to_hosts(main_copy, msg_ref, slots)

    to_hosts(px_copy, px_msg, px_slots)

    loads[5].wait()
    energy = jnp.zeros((8, LANES), F32)
    for k in range(nk):
        for t in range(nb):
            energy = jnp.where((row8 == k * nv + t // nc) & (lane8 // nvec == t % nc), energy_ref[k, t], energy)
    lifted = energy * own
    high, low = split_pair(lifted)
    own_low = own.astype(BF16)
    base_send[...] = pack(fold_blocks(dot(own_low, high, (0, 0)) + dot(own_low, low, (0, 0)), nvec))

    @pl.when(guest)
    def _():
        base_copy().start()

    for load in loads[6:]:
        load.wait()

    @pl.when(host)
    def _():
        late = jnp.logical_and(col == 0, row < 2)
        rank = jnp.where(late, 0, me - 1 - (me > cols).astype(jnp.int32))

        def turned_to(step):
            at = rank + step
            at = jnp.where(at >= count - 2, at - (count - 2), at)
            spot = at + 1 + (at >= cols - 1).astype(jnp.int32)
            return spot // cols, lax.rem(spot, cols)

        leading = [(0, 0), (1, 0)] + [turned_to(step) for step in range(1, count - 2)]
        at = iota((sheets, LANES), 0)
        to = iota((sheets, LANES), 1)
        same = at // 8 == (to % half) // nk
        place = at % 8
        for j in range(nv):
            select[:, j * LANES:(j + 1) * LANES] = one_hot(same & (place == to % nk * nv + j))
        for a in range(spans):
            select[:, (nv + a) * LANES:(nv + a + 1) * LANES] = one_hot(
                same & (place == to % nk * 2 * spans + 2 * a + to // half))
        at = iota((LANES, sheets), 0)
        to = iota((LANES, sheets), 1)
        select_q[...] = one_hot((to // 8 == (at % half) // nk) & (to % 8 == at % nk))
        at = iota((LANES, LANES), 0)
        to = iota((LANES, LANES), 1)
        fold = at // 2
        angle = ((fold * ((to % half) // 2)) % MX).astype(F32) * (2.0 * math.pi / MX)
        weight = jnp.where((fold == 0) | (fold == MX // 2), 1.0, 2.0) * (1 - 2 * ((at % 2) * (to % 2))).astype(F32)
        table = jnp.where(fold <= MX // 2, jnp.cos(angle) * weight, 0.0)
        screened = above(screening_ref[...], jnp.zeros((LANES - screening_ref.shape[0], LANES), F32))
        lam[...] = wide_dot(split_pair(screened), split_pair(table), (0, 0)) * (-1.0 / (total * total))
        second_half = lax.rem(seat, 2)
        band = lam[pl.ds(pl.multiple_of(second_half * half, 8), half), :]
        lane_d = iota((deep, LANES), 1)
        spectrum = above(*[
            jnp.where(lane_d < half, band[2 * a * deep:(2 * a + 1) * deep], band[(2 * a + 1) * deep:(2 * a + 2) * deep])
            for a in range(spans)])
        raw = jnp.broadcast_to(coulomb_ref[...], (width, LANES)) * (2.0 / (total * nb))
        lane_w = iota((width, LANES), 1)
        charges = []
        for a in range(spans):
            tiles = jnp.zeros((width, LANES), F32)
            for b in range(cols):
                for q in range(2):
                    shift = (width * (b - 2 * q - a)) % LANES
                    moving = raw if shift == 0 else pltpu.roll(raw, shift, 1)
                    tiles = jnp.where((lane_w // width == b) & (second_half == q), moving, tiles)
            charges.append(tiles)

        landed(slots.at[0:count - 1, 0:18], arrivals.at[0])
        got = slots[...].astype(F32)
        own_all, rest_all, wave_all = [
            got[:, 8 * part:8 * part + 8].reshape(sheets, LANES) for part in range(3)]
        own_all, rest_all = own_all.astype(BF16), rest_all.astype(BF16)
        wave_all = jnp.where(iota((sheets, LANES), 0) % 8 < nk, wave_all, 0.0).astype(BF16)
        factors = dot(rest_all, select[:, nv * LANES:], (0, 0))
        spread = dot(own_all, select[:, 0:nv * LANES], (0, 0))
        for v in range(nv):
            for c in range(nc):
                for a in range(spans):
                    lanes = slice(a * LANES, (a + 1) * LANES)
                    joined = (
                        factors[v * deep:(v + 1) * deep, lanes] * factors[half + c * deep:half + (c + 1) * deep, lanes])
                    pairs[v * nc + c, a * deep:(a + 1) * deep] = joined.astype(BF16).astype(F32)
        for t in range(nb):
            moved[t] = spread[t % nc * nvec:(t % nc + 1) * nvec, t // nc * LANES:(t // nc + 1) * LANES]
        waves = dot(select_q[...], wave_all, (1, 0))
        crossed = pltpu.roll(waves, half, 1)
        first = (at < half) & (to < half)
        second = (at >= half) & (to >= half)
        main = jnp.where(first, waves, jnp.where(second, crossed, 0.0)).astype(BF16)
        fine = jnp.where(first, crossed, jnp.where(second, waves, 0.0)).astype(BF16)
        none = jnp.zeros((LANES, LANES), BF16)
        ahead = above(beside(main, fine), beside(main, none))
        astern = above(beside(main, main), beside(fine, none))

        def through(values, weights, contract):
            both = dot(beside(*split_pair(values)), weights, contract)
            return both[:, 0:LANES] + both[:, LANES:]

        group = 2
        for first_l in range(0, levels, group):
            sums_l = [None] * group
            for t in range(nb):
                for u in range(group):
                    term = pairs[t, first_l + u:first_l + u + 1, :] * moved[t]
                    sums_l[u] = term if t == 0 else sums_l[u] + term
            for u in range(group):
                proj[first_l + u] = sums_l[u]
        spectral = through(proj[...].reshape(levels * nvec, LANES), ahead, (1, 0)).reshape(levels, nvec, LANES)
        scaled = spectral * spectrum[:, None, :]
        sides = [
            split_pair(jnp.concatenate([side[l] for l in range(levels)], axis=1)) for side in (spectral, scaled)]
        gram = wide_dot(*sides, (1, 1))

        landed(px_slots.at[0:count - 1], arrivals.at[1])
        taken_px = px_slots[...].astype(F32)
        exchange = beside(*[
            taken_px[:, 8 * a:8 * a + 8].reshape(sheets, LANES).astype(BF16) for a in range(spans)])
        crowd = dot(own_all, exchange, (0, 0))
        densities = [fold_blocks(crowd[:, a * LANES:(a + 1) * LANES], nvec) for a in range(spans)]
        charged = [density * charge for density, charge in zip(densities, charges)]
        gram = gram + wide_dot(
            split_pair(beside(*densities)), split_pair(beside(*charged) * (1.0 / cols)), (1, 1))
        proj[...] = through(scaled.reshape(levels * nvec, LANES), astern, (1, 1)).reshape(levels, nvec, LANES)
        for first_t in range(0, nb // 2, group):
            sums_t = [None] * group
            for l in range(levels):
                for u in range(group):
                    term = pairs[first_t + u, l:l + 1, :] * proj[l]
                    sums_t[u] = term if l == 0 else sums_t[u] + term
            for u in range(group):
                moved[first_t + u] = sums_t[u]
        landed(base_slot, arrivals.at[4])
        gram_slots[seat] = (
            base_send[...] + base_slot[...] + pack(jnp.concatenate([gram] * nc, axis=1)))
        start_all(gram_copy, leading[:2])

        blocks = beside(*[
            jnp.where(at // nvec == to // width, jnp.concatenate([charge] * (LANES // nvec), axis=0), 0.0)
            for charge in charged])
        whole = dot(exchange, above(*split_pair(blocks)), (1, 1))
        for first_t in range(nb // 2, nb, group):
            sums_t = [None] * group
            for l in range(levels):
                for u in range(group):
                    term = pairs[first_t + u, l:l + 1, :] * proj[l]
                    sums_t[u] = term if l == 0 else sums_t[u] + term
            for u in range(group):
                moved[first_t + u] = sums_t[u]
        placed = jnp.concatenate(
            [jnp.concatenate([moved[j * nc + c] for c in range(nc)], axis=0) for j in range(nv)], axis=1)
        whole = whole + dot(select[:, 0:nv * LANES], above(*split_pair(placed)), (1, 1))
        whole = whole[:, 0:LANES] + whole[:, LANES:]
        out_send[...] = whole.reshape(count, 8, LANES)
        start_all(out_copy, leading)
        start_all(gram_copy, leading[2:])
        out_slots[seat] = out_send[me]

    def each(run):
        @pl.when(host)
        def _():
            run(hosts - 1)

        @pl.when(guest)
        def _():
            run(hosts)

    each(lambda n: landed(gram_slots.at[0:n], arrivals.at[3]))
    sums = jnp.sum(gram_slots[...], axis=0) * (1.0 / (total * nb))
    turns = [sums] + [pltpu.roll(sums, b * nvec, 1) for b in range(1, nc)]
    for b in range(nc):
        alpha_ref[b * 8:b * 8 + 8] = turns[(-b) % nc][:, 0:nvec]
    mixed = jnp.concatenate(
        [jnp.where(lane8 // nvec == q, turns[(q - b) % nc], 0.0) for q in range(nc) for b in range(nc)], axis=0)
    high, low = split_pair(mixed)
    rest = lifted - dot(own_low, high, (1, 0)) - dot(own_low, low, (1, 0))

    each(lambda n: landed(out_slots.at[0:n], arrivals.at[2]))
    residual = rest + jnp.sum(out_slots[...], axis=0)
    for j in range(nv):
        out_ref[:, j * LANES:(j + 1) * LANES] = jnp.concatenate(
            [residual[k * nv + j:k * nv + j + 1] for k in range(nk)], axis=0)

    def drain(n):
        landed(slots.at[0:n, 0:18], sends.at[0])
        landed(px_slots.at[0:n], sends.at[1])

    each(drain)

    @pl.when(guest)
    def _():
        landed(base_slot, sends.at[4])

    @pl.when(host)
    def _():
        landed(out_send.at[0:count - 1], sends.at[2])
        landed(out_send.at[0:count - 1], sends.at[3])


def finish(out_ref, alpha_ref, out_hbm, alpha_hbm, sems):
    copies = [
        pltpu.make_async_copy(src, dst, sems.at[at])
        for at, (src, dst) in enumerate(((out_ref, out_hbm), (alpha_ref, alpha_hbm)))]
    for copy in copies:
        copy.start()
    for copy in copies:
        copy.wait()


def fast_on_device(pair_exchange, conduction, valence, coulomb, screening, energies, vectors, k_coords):
    nk, nb, planes = pair_exchange.shape
    nv, nc = valence.shape[1], conduction.shape[1]
    nvec = vectors.shape[1] // nb
    rows, cols = lax.axis_size("row"), lax.axis_size("col")
    count = rows * cols
    total = nk * count
    hosts = count // 2
    width = LANES // cols
    spans = planes // hosts // width
    levels = spans * width // 2
    vmem = pl.BlockSpec(memory_space=pltpu.VMEM)
    dma = pltpu.SemaphoreType.DMA
    results = pl.pallas_call(
        functools.partial(kernel, (rows, cols, nk, nv, nc, nvec, total)),
        out_shape=(
            pltpu.VMEM((nk, nb * nvec), F32),
            pltpu.VMEM((nvec, nvec), F32),
        ),
        in_specs=[pl.BlockSpec(memory_space=pl.ANY)] * 8,
        out_specs=(vmem, vmem),
        scratch_shapes=[
            pltpu.VMEM(pair_exchange.shape, BF16),
            pltpu.VMEM(conduction.shape, BF16),
            pltpu.VMEM(valence.shape, BF16),
            pltpu.VMEM((1, LANES), F32),
            pltpu.VMEM((screening.shape[0], LANES), F32),
            pltpu.VMEM(vectors.shape, BF16),
            pltpu.SMEM(energies.shape, F32),
            pltpu.SMEM(k_coords.shape, jnp.int32),
            dma((8,)),
            pltpu.VMEM((hosts, 32, LANES), BF16),
            pltpu.VMEM((count, 32, LANES), BF16),
            pltpu.VMEM((hosts, 16, LANES), BF16),
            pltpu.VMEM((count, 16, LANES), BF16),
            pltpu.VMEM((count * 8, (nv + spans) * LANES), BF16),
            pltpu.VMEM((LANES, count * 8), BF16),
            pltpu.VMEM((LANES, LANES), F32),
            pltpu.VMEM((nb, levels, LANES), F32),
            pltpu.VMEM((nb, nvec, LANES), F32),
            pltpu.VMEM((levels, nvec, LANES), F32),
            pltpu.VMEM((count, 8, LANES), F32),
            pltpu.VMEM((hosts, 8, LANES), F32),
            pltpu.VMEM((hosts, 8, LANES), F32),
            pltpu.VMEM((8, LANES), F32),
            pltpu.VMEM((8, LANES), F32),
            dma((5,)), dma((5,)),
        ],
        compiler_params=pltpu.CompilerParams(collective_id=0, has_side_effects=True),
    )(pair_exchange, conduction, valence, coulomb.reshape(1, planes), screening, vectors, energies, k_coords)
    return pl.pallas_call(
        finish,
        out_shape=(jax.ShapeDtypeStruct((nk, nb * nvec), F32), jax.ShapeDtypeStruct((nvec, nvec), F32)),
        in_specs=[vmem, vmem],
        out_specs=(pl.BlockSpec(memory_space=pl.ANY), pl.BlockSpec(memory_space=pl.ANY)),
        scratch_shapes=[dma((2,))],
    )(*[pltpu.with_memory_space_constraint(result, pltpu.VMEM) for result in results])


highest = lax.Precision.HIGHEST


def pair_factors(conduction, valence):
    count, valence_count, plane_count = valence.shape
    joined = (
        valence.astype(jnp.float32)[:, :, None, :] * conduction.astype(jnp.float32)[:, None, :, :]
    )
    return joined.reshape(count, valence_count * conduction.shape[1], plane_count).astype(
        jnp.bfloat16
    )


def transfer_index(rows_at, cols_at, mesh_cols):
    delta_first = jnp.mod(rows_at[:, None, 0] - cols_at[None, :, 0], MX)
    delta_second = jnp.mod(rows_at[:, None, 1] - cols_at[None, :, 1], mesh_cols)
    fold_first = jnp.minimum(delta_first, MX - delta_first)
    fold_second = jnp.minimum(delta_second, mesh_cols - delta_second)
    return (fold_first * (mesh_cols // 2 + 1) + fold_second).astype(jnp.int32)


def on_device(pair_exchange, conduction, valence, coulomb, screening, energies, vectors, k_coords):
    local_count, band_count, plane_count = pair_exchange.shape
    vector_count = vectors.shape[1] // band_count
    row_count = lax.axis_size("row")
    col_count = lax.axis_size("col")
    total_count = local_count * row_count * col_count
    mesh_cols = total_count // MX
    moving = vectors.reshape(local_count, band_count, vector_count)
    partial_density = jnp.einsum(
        "ktg,ktn->gn", pair_exchange, moving, preferred_element_type=jnp.float32
    )
    density = lax.psum(partial_density, ("row", "col"))
    block_size = 128
    sweeps = plane_count // block_size
    col_cond, col_val, col_vec, col_at = (
        lax.all_gather(conduction, "row", axis=0, tiled=True),
        lax.all_gather(valence, "row", axis=0, tiled=True),
        lax.all_gather(vectors, "row", axis=0, tiled=True),
        lax.all_gather(k_coords, "row", axis=0, tiled=True),
    )
    row_cond, row_val, row_at = (
        lax.all_gather(conduction, "col", axis=0, tiled=True),
        lax.all_gather(valence, "col", axis=0, tiled=True),
        lax.all_gather(k_coords, "col", axis=0, tiled=True),
    )
    row_pairs = pair_factors(row_cond, row_val)
    col_pairs = pair_factors(col_cond, col_val)
    indices = transfer_index(row_at, col_at, mesh_cols)
    col_moving = col_vec.reshape(-1, band_count, vector_count)

    def square_sweep(sweep_index, running):
        anchor = sweep_index * block_size
        coupling = jnp.take(
            lax.dynamic_slice_in_dim(screening, anchor, block_size, 1), indices, axis=0
        )
        row_block = lax.dynamic_slice_in_dim(row_pairs, anchor, block_size, 2)
        col_block = lax.dynamic_slice_in_dim(col_pairs, anchor, block_size, 2)
        col_proj = jnp.einsum(
            "ktg,ktn->kng", col_block, col_moving, preferred_element_type=jnp.float32
        )
        potential = jnp.einsum("ijg,jng->ing", coupling, col_proj, precision=highest)
        return running + jnp.einsum(
            "ktg,kng->ktn", row_block.astype(jnp.float32), potential, precision=highest
        )

    forward = lax.fori_loop(
        0,
        sweeps,
        square_sweep,
        jnp.zeros((row_pairs.shape[0], band_count, vector_count), jnp.float32),
    )
    owned = lax.psum_scatter(
        forward.reshape(col_count, local_count, band_count, vector_count),
        "col",
        scatter_dimension=0,
        tiled=True,
    )[0]
    moving_wide = moving.astype(jnp.float32)
    exchange_term = jnp.einsum(
        "ktg,gn->ktn", pair_exchange.astype(jnp.float32) * coulomb, density, precision=highest
    )
    applied = (
        energies[:, :, None] * moving_wide
        + 2.0 / (total_count * band_count) * exchange_term
        - owned / total_count
    )
    gram = jnp.einsum("ktm,ktn->mn", moving_wide, applied, precision=highest)
    alpha = lax.psum(gram, ("row", "col")) / (total_count * band_count)
    residual = applied - jnp.einsum("ktm,mn->ktn", moving_wide, alpha, precision=highest)
    return (residual.reshape(local_count, band_count * vector_count), alpha)


def fits(args, mesh):
    pair_exchange, conduction, valence, _, screening, _, vectors, _ = args
    rows, cols = mesh.shape["row"], mesh.shape["col"]
    points, nb, planes = pair_exchange.shape
    nk = points // (rows * cols)
    nv, nc = valence.shape[1], conduction.shape[1]
    nvec = vectors.shape[1] // nb
    return (
        planes == rows * LANES and rows == 8 and cols == 4 and rows * cols * nk * 2 == LANES and nk == 2 and nv == 4 and nc == 4
        and nc * nvec == LANES and points == 2 * MX and screening.shape[0] == MX + 2
    )


def solution(mesh):
    in_specs = (
        P(("row", "col"), None, None),
        P(("row", "col"), None, None),
        P(("row", "col"), None, None),
        P(),
        P(),
        P(("row", "col"), None),
        P(("row", "col"), None),
        P(("row", "col"), None),
    )
    out_specs = (P(("row", "col"), None), P())

    def run(*args):
        body = fast_on_device if fits(args, mesh) else on_device
        return jax.shard_map(
            body, mesh=mesh, in_specs=in_specs, out_specs=out_specs, check_vma=False
        )(*args)

    return run
```

```python
import functools
import math

import jax
import jax.numpy as jnp
from jax import lax
from jax.experimental import pallas as pl
from jax.experimental.pallas import tpu as pltpu
from jax.sharding import PartitionSpec as P

MX = 32
LANES = 128
MESH = pl.DeviceIdType.MESH
F32 = jnp.float32
BF16 = jnp.bfloat16


def split_pair(value):
    high = value.astype(BF16)
    return high, (value - high.astype(F32)).astype(BF16)


def dot(a, b, contract):
    return lax.dot_general(a, b, ((contract[0:1], contract[1:2]), ((), ())), preferred_element_type=F32)


def iota(shape, axis):
    return lax.broadcasted_iota(jnp.int32, shape, axis)


def one_hot(condition):
    return jnp.where(condition, 1.0, 0.0).astype(BF16)


def wide_dot(a, b, contract):
    high, low = a
    main, rest = b
    return dot(high, main, contract) + dot(low, main, contract) + dot(high, rest, contract)


def beside(*parts):
    return jnp.concatenate(parts, axis=1)


def above(*parts):
    return jnp.concatenate(parts, axis=0)


def swap_blocks(tile, lanes, rows):
    row_bit = (iota(tile.shape, 0) // rows) % 2
    lane_bit = (iota(tile.shape, 1) // lanes) % 2
    up = pltpu.roll(pltpu.roll(tile, lanes, 1), tile.shape[0] - rows, 0)
    down = pltpu.roll(pltpu.roll(tile, LANES - lanes, 1), rows, 0)
    return jnp.where(row_bit == lane_bit, tile, jnp.where(lane_bit == 1, up, down))


def fold_blocks(square, width):
    kept = jnp.where(iota(square.shape, 0) // width == iota(square.shape, 1) // width, square, 0.0)
    rows = kept[0:width]
    for at in range(width, square.shape[0], width):
        rows = rows + kept[at:at + width]
    half = rows + pltpu.roll(rows, LANES // 2, 1)
    return half + pltpu.roll(half, LANES // 4, 1)


def basis(phase, sign):
    angle = (phase % MX).astype(F32) * (2.0 * math.pi / MX)
    return (jnp.cos(angle) + jnp.sin(angle)) * (1 - 2 * (sign % 2)).astype(F32)


def kernel(
    dims, px_hbm, cond_hbm, val_hbm, coulomb_hbm, screening_hbm, vec_hbm, energy_hbm, place_hbm,
    out_ref, alpha_ref,
    px_ref, cond_ref, val_ref, coulomb_ref, screening_ref, vec_ref, energy_ref, place_ref,
    load_sem, msg_ref, slots, px_msg, px_slots, select, select_q, lam, pairs, moved, proj, out_send, out_slots, gram_slots,
    base_send, base_slot, sends, arrivals,
):
    rows, cols, nk, nv, nc, nvec, total = dims
    row, col = lax.axis_index("row"), lax.axis_index("col")
    me = row * cols + col
    count = rows * cols
    nb = nv * nc
    low_row, high_row = rows // 4, rows - rows // 4
    hosts = (high_row - low_row) * cols
    host = (row >= low_row) & (row < high_row)
    guest = jnp.logical_not(host)
    near_row = jnp.where(row < low_row, row + low_row, jnp.where(row >= high_row, row - low_row, row))
    seat = (near_row - low_row) * cols + col
    width = LANES // cols
    deep = width // 2
    unit = nk * nv
    half = LANES // 2
    sheets = count * 8
    spans = rows * LANES // hosts // width
    levels = spans * deep

    ring_rows = [row] + [lax.rem(row + step, rows) for step in range(1, rows)]
    ring_cols = [col] + [lax.rem(col + step, cols) for step in range(1, cols)]
    everyone = [(pr, pc) for i, pr in enumerate(ring_rows) for j, pc in enumerate(ring_cols) if i + j]
    signalled = [
        (jnp.where(me == at, rows - 1, at // cols), jnp.where(me == at, cols - 1, at % cols)) for at in range(count - 1)]
    host_rows = [low_row + lax.rem(near_row - low_row + step, high_row - low_row) for step in range(high_row - low_row)]
    left = lax.rem(col, 2)
    host_cols = [cols - 1 - col, lax.rem(col + 2, cols), col + 1 - 2 * left, col]
    host_peers = [(pr, pc) for pc in host_cols for pr in host_rows[::-1]]

    barrier = pltpu.get_barrier_semaphore()
    mine = pl.ds(pl.multiple_of(seat // 2 * LANES, LANES), LANES)
    loads = [
        pltpu.make_async_copy(src, dst, load_sem.at[at])
        for at, (src, dst) in enumerate((
            (val_hbm, val_ref), (cond_hbm, cond_ref), (vec_hbm, vec_ref), (place_hbm, place_ref), (px_hbm, px_ref),
            (energy_hbm, energy_ref), (screening_hbm.at[:, mine], screening_ref), (coulomb_hbm.at[:, mine], coulomb_ref)))
    ]
    for load in loads[:4]:
        load.start()

    @pl.when(host)
    def _():
        for peer in signalled:
            pl.semaphore_signal(barrier, inc=1, device_id=peer, device_id_type=MESH)

    for load in loads[4:]:
        load.start()
    row8 = iota((8, LANES), 0)
    lane8 = iota((8, LANES), 1)
    for load in loads[:4]:
        load.wait()

    vec = vec_ref[...].astype(F32)
    own = jnp.concatenate(
        [vec[k:k + 1, j * LANES:(j + 1) * LANES] for k in range(nk) for j in range(nv)], axis=0)
    tail = jnp.zeros((8, LANES), F32)
    wave = lane8 % half
    for k in range(nk):
        value = basis((wave // 2) * place_ref[k, 0], (wave % 2) * place_ref[k, 1])
        high = value.astype(BF16).astype(F32)
        tail = jnp.where(row8 == k, jnp.where(lane8 < half, high, value - high), tail)
    tail = above(tail, jnp.zeros((8, LANES), F32)).astype(BF16)
    for r in range(rows):
        span = slice(r * LANES, (r + 1) * LANES)
        turned = []
        for k in range(nk):
            tile = above(val_ref[k, :, span].astype(F32), cond_ref[k, :, span].astype(F32))
            for size in (4, 2, 1):
                tile = swap_blocks(tile, deep * size, size)
            turned.append(tile)
        flipped = [pltpu.roll(tile, 4, 0) for tile in turned]
        first_half = jnp.where(row8 < 4, turned[0], flipped[1])
        other_half = jnp.where(row8 < 4, flipped[0], turned[1])
        for q, low in enumerate((first_half, other_half)):
            msg_ref[r * 2 + q, 0:16] = above(own, low).astype(BF16)
            msg_ref[r * 2 + q, 16:32] = tail

    loads[4].wait()
    at = iota((nk * nb, nk * nb), 0)
    to = iota((nk * nb, nk * nb), 1)
    order = one_hot(to == (at % unit) // nv * nb + at % nv * nc + at // unit)
    arranged = dot(order, px_ref[...].reshape(nk * nb, px_ref.shape[2]), (1, 0))
    for r in range(rows):
        span = slice(r * LANES, (r + 1) * LANES)
        tiles = []
        for q in range(cols):
            tile = arranged[q * 8:q * 8 + 8, span]
            for b in range(cols):
                if b != q:
                    moving = pltpu.roll(arranged[b * 8:b * 8 + 8, span], (width * (b - q)) % LANES, 1)
                    tile = jnp.where(lane8 // width == b, moving, tile)
            tiles.append(tile)
        for q in range(2):
            px_msg[r * 2 + q] = above(tiles[2 * q], tiles[2 * q + 1]).astype(BF16)
    @pl.when(host)
    def _():
        pl.semaphore_wait(barrier, hosts - 1)

    @pl.when(guest)
    def _():
        pl.semaphore_wait(barrier, hosts)

    def main_copy(device):
        peer = (device[0] - low_row) * cols + device[1]
        return pltpu.make_async_remote_copy(
            src_ref=msg_ref.at[peer, 0:18], dst_ref=slots.at[me, 0:18],
            send_sem=sends.at[0], recv_sem=arrivals.at[0], device_id=device, device_id_type=MESH)

    def px_copy(device):
        peer = (device[0] - low_row) * cols + device[1]
        return pltpu.make_async_remote_copy(
            src_ref=px_msg.at[peer], dst_ref=px_slots.at[me],
            send_sem=sends.at[1], recv_sem=arrivals.at[1], device_id=device, device_id_type=MESH)

    def out_copy(device):
        peer = device[0] * cols + device[1]
        return pltpu.make_async_remote_copy(
            src_ref=out_send.at[peer], dst_ref=out_slots.at[seat],
            send_sem=sends.at[2], recv_sem=arrivals.at[2], device_id=device, device_id_type=MESH)

    def gram_copy(device):
        return pltpu.make_async_remote_copy(
            src_ref=gram_slots.at[seat], dst_ref=gram_slots.at[seat],
            send_sem=sends.at[3], recv_sem=arrivals.at[3], device_id=device, device_id_type=MESH)

    def base_copy():
        return pltpu.make_async_remote_copy(
            src_ref=base_send, dst_ref=base_slot,
            send_sem=sends.at[4], recv_sem=arrivals.at[4], device_id=(near_row, col), device_id_type=MESH)

    def start_all(copy, targets):
        for peer in targets:
            copy(peer).start()

    def pack(block):
        piece = block[0:8]
        for b in range(1, nc):
            piece = jnp.where(lane8 // nvec == b, block[b * 8:b * 8 + 8], piece)
        return piece

    def landed(ref, sem):
        pltpu.make_async_copy(ref, ref, sem).wait()

    def to_hosts(copy, here, there):
        start_all(copy, host_peers[:-1])

        @pl.when(guest)
        def _():
            copy(host_peers[-1]).start()

        @pl.when(host)
        def _():
            there[me] = here[seat]

    to_hosts(main_copy, msg_ref, slots)

    to_hosts(px_copy, px_msg, px_slots)

    loads[5].wait()
    energy = jnp.zeros((8, LANES), F32)
    for k in range(nk):
        for t in range(nb):
            energy = jnp.where((row8 == k * nv + t // nc) & (lane8 // nvec == t % nc), energy_ref[k, t], energy)
    lifted = energy * own
    high, low = split_pair(lifted)
    own_low = own.astype(BF16)
    base_send[...] = pack(fold_blocks(dot(own_low, high, (0, 0)) + dot(own_low, low, (0, 0)), nvec))

    @pl.when(guest)
    def _():
        base_copy().start()

    for load in loads[6:]:
        load.wait()

    @pl.when(host)
    def _():
        late = jnp.logical_and(col == 0, row < 2)
        rank = jnp.where(late, 0, me - 1 - (me > cols).astype(jnp.int32))

        def turned_to(step):
            at = rank + step
            at = jnp.where(at >= count - 2, at - (count - 2), at)
            spot = at + 1 + (at >= cols - 1).astype(jnp.int32)
            return spot // cols, lax.rem(spot, cols)

        leading = [(0, 0), (1, 0)] + [turned_to(step) for step in range(1, count - 2)]
        at = iota((sheets, LANES), 0)
        to = iota((sheets, LANES), 1)
        same = at // 8 == (to % half) // nk
        place = at % 8
        for j in range(nv):
            select[:, j * LANES:(j + 1) * LANES] = one_hot(same & (place == to % nk * nv + j))
        for a in range(spans):
            select[:, (nv + a) * LANES:(nv + a + 1) * LANES] = one_hot(
                same & (place == to % nk * 2 * spans + 2 * a + to // half))
        at = iota((LANES, sheets), 0)
        to = iota((LANES, sheets), 1)
        select_q[...] = one_hot((to // 8 == (at % half) // nk) & (to % 8 == at % nk))
        at = iota((LANES, LANES), 0)
        to = iota((LANES, LANES), 1)
        fold = at // 2
        angle = ((fold * ((to % half) // 2)) % MX).astype(F32) * (2.0 * math.pi / MX)
        weight = jnp.where((fold == 0) | (fold == MX // 2), 1.0, 2.0) * (1 - 2 * ((at % 2) * (to % 2))).astype(F32)
        table = jnp.where(fold <= MX // 2, jnp.cos(angle) * weight, 0.0)
        screened = above(screening_ref[...], jnp.zeros((LANES - screening_ref.shape[0], LANES), F32))
        lam[...] = wide_dot(split_pair(screened), split_pair(table), (0, 0)) * (-1.0 / (total * total))
        second_half = lax.rem(seat, 2)
        band = lam[pl.ds(pl.multiple_of(second_half * half, 8), half), :]
        lane_d = iota((deep, LANES), 1)
        spectrum = above(*[
            jnp.where(lane_d < half, band[2 * a * deep:(2 * a + 1) * deep], band[(2 * a + 1) * deep:(2 * a + 2) * deep])
            for a in range(spans)])
        raw = jnp.broadcast_to(coulomb_ref[...], (width, LANES)) * (2.0 / (total * nb))
        lane_w = iota((width, LANES), 1)
        charges = []
        for a in range(spans):
            tiles = jnp.zeros((width, LANES), F32)
            for b in range(cols):
                for q in range(2):
                    shift = (width * (b - 2 * q - a)) % LANES
                    moving = raw if shift == 0 else pltpu.roll(raw, shift, 1)
                    tiles = jnp.where((lane_w // width == b) & (second_half == q), moving, tiles)
            charges.append(tiles)

        landed(slots.at[0:count - 1, 0:18], arrivals.at[0])
        got = slots[...].astype(F32)
        own_all, rest_all, wave_all = [
            got[:, 8 * part:8 * part + 8].reshape(sheets, LANES) for part in range(3)]
        own_all, rest_all = own_all.astype(BF16), rest_all.astype(BF16)
        wave_all = jnp.where(iota((sheets, LANES), 0) % 8 < nk, wave_all, 0.0).astype(BF16)
        factors = dot(rest_all, select[:, nv * LANES:], (0, 0))
        spread = dot(own_all, select[:, 0:nv * LANES], (0, 0))
        for v in range(nv):
            for c in range(nc):
                for a in range(spans):
                    lanes = slice(a * LANES, (a + 1) * LANES)
                    joined = (
                        factors[v * deep:(v + 1) * deep, lanes] * factors[half + c * deep:half + (c + 1) * deep, lanes])
                    pairs[v * nc + c, a * deep:(a + 1) * deep] = joined.astype(BF16).astype(F32)
        for t in range(nb):
            moved[t] = spread[t % nc * nvec:(t % nc + 1) * nvec, t // nc * LANES:(t // nc + 1) * LANES]
        waves = dot(select_q[...], wave_all, (1, 0))
        crossed = pltpu.roll(waves, half, 1)
        first = (at < half) & (to < half)
        second = (at >= half) & (to >= half)
        main = jnp.where(first, waves, jnp.where(second, crossed, 0.0)).astype(BF16)
        fine = jnp.where(first, crossed, jnp.where(second, waves, 0.0)).astype(BF16)
        none = jnp.zeros((LANES, LANES), BF16)
        ahead = above(beside(main, fine), beside(main, none))
        astern = above(beside(main, main), beside(fine, none))

        def through(values, weights, contract):
            both = dot(beside(*split_pair(values)), weights, contract)
            return both[:, 0:LANES] + both[:, LANES:]

        def unfold(first_j, last_j):
            placed = beside(*[above(*[moved[j * nc + c] for c in range(nc)]) for j in range(first_j, last_j)])
            return dot(select[:, first_j * LANES:last_j * LANES], above(*split_pair(placed)), (1, 1))

        group = 2
        for first_l in range(0, levels, group):
            sums_l = [None] * group
            for t in range(nb):
                for u in range(group):
                    term = pairs[t, first_l + u:first_l + u + 1, :] * moved[t]
                    sums_l[u] = term if t == 0 else sums_l[u] + term
            for u in range(group):
                proj[first_l + u] = sums_l[u]
        spectral = through(proj[...].reshape(levels * nvec, LANES), ahead, (1, 0)).reshape(levels, nvec, LANES)
        scaled = spectral * spectrum[:, None, :]
        sides = [
            split_pair(jnp.concatenate([side[l] for l in range(levels)], axis=1)) for side in (spectral, scaled)]
        gram = wide_dot(*sides, (1, 1))

        landed(px_slots.at[0:count - 1], arrivals.at[1])
        taken_px = px_slots[...].astype(F32)
        exchange = beside(*[
            taken_px[:, 8 * a:8 * a + 8].reshape(sheets, LANES).astype(BF16) for a in range(spans)])
        crowd = dot(own_all, exchange, (0, 0))
        densities = [fold_blocks(crowd[:, a * LANES:(a + 1) * LANES], nvec) for a in range(spans)]
        charged = [density * charge for density, charge in zip(densities, charges)]
        gram = gram + wide_dot(
            split_pair(beside(*densities)), split_pair(beside(*charged) * (1.0 / cols)), (1, 1))
        proj[...] = through(scaled.reshape(levels * nvec, LANES), astern, (1, 1)).reshape(levels, nvec, LANES)
        for first_t in range(0, nb // 2, group):
            sums_t = [None] * group
            for l in range(levels):
                for u in range(group):
                    term = pairs[first_t + u, l:l + 1, :] * proj[l]
                    sums_t[u] = term if l == 0 else sums_t[u] + term
            for u in range(group):
                moved[first_t + u] = sums_t[u]
        landed(base_slot, arrivals.at[4])
        gram_slots[seat] = (
            base_send[...] + base_slot[...] + pack(jnp.concatenate([gram] * nc, axis=1)))
        start_all(gram_copy, leading[:2])

        blocks = beside(*[
            jnp.where(at // nvec == to // width, jnp.concatenate([charge] * (LANES // nvec), axis=0), 0.0)
            for charge in charged])
        whole = dot(exchange, above(*split_pair(blocks)), (1, 1))
        early = unfold(0, nv // 2)
        for first_t in range(nb // 2, nb - nc, group):
            sums_t = [None] * group
            for l in range(levels):
                for u in range(group):
                    term = pairs[first_t + u, l:l + 1, :] * proj[l]
                    sums_t[u] = term if l == 0 else sums_t[u] + term
            for u in range(group):
                moved[first_t + u] = sums_t[u]
        early = early + unfold(nv // 2, nv - 1)
        for first_t in range(nb - nc, nb, group):
            sums_t = [None] * group
            for l in range(levels):
                for u in range(group):
                    term = pairs[first_t + u, l:l + 1, :] * proj[l]
                    sums_t[u] = term if l == 0 else sums_t[u] + term
            for u in range(group):
                moved[first_t + u] = sums_t[u]
        whole = whole + early + unfold(nv - 1, nv)
        whole = whole[:, 0:LANES] + whole[:, LANES:]
        out_send[...] = whole.reshape(count, 8, LANES)
        start_all(out_copy, leading)
        start_all(gram_copy, leading[2:])
        out_slots[seat] = out_send[me]

    def each(run):
        @pl.when(host)
        def _():
            run(hosts - 1)

        @pl.when(guest)
        def _():
            run(hosts)

    each(lambda n: landed(gram_slots.at[0:n], arrivals.at[3]))
    sums = jnp.sum(gram_slots[...], axis=0) * (1.0 / (total * nb))
    turns = [sums] + [pltpu.roll(sums, b * nvec, 1) for b in range(1, nc)]
    for b in range(nc):
        alpha_ref[b * 8:b * 8 + 8] = turns[(-b) % nc][:, 0:nvec]
    mixed = jnp.concatenate(
        [jnp.where(lane8 // nvec == q, turns[(q - b) % nc], 0.0) for q in range(nc) for b in range(nc)], axis=0)
    high, low = split_pair(mixed)
    rest = lifted - dot(own_low, high, (1, 0)) - dot(own_low, low, (1, 0))

    each(lambda n: landed(out_slots.at[0:n], arrivals.at[2]))
    residual = rest + jnp.sum(out_slots[...], axis=0)
    for j in range(nv):
        out_ref[:, j * LANES:(j + 1) * LANES] = jnp.concatenate(
            [residual[k * nv + j:k * nv + j + 1] for k in range(nk)], axis=0)

    def drain(n):
        landed(slots.at[0:n, 0:18], sends.at[0])
        landed(px_slots.at[0:n], sends.at[1])

    each(drain)

    @pl.when(guest)
    def _():
        landed(base_slot, sends.at[4])

    @pl.when(host)
    def _():
        landed(out_send.at[0:count - 1], sends.at[2])
        landed(out_send.at[0:count - 1], sends.at[3])


def finish(out_ref, alpha_ref, out_hbm, alpha_hbm, sems):
    copies = [
        pltpu.make_async_copy(src, dst, sems.at[at])
        for at, (src, dst) in enumerate(((out_ref, out_hbm), (alpha_ref, alpha_hbm)))]
    for copy in copies:
        copy.start()
    for copy in copies:
        copy.wait()


def fast_on_device(pair_exchange, conduction, valence, coulomb, screening, energies, vectors, k_coords):
    nk, nb, planes = pair_exchange.shape
    nv, nc = valence.shape[1], conduction.shape[1]
    nvec = vectors.shape[1] // nb
    rows, cols = lax.axis_size("row"), lax.axis_size("col")
    count = rows * cols
    total = nk * count
    hosts = count // 2
    width = LANES // cols
    spans = planes // hosts // width
    levels = spans * width // 2
    vmem = pl.BlockSpec(memory_space=pltpu.VMEM)
    dma = pltpu.SemaphoreType.DMA
    results = pl.pallas_call(
        functools.partial(kernel, (rows, cols, nk, nv, nc, nvec, total)),
        out_shape=(
            pltpu.VMEM((nk, nb * nvec), F32),
            pltpu.VMEM((nvec, nvec), F32),
        ),
        in_specs=[pl.BlockSpec(memory_space=pl.ANY)] * 8,
        out_specs=(vmem, vmem),
        scratch_shapes=[
            pltpu.VMEM(pair_exchange.shape, BF16),
            pltpu.VMEM(conduction.shape, BF16),
            pltpu.VMEM(valence.shape, BF16),
            pltpu.VMEM((1, LANES), F32),
            pltpu.VMEM((screening.shape[0], LANES), F32),
            pltpu.VMEM(vectors.shape, BF16),
            pltpu.SMEM(energies.shape, F32),
            pltpu.SMEM(k_coords.shape, jnp.int32),
            dma((8,)),
            pltpu.VMEM((hosts, 32, LANES), BF16),
            pltpu.VMEM((count, 32, LANES), BF16),
            pltpu.VMEM((hosts, 16, LANES), BF16),
            pltpu.VMEM((count, 16, LANES), BF16),
            pltpu.VMEM((count * 8, (nv + spans) * LANES), BF16),
            pltpu.VMEM((LANES, count * 8), BF16),
            pltpu.VMEM((LANES, LANES), F32),
            pltpu.VMEM((nb, levels, LANES), F32),
            pltpu.VMEM((nb, nvec, LANES), F32),
            pltpu.VMEM((levels, nvec, LANES), F32),
            pltpu.VMEM((count, 8, LANES), F32),
            pltpu.VMEM((hosts, 8, LANES), F32),
            pltpu.VMEM((hosts, 8, LANES), F32),
            pltpu.VMEM((8, LANES), F32),
            pltpu.VMEM((8, LANES), F32),
            dma((5,)), dma((5,)),
        ],
        compiler_params=pltpu.CompilerParams(collective_id=0, has_side_effects=True),
    )(pair_exchange, conduction, valence, coulomb.reshape(1, planes), screening, vectors, energies, k_coords)
    return pl.pallas_call(
        finish,
        out_shape=(jax.ShapeDtypeStruct((nk, nb * nvec), F32), jax.ShapeDtypeStruct((nvec, nvec), F32)),
        in_specs=[vmem, vmem],
        out_specs=(pl.BlockSpec(memory_space=pl.ANY), pl.BlockSpec(memory_space=pl.ANY)),
        scratch_shapes=[dma((2,))],
    )(*[pltpu.with_memory_space_constraint(result, pltpu.VMEM) for result in results])


highest = lax.Precision.HIGHEST


def pair_factors(conduction, valence):
    count, valence_count, plane_count = valence.shape
    joined = (
        valence.astype(jnp.float32)[:, :, None, :] * conduction.astype(jnp.float32)[:, None, :, :]
    )
    return joined.reshape(count, valence_count * conduction.shape[1], plane_count).astype(
        jnp.bfloat16
    )


def transfer_index(rows_at, cols_at, mesh_cols):
    delta_first = jnp.mod(rows_at[:, None, 0] - cols_at[None, :, 0], MX)
    delta_second = jnp.mod(rows_at[:, None, 1] - cols_at[None, :, 1], mesh_cols)
    fold_first = jnp.minimum(delta_first, MX - delta_first)
    fold_second = jnp.minimum(delta_second, mesh_cols - delta_second)
    return (fold_first * (mesh_cols // 2 + 1) + fold_second).astype(jnp.int32)


def on_device(pair_exchange, conduction, valence, coulomb, screening, energies, vectors, k_coords):
    local_count, band_count, plane_count = pair_exchange.shape
    vector_count = vectors.shape[1] // band_count
    row_count = lax.axis_size("row")
    col_count = lax.axis_size("col")
    total_count = local_count * row_count * col_count
    mesh_cols = total_count // MX
    moving = vectors.reshape(local_count, band_count, vector_count)
    partial_density = jnp.einsum(
        "ktg,ktn->gn", pair_exchange, moving, preferred_element_type=jnp.float32
    )
    density = lax.psum(partial_density, ("row", "col"))
    block_size = 128
    sweeps = plane_count // block_size
    col_cond, col_val, col_vec, col_at = (
        lax.all_gather(conduction, "row", axis=0, tiled=True),
        lax.all_gather(valence, "row", axis=0, tiled=True),
        lax.all_gather(vectors, "row", axis=0, tiled=True),
        lax.all_gather(k_coords, "row", axis=0, tiled=True),
    )
    row_cond, row_val, row_at = (
        lax.all_gather(conduction, "col", axis=0, tiled=True),
        lax.all_gather(valence, "col", axis=0, tiled=True),
        lax.all_gather(k_coords, "col", axis=0, tiled=True),
    )
    row_pairs = pair_factors(row_cond, row_val)
    col_pairs = pair_factors(col_cond, col_val)
    indices = transfer_index(row_at, col_at, mesh_cols)
    col_moving = col_vec.reshape(-1, band_count, vector_count)

    def square_sweep(sweep_index, running):
        anchor = sweep_index * block_size
        coupling = jnp.take(
            lax.dynamic_slice_in_dim(screening, anchor, block_size, 1), indices, axis=0
        )
        row_block = lax.dynamic_slice_in_dim(row_pairs, anchor, block_size, 2)
        col_block = lax.dynamic_slice_in_dim(col_pairs, anchor, block_size, 2)
        col_proj = jnp.einsum(
            "ktg,ktn->kng", col_block, col_moving, preferred_element_type=jnp.float32
        )
        potential = jnp.einsum("ijg,jng->ing", coupling, col_proj, precision=highest)
        return running + jnp.einsum(
            "ktg,kng->ktn", row_block.astype(jnp.float32), potential, precision=highest
        )

    forward = lax.fori_loop(
        0,
        sweeps,
        square_sweep,
        jnp.zeros((row_pairs.shape[0], band_count, vector_count), jnp.float32),
    )
    owned = lax.psum_scatter(
        forward.reshape(col_count, local_count, band_count, vector_count),
        "col",
        scatter_dimension=0,
        tiled=True,
    )[0]
    moving_wide = moving.astype(jnp.float32)
    exchange_term = jnp.einsum(
        "ktg,gn->ktn", pair_exchange.astype(jnp.float32) * coulomb, density, precision=highest
    )
    applied = (
        energies[:, :, None] * moving_wide
        + 2.0 / (total_count * band_count) * exchange_term
        - owned / total_count
    )
    gram = jnp.einsum("ktm,ktn->mn", moving_wide, applied, precision=highest)
    alpha = lax.psum(gram, ("row", "col")) / (total_count * band_count)
    residual = applied - jnp.einsum("ktm,mn->ktn", moving_wide, alpha, precision=highest)
    return (residual.reshape(local_count, band_count * vector_count), alpha)


def fits(args, mesh):
    pair_exchange, conduction, valence, _, screening, _, vectors, _ = args
    rows, cols = mesh.shape["row"], mesh.shape["col"]
    points, nb, planes = pair_exchange.shape
    nk = points // (rows * cols)
    nv, nc = valence.shape[1], conduction.shape[1]
    nvec = vectors.shape[1] // nb
    return (
        planes == rows * LANES and rows == 8 and cols == 4 and rows * cols * nk * 2 == LANES and nk == 2 and nv == 4 and nc == 4
        and nc * nvec == LANES and points == 2 * MX and screening.shape[0] == MX + 2
    )


def solution(mesh):
    in_specs = (
        P(("row", "col"), None, None),
        P(("row", "col"), None, None),
        P(("row", "col"), None, None),
        P(),
        P(),
        P(("row", "col"), None),
        P(("row", "col"), None),
        P(("row", "col"), None),
    )
    out_specs = (P(("row", "col"), None), P())

    def run(*args):
        body = fast_on_device if fits(args, mesh) else on_device
        return jax.shard_map(
            body, mesh=mesh, in_specs=in_specs, out_specs=out_specs, check_vma=False
        )(*args)

    return run
```

```python
import functools
import math

import jax
import jax.numpy as jnp
from jax import lax
from jax.experimental import pallas as pl
from jax.experimental.pallas import tpu as pltpu
from jax.sharding import PartitionSpec as P

MX = 32
LANES = 128
MESH = pl.DeviceIdType.MESH
F32 = jnp.float32
BF16 = jnp.bfloat16


def split_pair(value):
    high = value.astype(BF16)
    return high, (value - high.astype(F32)).astype(BF16)


def dot(a, b, contract):
    return lax.dot_general(a, b, ((contract[0:1], contract[1:2]), ((), ())), preferred_element_type=F32)


def iota(shape, axis):
    return lax.broadcasted_iota(jnp.int32, shape, axis)


def one_hot(condition):
    return jnp.where(condition, 1.0, 0.0).astype(BF16)


def wide_dot(a, b, contract):
    high, low = a
    main, rest = b
    return dot(high, main, contract) + dot(low, main, contract) + dot(high, rest, contract)


def beside(*parts):
    return jnp.concatenate(parts, axis=1)


def above(*parts):
    return jnp.concatenate(parts, axis=0)


def swap_blocks(tile, lanes, rows):
    row_bit = (iota(tile.shape, 0) // rows) % 2
    lane_bit = (iota(tile.shape, 1) // lanes) % 2
    up = pltpu.roll(pltpu.roll(tile, lanes, 1), tile.shape[0] - rows, 0)
    down = pltpu.roll(pltpu.roll(tile, LANES - lanes, 1), rows, 0)
    return jnp.where(row_bit == lane_bit, tile, jnp.where(lane_bit == 1, up, down))


def fold_blocks(square, width):
    kept = jnp.where(iota(square.shape, 0) // width == iota(square.shape, 1) // width, square, 0.0)
    rows = kept[0:width]
    for at in range(width, square.shape[0], width):
        rows = rows + kept[at:at + width]
    half = rows + pltpu.roll(rows, LANES // 2, 1)
    return half + pltpu.roll(half, LANES // 4, 1)


def basis(phase, sign):
    angle = (phase % MX).astype(F32) * (2.0 * math.pi / MX)
    return (jnp.cos(angle) + jnp.sin(angle)) * (1 - 2 * (sign % 2)).astype(F32)


def kernel(
    dims, px_hbm, cond_hbm, val_hbm, coulomb_hbm, screening_hbm, vec_hbm, energy_hbm, place_hbm,
    out_ref, alpha_ref,
    px_ref, cond_ref, val_ref, coulomb_ref, screening_ref, vec_ref, energy_ref, place_ref,
    load_sem, msg_ref, slots, px_msg, px_slots, select, select_q, lam, pairs, moved, proj, out_send, out_slots, gram_slots,
    base_send, base_slot, sends, arrivals,
):
    rows, cols, nk, nv, nc, nvec, total = dims
    row, col = lax.axis_index("row"), lax.axis_index("col")
    me = row * cols + col
    count = rows * cols
    nb = nv * nc
    low_row, high_row = rows // 4, rows - rows // 4
    hosts = (high_row - low_row) * cols
    host = (row >= low_row) & (row < high_row)
    guest = jnp.logical_not(host)
    near_row = jnp.where(row < low_row, row + low_row, jnp.where(row >= high_row, row - low_row, row))
    seat = (near_row - low_row) * cols + col
    width = LANES // cols
    deep = width // 2
    unit = nk * nv
    half = LANES // 2
    sheets = count * 8
    spans = rows * LANES // hosts // width
    levels = spans * deep

    ring_rows = [row] + [lax.rem(row + step, rows) for step in range(1, rows)]
    ring_cols = [col] + [lax.rem(col + step, cols) for step in range(1, cols)]
    everyone = [(pr, pc) for i, pr in enumerate(ring_rows) for j, pc in enumerate(ring_cols) if i + j]
    signalled = [
        (jnp.where(me == at, rows - 1, at // cols), jnp.where(me == at, cols - 1, at % cols)) for at in range(count - 1)]
    host_rows = [low_row + lax.rem(near_row - low_row + step, high_row - low_row) for step in range(high_row - low_row)]
    left = lax.rem(col, 2)
    host_cols = [cols - 1 - col, lax.rem(col + 2, cols), col + 1 - 2 * left, col]
    host_peers = [(pr, pc) for pc in host_cols for pr in host_rows[::-1]]

    barrier = pltpu.get_barrier_semaphore()
    mine = pl.ds(pl.multiple_of(seat // 2 * LANES, LANES), LANES)
    loads = [
        pltpu.make_async_copy(src, dst, load_sem.at[at])
        for at, (src, dst) in enumerate((
            (val_hbm, val_ref), (cond_hbm, cond_ref), (vec_hbm, vec_ref), (place_hbm, place_ref), (px_hbm, px_ref),
            (energy_hbm, energy_ref), (screening_hbm.at[:, mine], screening_ref), (coulomb_hbm.at[:, mine], coulomb_ref)))
    ]
    for load in loads[:4]:
        load.start()

    @pl.when(host)
    def _():
        for peer in signalled:
            pl.semaphore_signal(barrier, inc=1, device_id=peer, device_id_type=MESH)

    for load in loads[4:]:
        load.start()
    row8 = iota((8, LANES), 0)
    lane8 = iota((8, LANES), 1)
    for load in loads[:4]:
        load.wait()

    vec = vec_ref[...].astype(F32)
    own = jnp.concatenate(
        [vec[k:k + 1, j * LANES:(j + 1) * LANES] for k in range(nk) for j in range(nv)], axis=0)
    tail = jnp.zeros((8, LANES), F32)
    wave = lane8 % half
    for k in range(nk):
        value = basis((wave // 2) * place_ref[k, 0], (wave % 2) * place_ref[k, 1])
        high = value.astype(BF16).astype(F32)
        tail = jnp.where(row8 == k, jnp.where(lane8 < half, high, value - high), tail)
    tail = above(tail, jnp.zeros((8, LANES), F32)).astype(BF16)
    for r in range(rows):
        span = slice(r * LANES, (r + 1) * LANES)
        turned = []
        for k in range(nk):
            tile = above(val_ref[k, :, span].astype(F32), cond_ref[k, :, span].astype(F32))
            for size in (4, 2, 1):
                tile = swap_blocks(tile, deep * size, size)
            turned.append(tile)
        flipped = [pltpu.roll(tile, 4, 0) for tile in turned]
        first_half = jnp.where(row8 < 4, turned[0], flipped[1])
        other_half = jnp.where(row8 < 4, flipped[0], turned[1])
        for q, low in enumerate((first_half, other_half)):
            msg_ref[r * 2 + q, 0:16] = above(own, low).astype(BF16)
            msg_ref[r * 2 + q, 16:32] = tail

    loads[4].wait()
    at = iota((nk * nb, nk * nb), 0)
    to = iota((nk * nb, nk * nb), 1)
    order = one_hot(to == (at % unit) // nv * nb + at % nv * nc + at // unit)
    arranged = dot(order, px_ref[...].reshape(nk * nb, px_ref.shape[2]), (1, 0))
    for r in range(rows):
        span = slice(r * LANES, (r + 1) * LANES)
        tiles = []
        for q in range(cols):
            tile = arranged[q * 8:q * 8 + 8, span]
            for b in range(cols):
                if b != q:
                    moving = pltpu.roll(arranged[b * 8:b * 8 + 8, span], (width * (b - q)) % LANES, 1)
                    tile = jnp.where(lane8 // width == b, moving, tile)
            tiles.append(tile)
        for q in range(2):
            px_msg[r * 2 + q] = above(tiles[2 * q], tiles[2 * q + 1]).astype(BF16)
    @pl.when(host)
    def _():
        pl.semaphore_wait(barrier, hosts - 1)

    @pl.when(guest)
    def _():
        pl.semaphore_wait(barrier, hosts)

    def main_copy(device):
        peer = (device[0] - low_row) * cols + device[1]
        return pltpu.make_async_remote_copy(
            src_ref=msg_ref.at[peer, 0:18], dst_ref=slots.at[me, 0:18],
            send_sem=sends.at[0], recv_sem=arrivals.at[0], device_id=device, device_id_type=MESH)

    def px_copy(device):
        peer = (device[0] - low_row) * cols + device[1]
        return pltpu.make_async_remote_copy(
            src_ref=px_msg.at[peer], dst_ref=px_slots.at[me],
            send_sem=sends.at[1], recv_sem=arrivals.at[1], device_id=device, device_id_type=MESH)

    def out_copy(device):
        peer = device[0] * cols + device[1]
        return pltpu.make_async_remote_copy(
            src_ref=out_send.at[peer], dst_ref=out_slots.at[seat],
            send_sem=sends.at[2], recv_sem=arrivals.at[2], device_id=device, device_id_type=MESH)

    def gram_copy(device):
        return pltpu.make_async_remote_copy(
            src_ref=gram_slots.at[seat], dst_ref=gram_slots.at[seat],
            send_sem=sends.at[3], recv_sem=arrivals.at[3], device_id=device, device_id_type=MESH)

    def base_copy():
        return pltpu.make_async_remote_copy(
            src_ref=base_send, dst_ref=base_slot,
            send_sem=sends.at[4], recv_sem=arrivals.at[4], device_id=(near_row, col), device_id_type=MESH)

    def start_all(copy, targets):
        for peer in targets:
            copy(peer).start()

    def pack(block):
        piece = block[0:8]
        for b in range(1, nc):
            piece = jnp.where(lane8 // nvec == b, block[b * 8:b * 8 + 8], piece)
        return piece

    def landed(ref, sem):
        pltpu.make_async_copy(ref, ref, sem).wait()

    def to_hosts(copy, here, there):
        start_all(copy, host_peers[:-1])

        @pl.when(guest)
        def _():
            copy(host_peers[-1]).start()

        @pl.when(host)
        def _():
            there[me] = here[seat]

    to_hosts(main_copy, msg_ref, slots)

    to_hosts(px_copy, px_msg, px_slots)

    loads[5].wait()
    energy = jnp.zeros((8, LANES), F32)
    for k in range(nk):
        for t in range(nb):
            energy = jnp.where((row8 == k * nv + t // nc) & (lane8 // nvec == t % nc), energy_ref[k, t], energy)
    lifted = energy * own
    high, low = split_pair(lifted)
    own_low = own.astype(BF16)
    base_send[...] = pack(fold_blocks(dot(own_low, high, (0, 0)) + dot(own_low, low, (0, 0)), nvec))

    @pl.when(guest)
    def _():
        base_copy().start()

    for load in loads[6:]:
        load.wait()

    @pl.when(host)
    def _():
        late = jnp.logical_and(col == 0, row < 2)
        rank = jnp.where(late, 0, me - 1 - (me > cols).astype(jnp.int32))

        def turned_to(step):
            at = rank + step
            at = jnp.where(at >= count - 2, at - (count - 2), at)
            spot = at + 1 + (at >= cols - 1).astype(jnp.int32)
            return spot // cols, lax.rem(spot, cols)

        leading = [(0, 0), (1, 0)] + [turned_to(step) for step in range(1, count - 2)]
        at = iota((sheets, LANES), 0)
        to = iota((sheets, LANES), 1)
        same = at // 8 == (to % half) // nk
        place = at % 8
        for j in range(nv):
            select[:, j * LANES:(j + 1) * LANES] = one_hot(same & (place == to % nk * nv + j))
        for a in range(spans):
            select[:, (nv + a) * LANES:(nv + a + 1) * LANES] = one_hot(
                same & (place == to % nk * 2 * spans + 2 * a + to // half))
        at = iota((LANES, sheets), 0)
        to = iota((LANES, sheets), 1)
        select_q[...] = one_hot((to // 8 == (at % half) // nk) & (to % 8 == at % nk))
        at = iota((LANES, LANES), 0)
        to = iota((LANES, LANES), 1)
        fold = at // 2
        angle = ((fold * ((to % half) // 2)) % MX).astype(F32) * (2.0 * math.pi / MX)
        weight = jnp.where((fold == 0) | (fold == MX // 2), 1.0, 2.0) * (1 - 2 * ((at % 2) * (to % 2))).astype(F32)
        table = jnp.where(fold <= MX // 2, jnp.cos(angle) * weight, 0.0)
        screened = above(screening_ref[...], jnp.zeros((LANES - screening_ref.shape[0], LANES), F32))
        lam[...] = wide_dot(split_pair(screened), split_pair(table), (0, 0)) * (-1.0 / (total * total))
        second_half = lax.rem(seat, 2)
        band = lam[pl.ds(pl.multiple_of(second_half * half, 8), half), :]
        lane_d = iota((deep, LANES), 1)
        spectrum = above(*[
            jnp.where(lane_d < half, band[2 * a * deep:(2 * a + 1) * deep], band[(2 * a + 1) * deep:(2 * a + 2) * deep])
            for a in range(spans)])
        raw = jnp.broadcast_to(coulomb_ref[...], (width, LANES)) * (2.0 / (total * nb))
        lane_w = iota((width, LANES), 1)
        charges = []
        for a in range(spans):
            tiles = jnp.zeros((width, LANES), F32)
            for b in range(cols):
                for q in range(2):
                    shift = (width * (b - 2 * q - a)) % LANES
                    moving = raw if shift == 0 else pltpu.roll(raw, shift, 1)
                    tiles = jnp.where((lane_w // width == b) & (second_half == q), moving, tiles)
            charges.append(tiles)

        landed(slots.at[0:count - 1, 0:18], arrivals.at[0])
        got = slots[...].astype(F32)
        own_all, rest_all, wave_all = [
            got[:, 8 * part:8 * part + 8].reshape(sheets, LANES) for part in range(3)]
        own_all, rest_all = own_all.astype(BF16), rest_all.astype(BF16)
        wave_all = jnp.where(iota((sheets, LANES), 0) % 8 < nk, wave_all, 0.0).astype(BF16)
        factors = dot(rest_all, select[:, nv * LANES:], (0, 0))
        spread = dot(own_all, select[:, 0:nv * LANES], (0, 0))
        for v in range(nv):
            for c in range(nc):
                for a in range(spans):
                    lanes = slice(a * LANES, (a + 1) * LANES)
                    joined = (
                        factors[v * deep:(v + 1) * deep, lanes] * factors[half + c * deep:half + (c + 1) * deep, lanes])
                    pairs[v * nc + c, a * deep:(a + 1) * deep] = joined.astype(BF16).astype(F32)
        for t in range(nb):
            moved[t] = spread[t % nc * nvec:(t % nc + 1) * nvec, t // nc * LANES:(t // nc + 1) * LANES]
        waves = dot(select_q[...], wave_all, (1, 0))
        crossed = pltpu.roll(waves, half, 1)
        first = (at < half) & (to < half)
        second = (at >= half) & (to >= half)
        main = jnp.where(first, waves, jnp.where(second, crossed, 0.0)).astype(BF16)
        fine = jnp.where(first, crossed, jnp.where(second, waves, 0.0)).astype(BF16)
        none = jnp.zeros((LANES, LANES), BF16)
        ahead = above(beside(main, fine), beside(main, none))
        astern = above(beside(main, main), beside(fine, none))

        def through(values, weights, contract):
            both = dot(beside(*split_pair(values)), weights, contract)
            return both[:, 0:LANES] + both[:, LANES:]

        def unfold(first_j, last_j):
            placed = beside(*[above(*[moved[j * nc + c] for c in range(nc)]) for j in range(first_j, last_j)])
            return dot(select[:, first_j * LANES:last_j * LANES], above(*split_pair(placed)), (1, 1))

        group = 2
        for first_l in range(0, levels, group):
            sums_l = [None] * group
            for t in range(nb):
                for u in range(group):
                    term = pairs[t, first_l + u:first_l + u + 1, :] * moved[t]
                    sums_l[u] = term if t == 0 else sums_l[u] + term
            for u in range(group):
                proj[first_l + u] = sums_l[u]
        spectral = through(proj[...].reshape(levels * nvec, LANES), ahead, (1, 0)).reshape(levels, nvec, LANES)
        scaled = spectral * spectrum[:, None, :]
        sides = [
            split_pair(jnp.concatenate([side[l] for l in range(levels)], axis=1)) for side in (spectral, scaled)]
        stacked = dot(above(*sides[0]), sides[1][0], (1, 1))
        gram = stacked[0:nvec] + stacked[nvec:] + dot(sides[0][0], sides[1][1], (1, 1))

        landed(px_slots.at[0:count - 1], arrivals.at[1])
        taken_px = px_slots[...].astype(F32)
        exchange = beside(*[
            taken_px[:, 8 * a:8 * a + 8].reshape(sheets, LANES).astype(BF16) for a in range(spans)])
        crowd = dot(own_all, exchange, (0, 0))
        densities = [fold_blocks(crowd[:, a * LANES:(a + 1) * LANES], nvec) for a in range(spans)]
        charged = [density * charge for density, charge in zip(densities, charges)]
        gram = gram + wide_dot(
            split_pair(beside(*densities)), split_pair(beside(*charged) * (1.0 / cols)), (1, 1))
        proj[...] = through(scaled.reshape(levels * nvec, LANES), astern, (1, 1)).reshape(levels, nvec, LANES)
        for first_t in range(0, nb // 2, group):
            sums_t = [None] * group
            for l in range(levels):
                for u in range(group):
                    term = pairs[first_t + u, l:l + 1, :] * proj[l]
                    sums_t[u] = term if l == 0 else sums_t[u] + term
            for u in range(group):
                moved[first_t + u] = sums_t[u]
        landed(base_slot, arrivals.at[4])
        gram_slots[seat] = (
            base_send[...] + base_slot[...] + pack(jnp.concatenate([gram] * nc, axis=1)))
        start_all(gram_copy, leading[:2])

        blocks = beside(*[
            jnp.where(at // nvec == to // width, jnp.concatenate([charge] * (LANES // nvec), axis=0), 0.0)
            for charge in charged])
        whole = dot(exchange, above(*split_pair(blocks)), (1, 1))
        early = unfold(0, nv // 2)
        for first_t in range(nb // 2, nb - nc, group):
            sums_t = [None] * group
            for l in range(levels):
                for u in range(group):
                    term = pairs[first_t + u, l:l + 1, :] * proj[l]
                    sums_t[u] = term if l == 0 else sums_t[u] + term
            for u in range(group):
                moved[first_t + u] = sums_t[u]
        early = early + unfold(nv // 2, nv - 1)
        for first_t in range(nb - nc, nb, group):
            sums_t = [None] * group
            for l in range(levels):
                for u in range(group):
                    term = pairs[first_t + u, l:l + 1, :] * proj[l]
                    sums_t[u] = term if l == 0 else sums_t[u] + term
            for u in range(group):
                moved[first_t + u] = sums_t[u]
        whole = whole + early + unfold(nv - 1, nv)
        whole = whole[:, 0:LANES] + whole[:, LANES:]
        out_send[...] = whole.reshape(count, 8, LANES)
        start_all(out_copy, leading)
        start_all(gram_copy, leading[2:])
        out_slots[seat] = out_send[me]

    def each(run):
        @pl.when(host)
        def _():
            run(hosts - 1)

        @pl.when(guest)
        def _():
            run(hosts)

    each(lambda n: landed(gram_slots.at[0:n], arrivals.at[3]))
    sums = jnp.sum(gram_slots[...], axis=0) * (1.0 / (total * nb))
    turns = [sums] + [pltpu.roll(sums, b * nvec, 1) for b in range(1, nc)]
    for b in range(nc):
        alpha_ref[b * 8:b * 8 + 8] = turns[(-b) % nc][:, 0:nvec]
    mixed = jnp.concatenate(
        [jnp.where(lane8 // nvec == q, turns[(q - b) % nc], 0.0) for q in range(nc) for b in range(nc)], axis=0)
    high, low = split_pair(mixed)
    rest = lifted - dot(own_low, high, (1, 0)) - dot(own_low, low, (1, 0))

    each(lambda n: landed(out_slots.at[0:n], arrivals.at[2]))
    residual = rest + jnp.sum(out_slots[...], axis=0)
    for j in range(nv):
        out_ref[:, j * LANES:(j + 1) * LANES] = jnp.concatenate(
            [residual[k * nv + j:k * nv + j + 1] for k in range(nk)], axis=0)

    def drain(n):
        landed(slots.at[0:n, 0:18], sends.at[0])
        landed(px_slots.at[0:n], sends.at[1])

    each(drain)

    @pl.when(guest)
    def _():
        landed(base_slot, sends.at[4])

    @pl.when(host)
    def _():
        landed(out_send.at[0:count - 1], sends.at[2])
        landed(out_send.at[0:count - 1], sends.at[3])


def finish(out_ref, alpha_ref, out_hbm, alpha_hbm, sems):
    copies = [
        pltpu.make_async_copy(src, dst, sems.at[at])
        for at, (src, dst) in enumerate(((out_ref, out_hbm), (alpha_ref, alpha_hbm)))]
    for copy in copies:
        copy.start()
    for copy in copies:
        copy.wait()


def fast_on_device(pair_exchange, conduction, valence, coulomb, screening, energies, vectors, k_coords):
    nk, nb, planes = pair_exchange.shape
    nv, nc = valence.shape[1], conduction.shape[1]
    nvec = vectors.shape[1] // nb
    rows, cols = lax.axis_size("row"), lax.axis_size("col")
    count = rows * cols
    total = nk * count
    hosts = count // 2
    width = LANES // cols
    spans = planes // hosts // width
    levels = spans * width // 2
    vmem = pl.BlockSpec(memory_space=pltpu.VMEM)
    dma = pltpu.SemaphoreType.DMA
    results = pl.pallas_call(
        functools.partial(kernel, (rows, cols, nk, nv, nc, nvec, total)),
        out_shape=(
            pltpu.VMEM((nk, nb * nvec), F32),
            pltpu.VMEM((nvec, nvec), F32),
        ),
        in_specs=[pl.BlockSpec(memory_space=pl.ANY)] * 8,
        out_specs=(vmem, vmem),
        scratch_shapes=[
            pltpu.VMEM(pair_exchange.shape, BF16),
            pltpu.VMEM(conduction.shape, BF16),
            pltpu.VMEM(valence.shape, BF16),
            pltpu.VMEM((1, LANES), F32),
            pltpu.VMEM((screening.shape[0], LANES), F32),
            pltpu.VMEM(vectors.shape, BF16),
            pltpu.SMEM(energies.shape, F32),
            pltpu.SMEM(k_coords.shape, jnp.int32),
            dma((8,)),
            pltpu.VMEM((hosts, 32, LANES), BF16),
            pltpu.VMEM((count, 32, LANES), BF16),
            pltpu.VMEM((hosts, 16, LANES), BF16),
            pltpu.VMEM((count, 16, LANES), BF16),
            pltpu.VMEM((count * 8, (nv + spans) * LANES), BF16),
            pltpu.VMEM((LANES, count * 8), BF16),
            pltpu.VMEM((LANES, LANES), F32),
            pltpu.VMEM((nb, levels, LANES), F32),
            pltpu.VMEM((nb, nvec, LANES), F32),
            pltpu.VMEM((levels, nvec, LANES), F32),
            pltpu.VMEM((count, 8, LANES), F32),
            pltpu.VMEM((hosts, 8, LANES), F32),
            pltpu.VMEM((hosts, 8, LANES), F32),
            pltpu.VMEM((8, LANES), F32),
            pltpu.VMEM((8, LANES), F32),
            dma((5,)), dma((5,)),
        ],
        compiler_params=pltpu.CompilerParams(collective_id=0, has_side_effects=True),
    )(pair_exchange, conduction, valence, coulomb.reshape(1, planes), screening, vectors, energies, k_coords)
    return pl.pallas_call(
        finish,
        out_shape=(jax.ShapeDtypeStruct((nk, nb * nvec), F32), jax.ShapeDtypeStruct((nvec, nvec), F32)),
        in_specs=[vmem, vmem],
        out_specs=(pl.BlockSpec(memory_space=pl.ANY), pl.BlockSpec(memory_space=pl.ANY)),
        scratch_shapes=[dma((2,))],
    )(*[pltpu.with_memory_space_constraint(result, pltpu.VMEM) for result in results])


highest = lax.Precision.HIGHEST


def pair_factors(conduction, valence):
    count, valence_count, plane_count = valence.shape
    joined = (
        valence.astype(jnp.float32)[:, :, None, :] * conduction.astype(jnp.float32)[:, None, :, :]
    )
    return joined.reshape(count, valence_count * conduction.shape[1], plane_count).astype(
        jnp.bfloat16
    )


def transfer_index(rows_at, cols_at, mesh_cols):
    delta_first = jnp.mod(rows_at[:, None, 0] - cols_at[None, :, 0], MX)
    delta_second = jnp.mod(rows_at[:, None, 1] - cols_at[None, :, 1], mesh_cols)
    fold_first = jnp.minimum(delta_first, MX - delta_first)
    fold_second = jnp.minimum(delta_second, mesh_cols - delta_second)
    return (fold_first * (mesh_cols // 2 + 1) + fold_second).astype(jnp.int32)


def on_device(pair_exchange, conduction, valence, coulomb, screening, energies, vectors, k_coords):
    local_count, band_count, plane_count = pair_exchange.shape
    vector_count = vectors.shape[1] // band_count
    row_count = lax.axis_size("row")
    col_count = lax.axis_size("col")
    total_count = local_count * row_count * col_count
    mesh_cols = total_count // MX
    moving = vectors.reshape(local_count, band_count, vector_count)
    partial_density = jnp.einsum(
        "ktg,ktn->gn", pair_exchange, moving, preferred_element_type=jnp.float32
    )
    density = lax.psum(partial_density, ("row", "col"))
    block_size = 128
    sweeps = plane_count // block_size
    col_cond, col_val, col_vec, col_at = (
        lax.all_gather(conduction, "row", axis=0, tiled=True),
        lax.all_gather(valence, "row", axis=0, tiled=True),
        lax.all_gather(vectors, "row", axis=0, tiled=True),
        lax.all_gather(k_coords, "row", axis=0, tiled=True),
    )
    row_cond, row_val, row_at = (
        lax.all_gather(conduction, "col", axis=0, tiled=True),
        lax.all_gather(valence, "col", axis=0, tiled=True),
        lax.all_gather(k_coords, "col", axis=0, tiled=True),
    )
    row_pairs = pair_factors(row_cond, row_val)
    col_pairs = pair_factors(col_cond, col_val)
    indices = transfer_index(row_at, col_at, mesh_cols)
    col_moving = col_vec.reshape(-1, band_count, vector_count)

    def square_sweep(sweep_index, running):
        anchor = sweep_index * block_size
        coupling = jnp.take(
            lax.dynamic_slice_in_dim(screening, anchor, block_size, 1), indices, axis=0
        )
        row_block = lax.dynamic_slice_in_dim(row_pairs, anchor, block_size, 2)
        col_block = lax.dynamic_slice_in_dim(col_pairs, anchor, block_size, 2)
        col_proj = jnp.einsum(
            "ktg,ktn->kng", col_block, col_moving, preferred_element_type=jnp.float32
        )
        potential = jnp.einsum("ijg,jng->ing", coupling, col_proj, precision=highest)
        return running + jnp.einsum(
            "ktg,kng->ktn", row_block.astype(jnp.float32), potential, precision=highest
        )

    forward = lax.fori_loop(
        0,
        sweeps,
        square_sweep,
        jnp.zeros((row_pairs.shape[0], band_count, vector_count), jnp.float32),
    )
    owned = lax.psum_scatter(
        forward.reshape(col_count, local_count, band_count, vector_count),
        "col",
        scatter_dimension=0,
        tiled=True,
    )[0]
    moving_wide = moving.astype(jnp.float32)
    exchange_term = jnp.einsum(
        "ktg,gn->ktn", pair_exchange.astype(jnp.float32) * coulomb, density, precision=highest
    )
    applied = (
        energies[:, :, None] * moving_wide
        + 2.0 / (total_count * band_count) * exchange_term
        - owned / total_count
    )
    gram = jnp.einsum("ktm,ktn->mn", moving_wide, applied, precision=highest)
    alpha = lax.psum(gram, ("row", "col")) / (total_count * band_count)
    residual = applied - jnp.einsum("ktm,mn->ktn", moving_wide, alpha, precision=highest)
    return (residual.reshape(local_count, band_count * vector_count), alpha)


def fits(args, mesh):
    pair_exchange, conduction, valence, _, screening, _, vectors, _ = args
    rows, cols = mesh.shape["row"], mesh.shape["col"]
    points, nb, planes = pair_exchange.shape
    nk = points // (rows * cols)
    nv, nc = valence.shape[1], conduction.shape[1]
    nvec = vectors.shape[1] // nb
    return (
        planes == rows * LANES and rows == 8 and cols == 4 and rows * cols * nk * 2 == LANES and nk == 2 and nv == 4 and nc == 4
        and nc * nvec == LANES and points == 2 * MX and screening.shape[0] == MX + 2
    )


def solution(mesh):
    in_specs = (
        P(("row", "col"), None, None),
        P(("row", "col"), None, None),
        P(("row", "col"), None, None),
        P(),
        P(),
        P(("row", "col"), None),
        P(("row", "col"), None),
        P(("row", "col"), None),
    )
    out_specs = (P(("row", "col"), None), P())

    def run(*args):
        body = fast_on_device if fits(args, mesh) else on_device
        return jax.shard_map(
            body, mesh=mesh, in_specs=in_specs, out_specs=out_specs, check_vma=False
        )(*args)

    return run
```

```python
import functools
import math

import jax
import jax.numpy as jnp
from jax import lax
from jax.experimental import pallas as pl
from jax.experimental.pallas import tpu as pltpu
from jax.sharding import PartitionSpec as P

MX = 32
LANES = 128
MESH = pl.DeviceIdType.MESH
F32 = jnp.float32
BF16 = jnp.bfloat16


def split_pair(value):
    high = value.astype(BF16)
    return high, (value - high.astype(F32)).astype(BF16)


def dot(a, b, contract):
    return lax.dot_general(a, b, ((contract[0:1], contract[1:2]), ((), ())), preferred_element_type=F32)


def iota(shape, axis):
    return lax.broadcasted_iota(jnp.int32, shape, axis)


def one_hot(condition):
    return jnp.where(condition, 1.0, 0.0).astype(BF16)


def wide_dot(a, b, contract):
    high, low = a
    main, rest = b
    return dot(high, main, contract) + dot(low, main, contract) + dot(high, rest, contract)


def beside(*parts):
    return jnp.concatenate(parts, axis=1)


def above(*parts):
    return jnp.concatenate(parts, axis=0)


def swap_blocks(tile, lanes, rows):
    row_bit = (iota(tile.shape, 0) // rows) % 2
    lane_bit = (iota(tile.shape, 1) // lanes) % 2
    up = pltpu.roll(pltpu.roll(tile, lanes, 1), tile.shape[0] - rows, 0)
    down = pltpu.roll(pltpu.roll(tile, LANES - lanes, 1), rows, 0)
    return jnp.where(row_bit == lane_bit, tile, jnp.where(lane_bit == 1, up, down))


def fold_blocks(square, width):
    kept = jnp.where(iota(square.shape, 0) // width == iota(square.shape, 1) // width, square, 0.0)
    rows = kept[0:width]
    for at in range(width, square.shape[0], width):
        rows = rows + kept[at:at + width]
    half = rows + pltpu.roll(rows, LANES // 2, 1)
    return half + pltpu.roll(half, LANES // 4, 1)


def basis(phase, sign):
    angle = (phase % MX).astype(F32) * (2.0 * math.pi / MX)
    return (jnp.cos(angle) + jnp.sin(angle)) * (1 - 2 * (sign % 2)).astype(F32)


def kernel(
    dims, px_hbm, cond_hbm, val_hbm, coulomb_hbm, screening_hbm, vec_hbm, energy_hbm, place_hbm,
    out_ref, alpha_ref,
    px_ref, cond_ref, val_ref, coulomb_ref, screening_ref, vec_ref, energy_ref, place_ref,
    load_sem, msg_ref, slots, px_msg, px_slots, select, select_q, lam, pairs, moved, proj, out_send, out_slots, gram_slots,
    base_send, base_slot, sends, arrivals,
):
    rows, cols, nk, nv, nc, nvec, total = dims
    row, col = lax.axis_index("row"), lax.axis_index("col")
    me = row * cols + col
    count = rows * cols
    nb = nv * nc
    low_row, high_row = rows // 4, rows - rows // 4
    hosts = (high_row - low_row) * cols
    host = (row >= low_row) & (row < high_row)
    guest = jnp.logical_not(host)
    near_row = jnp.where(row < low_row, row + low_row, jnp.where(row >= high_row, row - low_row, row))
    seat = (near_row - low_row) * cols + col
    width = LANES // cols
    deep = width // 2
    unit = nk * nv
    half = LANES // 2
    sheets = count * 8
    spans = rows * LANES // hosts // width
    levels = spans * deep

    ring_rows = [row] + [lax.rem(row + step, rows) for step in range(1, rows)]
    ring_cols = [col] + [lax.rem(col + step, cols) for step in range(1, cols)]
    everyone = [(pr, pc) for i, pr in enumerate(ring_rows) for j, pc in enumerate(ring_cols) if i + j]
    signalled = [
        (jnp.where(me == at, rows - 1, at // cols), jnp.where(me == at, cols - 1, at % cols)) for at in range(count - 1)]
    host_rows = [low_row + lax.rem(near_row - low_row + step, high_row - low_row) for step in range(high_row - low_row)]
    left = lax.rem(col, 2)
    host_cols = [cols - 1 - col, lax.rem(col + 2, cols), col + 1 - 2 * left, col]
    host_peers = [(pr, pc) for pc in [host_cols[0], host_cols[2], host_cols[1], host_cols[3]] for pr in [host_rows[2], host_rows[3], host_rows[1], host_rows[0]]]

    barrier = pltpu.get_barrier_semaphore()
    mine = pl.ds(pl.multiple_of(seat // 2 * LANES, LANES), LANES)
    loads = [
        pltpu.make_async_copy(src, dst, load_sem.at[at])
        for at, (src, dst) in enumerate((
            (val_hbm, val_ref), (cond_hbm, cond_ref), (vec_hbm, vec_ref), (place_hbm, place_ref), (px_hbm, px_ref),
            (energy_hbm, energy_ref), (screening_hbm.at[:, mine], screening_ref), (coulomb_hbm.at[:, mine], coulomb_ref)))
    ]
    for load in loads[:4]:
        load.start()

    @pl.when(host)
    def _():
        for peer in signalled:
            pl.semaphore_signal(barrier, inc=1, device_id=peer, device_id_type=MESH)

    for load in loads[4:]:
        load.start()
    row8 = iota((8, LANES), 0)
    lane8 = iota((8, LANES), 1)
    for load in loads[:4]:
        load.wait()

    vec = vec_ref[...].astype(F32)
    own = jnp.concatenate(
        [vec[k:k + 1, j * LANES:(j + 1) * LANES] for k in range(nk) for j in range(nv)], axis=0)
    tail = jnp.zeros((8, LANES), F32)
    wave = lane8 % half
    for k in range(nk):
        value = basis((wave // 2) * place_ref[k, 0], (wave % 2) * place_ref[k, 1])
        high = value.astype(BF16).astype(F32)
        tail = jnp.where(row8 == k, jnp.where(lane8 < half, high, value - high), tail)
    tail = above(tail, jnp.zeros((8, LANES), F32)).astype(BF16)
    for r in range(rows):
        span = slice(r * LANES, (r + 1) * LANES)
        turned = []
        for k in range(nk):
            tile = above(val_ref[k, :, span].astype(F32), cond_ref[k, :, span].astype(F32))
            for size in (4, 2, 1):
                tile = swap_blocks(tile, deep * size, size)
            turned.append(tile)
        flipped = [pltpu.roll(tile, 4, 0) for tile in turned]
        first_half = jnp.where(row8 < 4, turned[0], flipped[1])
        other_half = jnp.where(row8 < 4, flipped[0], turned[1])
        for q, low in enumerate((first_half, other_half)):
            msg_ref[r * 2 + q, 0:16] = above(own, low).astype(BF16)
            msg_ref[r * 2 + q, 16:32] = tail

    loads[4].wait()
    at = iota((nk * nb, nk * nb), 0)
    to = iota((nk * nb, nk * nb), 1)
    order = one_hot(to == (at % unit) // nv * nb + at % nv * nc + at // unit)
    arranged = dot(order, px_ref[...].reshape(nk * nb, px_ref.shape[2]), (1, 0))
    for r in range(rows):
        span = slice(r * LANES, (r + 1) * LANES)
        tiles = []
        for q in range(cols):
            tile = arranged[q * 8:q * 8 + 8, span]
            for b in range(cols):
                if b != q:
                    moving = pltpu.roll(arranged[b * 8:b * 8 + 8, span], (width * (b - q)) % LANES, 1)
                    tile = jnp.where(lane8 // width == b, moving, tile)
            tiles.append(tile)
        for q in range(2):
            px_msg[r * 2 + q] = above(tiles[2 * q], tiles[2 * q + 1]).astype(BF16)
    @pl.when(host)
    def _():
        pl.semaphore_wait(barrier, hosts - 1)

    @pl.when(guest)
    def _():
        pl.semaphore_wait(barrier, hosts)

    def main_copy(device):
        peer = (device[0] - low_row) * cols + device[1]
        return pltpu.make_async_remote_copy(
            src_ref=msg_ref.at[peer, 0:18], dst_ref=slots.at[me, 0:18],
            send_sem=sends.at[0], recv_sem=arrivals.at[0], device_id=device, device_id_type=MESH)

    def px_copy(device):
        peer = (device[0] - low_row) * cols + device[1]
        return pltpu.make_async_remote_copy(
            src_ref=px_msg.at[peer], dst_ref=px_slots.at[me],
            send_sem=sends.at[1], recv_sem=arrivals.at[1], device_id=device, device_id_type=MESH)

    def out_copy(device):
        peer = device[0] * cols + device[1]
        return pltpu.make_async_remote_copy(
            src_ref=out_send.at[peer], dst_ref=out_slots.at[seat],
            send_sem=sends.at[2], recv_sem=arrivals.at[2], device_id=device, device_id_type=MESH)

    def gram_copy(device):
        return pltpu.make_async_remote_copy(
            src_ref=gram_slots.at[seat], dst_ref=gram_slots.at[seat],
            send_sem=sends.at[3], recv_sem=arrivals.at[3], device_id=device, device_id_type=MESH)

    def base_copy():
        return pltpu.make_async_remote_copy(
            src_ref=base_send, dst_ref=base_slot,
            send_sem=sends.at[4], recv_sem=arrivals.at[4], device_id=(near_row, col), device_id_type=MESH)

    def start_all(copy, targets):
        for peer in targets:
            copy(peer).start()

    def pack(block):
        piece = block[0:8]
        for b in range(1, nc):
            piece = jnp.where(lane8 // nvec == b, block[b * 8:b * 8 + 8], piece)
        return piece

    def landed(ref, sem):
        pltpu.make_async_copy(ref, ref, sem).wait()

    def to_hosts(copy, here, there):
        start_all(copy, host_peers[:-1])

        @pl.when(guest)
        def _():
            copy(host_peers[-1]).start()

        @pl.when(host)
        def _():
            there[me] = here[seat]

    to_hosts(main_copy, msg_ref, slots)

    to_hosts(px_copy, px_msg, px_slots)

    loads[5].wait()
    energy = jnp.zeros((8, LANES), F32)
    for k in range(nk):
        for t in range(nb):
            energy = jnp.where((row8 == k * nv + t // nc) & (lane8 // nvec == t % nc), energy_ref[k, t], energy)
    lifted = energy * own
    high, low = split_pair(lifted)
    own_low = own.astype(BF16)
    base_send[...] = pack(fold_blocks(dot(own_low, high, (0, 0)) + dot(own_low, low, (0, 0)), nvec))

    @pl.when(guest)
    def _():
        base_copy().start()

    for load in loads[6:]:
        load.wait()

    @pl.when(host)
    def _():
        late = jnp.logical_and(col == 0, row < 2)
        rank = jnp.where(late, 0, me - 1 - (me > cols).astype(jnp.int32))

        def turned_to(step):
            at = rank + step
            at = jnp.where(at >= count - 2, at - (count - 2), at)
            spot = at + 1 + (at >= cols - 1).astype(jnp.int32)
            return spot // cols, lax.rem(spot, cols)

        leading = [(0, 0), (1, 0)] + [turned_to(step) for step in range(1, count - 2)]
        at = iota((sheets, LANES), 0)
        to = iota((sheets, LANES), 1)
        same = at // 8 == (to % half) // nk
        place = at % 8
        for j in range(nv):
            select[:, j * LANES:(j + 1) * LANES] = one_hot(same & (place == to % nk * nv + j))
        for a in range(spans):
            select[:, (nv + a) * LANES:(nv + a + 1) * LANES] = one_hot(
                same & (place == to % nk * 2 * spans + 2 * a + to // half))
        at = iota((LANES, sheets), 0)
        to = iota((LANES, sheets), 1)
        select_q[...] = one_hot((to // 8 == (at % half) // nk) & (to % 8 == at % nk))
        at = iota((LANES, LANES), 0)
        to = iota((LANES, LANES), 1)
        fold = at // 2
        angle = ((fold * ((to % half) // 2)) % MX).astype(F32) * (2.0 * math.pi / MX)
        weight = jnp.where((fold == 0) | (fold == MX // 2), 1.0, 2.0) * (1 - 2 * ((at % 2) * (to % 2))).astype(F32)
        table = jnp.where(fold <= MX // 2, jnp.cos(angle) * weight, 0.0)
        screened = above(screening_ref[...], jnp.zeros((LANES - screening_ref.shape[0], LANES), F32))
        lam[...] = wide_dot(split_pair(screened), split_pair(table), (0, 0)) * (-1.0 / (total * total))
        second_half = lax.rem(seat, 2)
        band = lam[pl.ds(pl.multiple_of(second_half * half, 8), half), :]
        lane_d = iota((deep, LANES), 1)
        spectrum = above(*[
            jnp.where(lane_d < half, band[2 * a * deep:(2 * a + 1) * deep], band[(2 * a + 1) * deep:(2 * a + 2) * deep])
            for a in range(spans)])
        raw = jnp.broadcast_to(coulomb_ref[...], (width, LANES)) * (2.0 / (total * nb))
        lane_w = iota((width, LANES), 1)
        charges = []
        for a in range(spans):
            tiles = jnp.zeros((width, LANES), F32)
            for b in range(cols):
                for q in range(2):
                    shift = (width * (b - 2 * q - a)) % LANES
                    moving = raw if shift == 0 else pltpu.roll(raw, shift, 1)
                    tiles = jnp.where((lane_w // width == b) & (second_half == q), moving, tiles)
            charges.append(tiles)

        landed(slots.at[0:count - 1, 0:18], arrivals.at[0])
        got = slots[...].astype(F32)
        own_all, rest_all, wave_all = [
            got[:, 8 * part:8 * part + 8].reshape(sheets, LANES) for part in range(3)]
        own_all, rest_all = own_all.astype(BF16), rest_all.astype(BF16)
        wave_all = jnp.where(iota((sheets, LANES), 0) % 8 < nk, wave_all, 0.0).astype(BF16)
        factors = dot(rest_all, select[:, nv * LANES:], (0, 0))
        spread = dot(own_all, select[:, 0:nv * LANES], (0, 0))
        for v in range(nv):
            for c in range(nc):
                for a in range(spans):
                    lanes = slice(a * LANES, (a + 1) * LANES)
                    joined = (
                        factors[v * deep:(v + 1) * deep, lanes] * factors[half + c * deep:half + (c + 1) * deep, lanes])
                    pairs[v * nc + c, a * deep:(a + 1) * deep] = joined.astype(BF16).astype(F32)
        for t in range(nb):
            moved[t] = spread[t % nc * nvec:(t % nc + 1) * nvec, t // nc * LANES:(t // nc + 1) * LANES]
        waves = dot(select_q[...], wave_all, (1, 0))
        crossed = pltpu.roll(waves, half, 1)
        first = (at < half) & (to < half)
        second = (at >= half) & (to >= half)
        main = jnp.where(first, waves, jnp.where(second, crossed, 0.0)).astype(BF16)
        fine = jnp.where(first, crossed, jnp.where(second, waves, 0.0)).astype(BF16)
        none = jnp.zeros((LANES, LANES), BF16)
        ahead = above(beside(main, fine), beside(main, none))
        astern = above(beside(main, main), beside(fine, none))

        def through(values, weights, contract):
            both = dot(beside(*split_pair(values)), weights, contract)
            return both[:, 0:LANES] + both[:, LANES:]

        def unfold(first_j, last_j):
            placed = beside(*[above(*[moved[j * nc + c] for c in range(nc)]) for j in range(first_j, last_j)])
            return dot(select[:, first_j * LANES:last_j * LANES], above(*split_pair(placed)), (1, 1))

        group = 2
        for first_l in range(0, levels, group):
            sums_l = [None] * group
            for t in range(nb):
                for u in range(group):
                    term = pairs[t, first_l + u:first_l + u + 1, :] * moved[t]
                    sums_l[u] = term if t == 0 else sums_l[u] + term
            for u in range(group):
                proj[first_l + u] = sums_l[u]
        spectral = through(proj[...].reshape(levels * nvec, LANES), ahead, (1, 0)).reshape(levels, nvec, LANES)
        scaled = spectral * spectrum[:, None, :]
        sides = [
            split_pair(jnp.concatenate([side[l] for l in range(levels)], axis=1)) for side in (spectral, scaled)]
        stacked = dot(above(*sides[0]), sides[1][0], (1, 1))
        gram = stacked[0:nvec] + stacked[nvec:] + dot(sides[0][0], sides[1][1], (1, 1))

        landed(px_slots.at[0:count - 1], arrivals.at[1])
        taken_px = px_slots[...].astype(F32)
        exchange = beside(*[
            taken_px[:, 8 * a:8 * a + 8].reshape(sheets, LANES).astype(BF16) for a in range(spans)])
        crowd = dot(own_all, exchange, (0, 0))
        densities = [fold_blocks(crowd[:, a * LANES:(a + 1) * LANES], nvec) for a in range(spans)]
        charged = [density * charge for density, charge in zip(densities, charges)]
        gram = gram + wide_dot(
            split_pair(beside(*densities)), split_pair(beside(*charged) * (1.0 / cols)), (1, 1))
        proj[...] = through(scaled.reshape(levels * nvec, LANES), astern, (1, 1)).reshape(levels, nvec, LANES)
        for first_t in range(0, nb // 2, group):
            sums_t = [None] * group
            for l in range(levels):
                for u in range(group):
                    term = pairs[first_t + u, l:l + 1, :] * proj[l]
                    sums_t[u] = term if l == 0 else sums_t[u] + term
            for u in range(group):
                moved[first_t + u] = sums_t[u]
        landed(base_slot, arrivals.at[4])
        gram_slots[seat] = (
            base_send[...] + base_slot[...] + pack(jnp.concatenate([gram] * nc, axis=1)))
        start_all(gram_copy, leading[:2])

        blocks = beside(*[
            jnp.where(at // nvec == to // width, jnp.concatenate([charge] * (LANES // nvec), axis=0), 0.0)
            for charge in charged])
        whole = dot(exchange, above(*split_pair(blocks)), (1, 1))
        early = unfold(0, nv // 2)
        for first_t in range(nb // 2, nb - nc, group):
            sums_t = [None] * group
            for l in range(levels):
                for u in range(group):
                    term = pairs[first_t + u, l:l + 1, :] * proj[l]
                    sums_t[u] = term if l == 0 else sums_t[u] + term
            for u in range(group):
                moved[first_t + u] = sums_t[u]
        early = early + unfold(nv // 2, nv - 1)
        for first_t in range(nb - nc, nb, group):
            sums_t = [None] * group
            for l in range(levels):
                for u in range(group):
                    term = pairs[first_t + u, l:l + 1, :] * proj[l]
                    sums_t[u] = term if l == 0 else sums_t[u] + term
            for u in range(group):
                moved[first_t + u] = sums_t[u]
        whole = whole + early + unfold(nv - 1, nv)
        whole = whole[:, 0:LANES] + whole[:, LANES:]
        out_send[...] = whole.reshape(count, 8, LANES)
        start_all(out_copy, leading)
        start_all(gram_copy, leading[2:])
        out_slots[seat] = out_send[me]

    def each(run):
        @pl.when(host)
        def _():
            run(hosts - 1)

        @pl.when(guest)
        def _():
            run(hosts)

    each(lambda n: landed(gram_slots.at[0:n], arrivals.at[3]))
    sums = jnp.sum(gram_slots[...], axis=0) * (1.0 / (total * nb))
    turns = [sums] + [pltpu.roll(sums, b * nvec, 1) for b in range(1, nc)]
    for b in range(nc):
        alpha_ref[b * 8:b * 8 + 8] = turns[(-b) % nc][:, 0:nvec]
    mixed = jnp.concatenate(
        [jnp.where(lane8 // nvec == q, turns[(q - b) % nc], 0.0) for q in range(nc) for b in range(nc)], axis=0)
    high, low = split_pair(mixed)
    rest = lifted - dot(own_low, high, (1, 0)) - dot(own_low, low, (1, 0))

    each(lambda n: landed(out_slots.at[0:n], arrivals.at[2]))
    residual = rest + jnp.sum(out_slots[...], axis=0)
    for j in range(nv):
        out_ref[:, j * LANES:(j + 1) * LANES] = jnp.concatenate(
            [residual[k * nv + j:k * nv + j + 1] for k in range(nk)], axis=0)

    def drain(n):
        landed(slots.at[0:n, 0:18], sends.at[0])
        landed(px_slots.at[0:n], sends.at[1])

    each(drain)

    @pl.when(guest)
    def _():
        landed(base_slot, sends.at[4])

    @pl.when(host)
    def _():
        landed(out_send.at[0:count - 1], sends.at[2])
        landed(out_send.at[0:count - 1], sends.at[3])


def finish(out_ref, alpha_ref, out_hbm, alpha_hbm, sems):
    copies = [
        pltpu.make_async_copy(src, dst, sems.at[at])
        for at, (src, dst) in enumerate(((out_ref, out_hbm), (alpha_ref, alpha_hbm)))]
    for copy in copies:
        copy.start()
    for copy in copies:
        copy.wait()


def fast_on_device(pair_exchange, conduction, valence, coulomb, screening, energies, vectors, k_coords):
    nk, nb, planes = pair_exchange.shape
    nv, nc = valence.shape[1], conduction.shape[1]
    nvec = vectors.shape[1] // nb
    rows, cols = lax.axis_size("row"), lax.axis_size("col")
    count = rows * cols
    total = nk * count
    hosts = count // 2
    width = LANES // cols
    spans = planes // hosts // width
    levels = spans * width // 2
    vmem = pl.BlockSpec(memory_space=pltpu.VMEM)
    dma = pltpu.SemaphoreType.DMA
    results = pl.pallas_call(
        functools.partial(kernel, (rows, cols, nk, nv, nc, nvec, total)),
        out_shape=(
            pltpu.VMEM((nk, nb * nvec), F32),
            pltpu.VMEM((nvec, nvec), F32),
        ),
        in_specs=[pl.BlockSpec(memory_space=pl.ANY)] * 8,
        out_specs=(vmem, vmem),
        scratch_shapes=[
            pltpu.VMEM(pair_exchange.shape, BF16),
            pltpu.VMEM(conduction.shape, BF16),
            pltpu.VMEM(valence.shape, BF16),
            pltpu.VMEM((1, LANES), F32),
            pltpu.VMEM((screening.shape[0], LANES), F32),
            pltpu.VMEM(vectors.shape, BF16),
            pltpu.SMEM(energies.shape, F32),
            pltpu.SMEM(k_coords.shape, jnp.int32),
            dma((8,)),
            pltpu.VMEM((hosts, 32, LANES), BF16),
            pltpu.VMEM((count, 32, LANES), BF16),
            pltpu.VMEM((hosts, 16, LANES), BF16),
            pltpu.VMEM((count, 16, LANES), BF16),
            pltpu.VMEM((count * 8, (nv + spans) * LANES), BF16),
            pltpu.VMEM((LANES, count * 8), BF16),
            pltpu.VMEM((LANES, LANES), F32),
            pltpu.VMEM((nb, levels, LANES), F32),
            pltpu.VMEM((nb, nvec, LANES), F32),
            pltpu.VMEM((levels, nvec, LANES), F32),
            pltpu.VMEM((count, 8, LANES), F32),
            pltpu.VMEM((hosts, 8, LANES), F32),
            pltpu.VMEM((hosts, 8, LANES), F32),
            pltpu.VMEM((8, LANES), F32),
            pltpu.VMEM((8, LANES), F32),
            dma((5,)), dma((5,)),
        ],
        compiler_params=pltpu.CompilerParams(collective_id=0, has_side_effects=True),
    )(pair_exchange, conduction, valence, coulomb.reshape(1, planes), screening, vectors, energies, k_coords)
    return pl.pallas_call(
        finish,
        out_shape=(jax.ShapeDtypeStruct((nk, nb * nvec), F32), jax.ShapeDtypeStruct((nvec, nvec), F32)),
        in_specs=[vmem, vmem],
        out_specs=(pl.BlockSpec(memory_space=pl.ANY), pl.BlockSpec(memory_space=pl.ANY)),
        scratch_shapes=[dma((2,))],
    )(*[pltpu.with_memory_space_constraint(result, pltpu.VMEM) for result in results])


highest = lax.Precision.HIGHEST


def pair_factors(conduction, valence):
    count, valence_count, plane_count = valence.shape
    joined = (
        valence.astype(jnp.float32)[:, :, None, :] * conduction.astype(jnp.float32)[:, None, :, :]
    )
    return joined.reshape(count, valence_count * conduction.shape[1], plane_count).astype(
        jnp.bfloat16
    )


def transfer_index(rows_at, cols_at, mesh_cols):
    delta_first = jnp.mod(rows_at[:, None, 0] - cols_at[None, :, 0], MX)
    delta_second = jnp.mod(rows_at[:, None, 1] - cols_at[None, :, 1], mesh_cols)
    fold_first = jnp.minimum(delta_first, MX - delta_first)
    fold_second = jnp.minimum(delta_second, mesh_cols - delta_second)
    return (fold_first * (mesh_cols // 2 + 1) + fold_second).astype(jnp.int32)


def on_device(pair_exchange, conduction, valence, coulomb, screening, energies, vectors, k_coords):
    local_count, band_count, plane_count = pair_exchange.shape
    vector_count = vectors.shape[1] // band_count
    row_count = lax.axis_size("row")
    col_count = lax.axis_size("col")
    total_count = local_count * row_count * col_count
    mesh_cols = total_count // MX
    moving = vectors.reshape(local_count, band_count, vector_count)
    partial_density = jnp.einsum(
        "ktg,ktn->gn", pair_exchange, moving, preferred_element_type=jnp.float32
    )
    density = lax.psum(partial_density, ("row", "col"))
    block_size = 128
    sweeps = plane_count // block_size
    col_cond, col_val, col_vec, col_at = (
        lax.all_gather(conduction, "row", axis=0, tiled=True),
        lax.all_gather(valence, "row", axis=0, tiled=True),
        lax.all_gather(vectors, "row", axis=0, tiled=True),
        lax.all_gather(k_coords, "row", axis=0, tiled=True),
    )
    row_cond, row_val, row_at = (
        lax.all_gather(conduction, "col", axis=0, tiled=True),
        lax.all_gather(valence, "col", axis=0, tiled=True),
        lax.all_gather(k_coords, "col", axis=0, tiled=True),
    )
    row_pairs = pair_factors(row_cond, row_val)
    col_pairs = pair_factors(col_cond, col_val)
    indices = transfer_index(row_at, col_at, mesh_cols)
    col_moving = col_vec.reshape(-1, band_count, vector_count)

    def square_sweep(sweep_index, running):
        anchor = sweep_index * block_size
        coupling = jnp.take(
            lax.dynamic_slice_in_dim(screening, anchor, block_size, 1), indices, axis=0
        )
        row_block = lax.dynamic_slice_in_dim(row_pairs, anchor, block_size, 2)
        col_block = lax.dynamic_slice_in_dim(col_pairs, anchor, block_size, 2)
        col_proj = jnp.einsum(
            "ktg,ktn->kng", col_block, col_moving, preferred_element_type=jnp.float32
        )
        potential = jnp.einsum("ijg,jng->ing", coupling, col_proj, precision=highest)
        return running + jnp.einsum(
            "ktg,kng->ktn", row_block.astype(jnp.float32), potential, precision=highest
        )

    forward = lax.fori_loop(
        0,
        sweeps,
        square_sweep,
        jnp.zeros((row_pairs.shape[0], band_count, vector_count), jnp.float32),
    )
    owned = lax.psum_scatter(
        forward.reshape(col_count, local_count, band_count, vector_count),
        "col",
        scatter_dimension=0,
        tiled=True,
    )[0]
    moving_wide = moving.astype(jnp.float32)
    exchange_term = jnp.einsum(
        "ktg,gn->ktn", pair_exchange.astype(jnp.float32) * coulomb, density, precision=highest
    )
    applied = (
        energies[:, :, None] * moving_wide
        + 2.0 / (total_count * band_count) * exchange_term
        - owned / total_count
    )
    gram = jnp.einsum("ktm,ktn->mn", moving_wide, applied, precision=highest)
    alpha = lax.psum(gram, ("row", "col")) / (total_count * band_count)
    residual = applied - jnp.einsum("ktm,mn->ktn", moving_wide, alpha, precision=highest)
    return (residual.reshape(local_count, band_count * vector_count), alpha)


def fits(args, mesh):
    pair_exchange, conduction, valence, _, screening, _, vectors, _ = args
    rows, cols = mesh.shape["row"], mesh.shape["col"]
    points, nb, planes = pair_exchange.shape
    nk = points // (rows * cols)
    nv, nc = valence.shape[1], conduction.shape[1]
    nvec = vectors.shape[1] // nb
    return (
        planes == rows * LANES and rows == 8 and cols == 4 and rows * cols * nk * 2 == LANES and nk == 2 and nv == 4 and nc == 4
        and nc * nvec == LANES and points == 2 * MX and screening.shape[0] == MX + 2
    )


def solution(mesh):
    in_specs = (
        P(("row", "col"), None, None),
        P(("row", "col"), None, None),
        P(("row", "col"), None, None),
        P(),
        P(),
        P(("row", "col"), None),
        P(("row", "col"), None),
        P(("row", "col"), None),
    )
    out_specs = (P(("row", "col"), None), P())

    def run(*args):
        body = fast_on_device if fits(args, mesh) else on_device
        return jax.shard_map(
            body, mesh=mesh, in_specs=in_specs, out_specs=out_specs, check_vma=False
        )(*args)

    return run
```
